32 devices in a mesh: dp: 8 (over z, y), mp: 4 (over x, core).
Axes of the slice: x: 2, y: 2, z: 4, core: 2. Of those that a mesh axis runs over, the one named last changes fastest.
Arguments:
- inputs: bfloat16 [16384, 1024], P(('dp', 'mp')), may hold values from -6 to 6
- first_values: bfloat16 [16384, 8, 64], P('dp', 'mp'), may hold values from -6 to 6
- cotangent: bfloat16 [16384, 1024], P(('dp', 'mp')), may hold values from -6 to 6
- seq_lengths: int32 [32], P('dp'), may hold values from 0 to 1024, as said below
- value_owner: int32 [8], replicated, may hold values from 0 to 7, each once
- attn_norm_gain: float32 [1024], replicated, may hold values from 0.5 to 1.5
- attn_norm_bias: float32 [1024], replicated, may hold values from -3 to 3
- qkv_weight: bfloat16 [1024, 8, 5, 64], P(None, 'mp'), may hold values from -0.25 to 0.25
- qv_bias: float32 [8, 3, 64], P('mp'), may hold values from -3 to 3
- out_weight: bfloat16 [8, 2, 64, 1024], P('mp'), may hold values from -0.75 to 0.75
- out_bias: float32 [1024], replicated, may hold values from -3 to 3
- mlp_norm_gain: float32 [1024], replicated, may hold values from 0.5 to 1.5
- mlp_norm_bias: float32 [1024], replicated, may hold values from -3 to 3
- up_weight: bfloat16 [1024, 4096], P(None, 'mp'), may hold values from -0.1875 to 0.1875
- up_bias: float32 [4096], P('mp'), may hold values from -3 to 3
- down_weight: bfloat16 [4096, 1024], P('mp'), may hold values from -0.09375 to 0.09375
- down_bias: float32 [1024], replicated, may hold values from -3 to 3
Outputs:
- output: bfloat16 [16384, 1024], P(('dp', 'mp'))
- grad_inputs: bfloat16 [16384, 1024], P(('dp', 'mp'))
- grad_first_values: bfloat16 [16384, 8, 64], P('dp', 'mp')
- grad_attn_norm_gain: float32 [1024], replicated
- grad_attn_norm_bias: float32 [1024], replicated
- grad_qkv_weight: float32 [1024, 8, 5, 64], P(None, 'mp')
- grad_qv_bias: float32 [8, 3, 64], P('mp')
- grad_out_weight: float32 [8, 2, 64, 1024], P('mp')
- grad_out_bias: float32 [1024], replicated
- grad_mlp_norm_gain: float32 [1024], replicated
- grad_mlp_norm_bias: float32 [1024], replicated
- grad_up_weight: float32 [1024, 4096], P(None, 'mp')
- grad_up_bias: float32 [4096], P('mp')
- grad_down_weight: float32 [4096, 1024], P('mp')
- grad_down_bias: float32 [1024], replicated
The draws below stay inside these ranges and needn't reach their ends.
Inputs may be any that keep to these rules, and one draw needn't show every extreme that they name: `seq_lengths`: each data group's 4 entries, in row order, are the lengths of the sequences packed into its 2048 rows: each 512 or 1024, then zeros for unused slots; they sum to 2048, and some group holds a sequence of 1024. A permutation: skip-value head p reuses the first layer's value head value_owner[p].
All inputs are finite; a program needn't handle non-finite values.
Results may differ from the reference program's by a relative error of at most 0.019.
Values may be sent and summed in bfloat16 or wider, within the bound.
A program may use at most 128 MiB of HBM per device.

```python
import jax
import jax.numpy as jnp
from jax import lax

D = 1024
HD = 64
FF = 4096
SHORT = 512
SLOTS = 4
PAIRS = 8
GROUP = 2048
GROUPS = 8
TOKENS = 16384
QB = 512
N_MP = 4


def draw_seq_lengths(key, part):
    patterns = jnp.array([[2, 2, 0, 0], [2, 1, 1, 0], [1, 2, 1, 0], [1, 1, 2, 0], [1, 1, 1, 1]], dtype=jnp.int32)
    picks = jax.random.randint(key, (GROUPS,), 0, 5)
    forced = jax.random.randint(jax.random.fold_in(key, 7), (), 0, GROUPS)
    picks = jnp.where(jnp.arange(GROUPS) == forced, 0, picks)
    return (patterns[picks] * SHORT).reshape(GROUPS * SLOTS).astype(jnp.int32)


def steps_of(key, extent, split, least, largest):
    factor_of, own = 1.0, jax.random.fold_in(key, 6)
    for position, shards_of in split:
        heights = jnp.exp(jax.random.uniform(jax.random.fold_in(own, position), (shards_of,), jnp.float32, least / len(split), largest / len(split)))
        factor_of = factor_of * jnp.repeat(heights, extent[position] // shards_of).reshape([-1 if axis == position else 1 for axis in range(len(extent))])
    return factor_of


def normal_values(key, extent, width, limit, shards=(), kind=jnp.bfloat16):
    loudness = steps_of(key, extent, shards, -0.22, 0.18) if shards else 1.0
    values = jax.random.normal(key, extent, jnp.float32) * width * loudness
    return jnp.minimum(jnp.maximum(values, -limit), limit).astype(kind)


def setup_inputs(seed: int = 0) -> dict:
    arg_keys = jax.random.split(jax.random.key(seed), 18)
    inputs = normal_values(arg_keys[0], (TOKENS, D), 1.0, 6.0, ((0, 32),))
    first_values = normal_values(arg_keys[1], (TOKENS, PAIRS, HD), 1.0, 6.0, ((0, 8), (1, 4)))
    cotangent = normal_values(arg_keys[2], (TOKENS, D), 1.0, 6.0, ((0, 32),))
    seq_lengths = draw_seq_lengths(jax.random.fold_in(arg_keys[17], 71), 0)
    value_owner = jax.random.permutation(arg_keys[4], PAIRS).astype(jnp.int32)
    attn_norm_gain = jnp.clip(1.0 + 0.1 * jax.random.normal(arg_keys[5], (D,), jnp.float32), 0.5, 1.5)
    attn_norm_bias = normal_values(arg_keys[6], (D,), 0.3, 3.0, (), jnp.float32)
    qkv_weight = normal_values(arg_keys[7], (D, PAIRS, 5, HD), (D // 2) ** -0.5, 0.25, ((1, 4),))
    qv_bias = normal_values(arg_keys[8], (PAIRS, 3, HD), 0.5, 3.0, ((0, 4),), jnp.float32)
    out_weight = normal_values(arg_keys[9], (PAIRS, 2, HD, D), (2 * PAIRS * HD // 16) ** -0.5, 0.75, ((0, 4),))
    out_bias = normal_values(arg_keys[10], (D,), 0.3, 3.0, (), jnp.float32)
    mlp_norm_gain = jnp.clip(1.0 + 0.1 * jax.random.normal(arg_keys[11], (D,), jnp.float32), 0.5, 1.5)
    mlp_norm_bias = normal_values(arg_keys[12], (D,), 0.3, 3.0, (), jnp.float32)
    up_weight = normal_values(arg_keys[13], (D, FF), D ** -0.5, 0.1875, ((1, 4),))
    up_bias = normal_values(arg_keys[14], (FF,), 0.5, 3.0, ((0, 4),), jnp.float32)
    down_weight = normal_values(arg_keys[15], (FF, D), FF ** -0.5, 0.09375, ((0, 4),))
    down_bias = normal_values(arg_keys[16], (D,), 0.3, 3.0, (), jnp.float32)
    return dict(inputs=inputs, first_values=first_values, cotangent=cotangent, seq_lengths=seq_lengths, value_owner=value_owner, attn_norm_gain=attn_norm_gain, attn_norm_bias=attn_norm_bias, qkv_weight=qkv_weight, qv_bias=qv_bias, out_weight=out_weight, out_bias=out_bias, mlp_norm_gain=mlp_norm_gain, mlp_norm_bias=mlp_norm_bias, up_weight=up_weight, up_bias=up_bias, down_weight=down_weight, down_bias=down_bias)


EPSILON = 1e-05
MASKED = -1e+30
GELU_C = 0.7978845608028654
HIGHEST = lax.Precision.HIGHEST

@jax.custom_vjp
def low(v):
    return lax.optimization_barrier(v.astype(jnp.bfloat16)).astype(jnp.float32)

@jax.custom_vjp
def low_back(v):
    return v

def low_keep(v):
    return (low(v), None)

def low_pass(kept, grad):
    return (grad,)

def back_keep(v):
    return (v, None)

def back_low(kept, grad):
    return (low(grad),)
low.defvjp(low_keep, low_pass)
low_back.defvjp(back_keep, back_low)

def layer_norm(values, scale_gain, scale_bias):
    average = lax.optimization_barrier(jnp.mean(values, axis=-1, keepdims=True))
    centered = values - average
    variance = lax.optimization_barrier(jnp.mean(centered * centered, axis=-1, keepdims=True))
    return centered * lax.rsqrt(variance + EPSILON) * scale_gain + scale_bias

def gelu_tanh(values):
    return 0.5 * values * (1.0 + jnp.tanh(GELU_C * (values + 0.044715 * values * values * values)))

def row_starts(lengths, group_rows):
    ends = jnp.cumsum(lengths).astype(jnp.int32)
    begins = (ends - lengths).astype(jnp.int32)
    positions = jnp.arange(group_rows, dtype=jnp.int32)
    inside = begins[None, :] <= positions[:, None]
    return lax.optimization_barrier(jnp.max(jnp.where(inside, begins[None, :], 0), axis=1)).astype(jnp.int32)

def block_mask(starts, first_row, block_rows, span):
    own_rows = first_row + jnp.arange(block_rows, dtype=jnp.int32)
    key_rows = first_row - (span - block_rows) + jnp.arange(span, dtype=jnp.int32)
    begin = lax.dynamic_slice_in_dim(starts, first_row, block_rows, 0)
    return (key_rows[None, :] >= begin[:, None]) & (key_rows[None, :] <= own_rows[:, None])

def attention(queries, keys, values_in, starts):
    heads = queries.shape[1]
    long_len = 2 * SHORT
    span = long_len + QB
    scale = HD ** (-0.5)
    zero_pad = jnp.zeros((long_len, heads, HD), jnp.float32)
    keys_pad = jnp.concatenate([zero_pad, keys], 0)
    values_pad = jnp.concatenate([zero_pad, values_in], 0)

    def one_block(block_index):
        first_row = (block_index * QB).astype(jnp.int32)
        query_blk = lax.dynamic_slice_in_dim(queries, first_row, QB, 0)
        key_blk = lax.dynamic_slice_in_dim(keys_pad, first_row, span, 0)
        value_blk = lax.dynamic_slice_in_dim(values_pad, first_row, span, 0)
        allowed = block_mask(starts, first_row, QB, span)
        scores = low_back(jnp.einsum('qhd,khd->hqk', query_blk, key_blk, precision=HIGHEST) * scale)
        scores = jnp.where(allowed[None], scores, MASKED)
        top_score = lax.optimization_barrier(jnp.max(scores, axis=-1, keepdims=True))
        weights = jnp.exp(scores - top_score)
        probs = weights / lax.optimization_barrier(jnp.sum(weights, axis=-1, keepdims=True))
        return jnp.einsum('hqk,khd->qhd', low(probs), value_blk, precision=HIGHEST)
    mixed = lax.map(jax.checkpoint(one_block), jnp.arange(GROUP // QB, dtype=jnp.int32))
    return mixed.reshape(GROUP, heads, HD)

def group_forward(params, rows_in, values_in, lengths, value_owner):
    norm_one_gain, norm_one_bias, qkv_weight, qv_bias, out_weight, out_bias, norm_two_gain, norm_two_bias, up_weight, up_bias, down_weight, down_bias = params
    starts = row_starts(lengths, GROUP)
    normed_one = low(layer_norm(rows_in, norm_one_gain, norm_one_bias))
    projected = jnp.einsum('gd,dpkh->gpkh', normed_one, qkv_weight, precision=HIGHEST)
    queries = low(low_back(projected[:, :, 0:2] + qv_bias[None, :, 0:2]))
    keys = low(low_back(projected[:, :, 2:4]))
    fresh = low(low_back(projected[:, :, 4] + qv_bias[None, :, 2]))
    skipped = jnp.take(values_in, value_owner, axis=1)
    values_all = jnp.stack([fresh, skipped], axis=2)
    mixed = attention(queries.reshape(GROUP, 2 * PAIRS, HD), keys.reshape(GROUP, 2 * PAIRS, HD), values_all.reshape(GROUP, 2 * PAIRS, HD), starts)
    mixed = low(low_back(mixed)).reshape(GROUP, PAIRS, 2, HD)
    pairs_dev = PAIRS // N_MP
    attn_total = jnp.zeros((GROUP, D), jnp.float32)
    for member in range(N_MP):
        lower = member * pairs_dev
        attn_total = attn_total + low(jnp.einsum('gpkh,pkhd->gd', mixed[:, lower:lower + pairs_dev], out_weight[lower:lower + pairs_dev], precision=HIGHEST))
    residual = rows_in + low_back(attn_total) + out_bias
    normed_two = low(layer_norm(residual, norm_two_gain, norm_two_bias))
    hidden_pre = low_back(jnp.dot(normed_two, up_weight, precision=HIGHEST) + up_bias)
    hidden = low(gelu_tanh(hidden_pre))
    units_dev = FF // N_MP
    mlp_total = jnp.zeros((GROUP, D), jnp.float32)
    for member in range(N_MP):
        lower = member * units_dev
        mlp_total = mlp_total + low(jnp.dot(hidden[:, lower:lower + units_dev], down_weight[lower:lower + units_dev], precision=HIGHEST))
    return residual + mlp_total + down_bias

def reference(inputs, first_values, cotangent, seq_lengths, value_owner, attn_norm_gain, attn_norm_bias, qkv_weight, qv_bias, out_weight, out_bias, mlp_norm_gain, mlp_norm_bias, up_weight, up_bias, down_weight, down_bias):
    listed = (attn_norm_gain, attn_norm_bias, qkv_weight, qv_bias, out_weight, out_bias, mlp_norm_gain, mlp_norm_bias, up_weight, up_bias, down_weight, down_bias)
    params_in = tuple((argument.astype(jnp.float32) for argument in listed))
    rows_in = inputs.astype(jnp.float32).reshape(GROUPS, GROUP, D)
    values_in = first_values.astype(jnp.float32).reshape(GROUPS, GROUP, PAIRS, HD)
    lengths = seq_lengths.reshape(GROUPS, SLOTS)

    def whole_layer(params, rows_all, values_all):

        def one_group(carried, group_item):
            return (carried, group_forward(params, group_item[0], group_item[1], group_item[2], value_owner))
        return lax.scan(jax.checkpoint(one_group), jnp.zeros((), jnp.float32), (rows_all, values_all, lengths))[1]
    layer_out, backward = jax.vjp(whole_layer, params_in, rows_in, values_in)
    grads, grad_rows, grad_values = backward(cotangent.astype(jnp.float32).reshape(GROUPS, GROUP, D))
    return (layer_out.reshape(TOKENS, D).astype(jnp.bfloat16), grad_rows.reshape(TOKENS, D).astype(jnp.bfloat16), grad_values.reshape(TOKENS, PAIRS, HD).astype(jnp.bfloat16), grads[0], grads[1], grads[2], grads[3], grads[4], grads[5], grads[6], grads[7], grads[8], grads[9], grads[10], grads[11])
```

```python
import functools

import jax
import jax.numpy as jnp
from jax import lax
from jax.experimental import pallas as pl
from jax.experimental.pallas import tpu as pltpu
from jax.sharding import PartitionSpec as P

SHORT = 512
QROWS = 256
LANES = 128
PACK = 6

EPSILON = 1e-05
MASKED = -1e30
GELU_C = 0.7978845608028654
BF16 = jnp.bfloat16
F32 = jnp.float32


def layer_norm(values, scale_gain, scale_bias):
    average = jnp.mean(values, axis=-1, keepdims=True)
    centered = values - average
    variance = jnp.mean(centered * centered, axis=-1, keepdims=True)
    return centered * lax.rsqrt(variance + EPSILON) * scale_gain + scale_bias


def gelu_tanh(values):
    return 0.5 * values * (1.0 + jnp.tanh(GELU_C * (values + 0.044715 * values * values * values)))


def rows_product(left, right):
    return lax.dot_general(left, right, (((0,), (0,)), ((), ())), preferred_element_type=F32)


def back_product(left, weight):
    return lax.dot_general(left, weight, (((1,), (1,)), ((), ())), preferred_element_type=F32)


def product(left, right):
    return jnp.dot(left, right, preferred_element_type=F32)


def opens_at(lengths, row):
    begin, opens = jnp.int32(0), jnp.int32(0)
    for slot in range(lengths.shape[0]):
        opens = jnp.maximum(opens, jnp.where(begin == row, 1, 0))
        begin = begin + lengths[slot]
    return opens


def head_lanes(head):
    lane = lax.broadcasted_iota(jnp.int32, (1, LANES), 1)
    return (lane < LANES // 2) if head == 0 else (lane >= LANES // 2)


def causal_tile():
    row = lax.broadcasted_iota(jnp.int32, (QROWS, QROWS), 0)
    column = lax.broadcasted_iota(jnp.int32, (QROWS, QROWS), 1)
    return column <= row


def pick_values(half, qkv_ref, first_ref, value_ref):
    held = first_ref[0]
    if held.shape[1] < LANES:
        turned = jnp.concatenate([held, held], axis=1)
    else:
        turned = jnp.concatenate([held[:, LANES // 2 :], held[:, : LANES // 2]], axis=1)
        turned = jnp.where(half == 1, held, turned)
    value_ref[...] = jnp.where(head_lanes(0), qkv_ref[:, 2 * LANES : 3 * LANES], turned)


def attend_forward_kernel(pairs, lengths, owner, place, qkv_ref, first_ref, mixed_ref, totals_ref, value_ref):
    pick_values(lax.rem(owner[place[0] * pairs + pl.program_id(0)], pairs), qkv_ref, first_ref, value_ref)
    blocks = qkv_ref.shape[0] // SHORT
    scale = (LANES // 2) ** (-0.5)

    def block(index, carried):
        base = pl.multiple_of(index * SHORT, SHORT)
        for half in range(SHORT // QROWS):
            first = base + half * QROWS

            def attend(with_previous):
                query = qkv_ref[pl.ds(first, QROWS), 0:LANES] * jnp.asarray(scale, BF16)
                spans = []
                if with_previous:
                    spans.append((base - SHORT, SHORT))
                if half:
                    spans.append((base, half * QROWS))
                spans.append((first, QROWS))
                mixed = jnp.zeros((QROWS, LANES), F32)
                totals = []
                for head in range(2):
                    chosen = head_lanes(head)
                    query_head = jnp.where(chosen, query, jnp.zeros_like(query))
                    scores = [
                        back_product(query_head, qkv_ref[pl.ds(at, size), LANES : 2 * LANES])
                        for at, size in spans
                    ]
                    scores[-1] = jnp.where(causal_tile(), scores[-1], MASKED)
                    top = scores[0].max(axis=1, keepdims=True)
                    for part in scores[1:]:
                        top = jnp.maximum(top, part.max(axis=1, keepdims=True))
                    total = jnp.zeros((QROWS, 1), F32)
                    gathered = jnp.zeros((QROWS, LANES), F32)
                    for (at, size), part in zip(spans, scores):
                        weights = jnp.exp(part - top)
                        total = total + weights.sum(axis=1, keepdims=True)
                        values = value_ref[pl.ds(at, size), :]
                        values = jnp.where(chosen, values, jnp.zeros_like(values))
                        gathered = gathered + product(weights.astype(BF16), values)
                    mixed = mixed + gathered / total
                    totals.append(top + jnp.log(total))
                mixed_ref[pl.ds(first, QROWS), :] = mixed.astype(BF16)
                totals_ref[pl.ds(first, QROWS), :] = jnp.where(
                    head_lanes(0), totals[0], totals[1]
                )

            @pl.when(opens_at(lengths, base) == 0)
            def _():
                attend(True)

            @pl.when(opens_at(lengths, base) == 1)
            def _():
                attend(False)

        return carried

    lax.fori_loop(0, blocks, block, 0)


def attend_backward_kernel(
    pairs, lengths, owner, place, qkv_ref, first_ref, grad_ref, totals_ref, out_ref, key_sum, value_sum, value_ref
):
    pick_values(lax.rem(owner[place[0] * pairs + pl.program_id(0)], pairs), qkv_ref, first_ref, value_ref)
    blocks = qkv_ref.shape[0] // SHORT
    scale = (LANES // 2) ** (-0.5)
    key_sum[...] = jnp.zeros_like(key_sum)
    value_sum[...] = jnp.zeros_like(value_sum)

    def block(index, carried):
        base = pl.multiple_of(index * SHORT, SHORT)
        for half in range(SHORT // QROWS):
            first = base + half * QROWS

            def attend(with_previous):
                query = qkv_ref[pl.ds(first, QROWS), 0:LANES] * jnp.asarray(scale, BF16)
                grad = grad_ref[pl.ds(first, QROWS), :]
                spans = []
                if with_previous:
                    spans.append((base - SHORT, SHORT))
                if half:
                    spans.append((base, half * QROWS))
                spans.append((first, QROWS))
                grad_query = jnp.zeros((QROWS, LANES), F32)
                for head in range(2):
                    chosen = head_lanes(head)
                    query_head = jnp.where(chosen, query, jnp.zeros_like(query))
                    grad_head = jnp.where(chosen, grad, jnp.zeros_like(grad))
                    at_lane = head * (LANES // 2)
                    totals = totals_ref[pl.ds(first, QROWS), at_lane : at_lane + 1]
                    probs, grads = [], []
                    inner = jnp.zeros((QROWS, 1), F32)
                    for at, size in spans:
                        keys = qkv_ref[pl.ds(at, size), LANES : 2 * LANES]
                        part = jnp.exp(back_product(query_head, keys) - totals)
                        if at is first:
                            part = jnp.where(causal_tile(), part, 0.0)
                        values = value_ref[pl.ds(at, size), :]
                        weighted = part * back_product(grad_head, values)
                        inner = inner + weighted.sum(axis=1, keepdims=True)
                        probs.append(part)
                        grads.append(weighted)
                    for (at, size), part, weighted in zip(spans, probs, grads):
                        keys = qkv_ref[pl.ds(at, size), LANES : 2 * LANES]
                        keys = jnp.where(chosen, keys, jnp.zeros_like(keys))
                        grad_scores = (weighted - part * inner).astype(BF16)
                        grad_query = grad_query + product(grad_scores, keys)
                        key_sum[pl.ds(at, size), :] += rows_product(grad_scores, query_head)
                        value_sum[pl.ds(at, size), :] += rows_product(part.astype(BF16), grad_head)
                out_ref[pl.ds(first, QROWS), 0:LANES] = (grad_query * scale).astype(BF16)

            @pl.when(opens_at(lengths, base) == 0)
            def _():
                attend(True)

            @pl.when(opens_at(lengths, base) == 1)
            def _():
                attend(False)

        return carried

    lax.fori_loop(0, blocks, block, 0)
    out_ref[:, LANES : 2 * LANES] = key_sum[...].astype(BF16)
    out_ref[:, 2 * LANES : 3 * LANES] = value_sum[...].astype(BF16)


def attend_forward(lengths, owner, place, packed, firsts):
    rows, pairs = packed.shape[0], packed.shape[1] // (3 * LANES)
    return pl.pallas_call(
        functools.partial(attend_forward_kernel, pairs),
        grid_spec=pltpu.PrefetchScalarGridSpec(
            num_scalar_prefetch=3,
            grid=(pairs,),
            in_specs=[
                pl.BlockSpec((rows, 3 * LANES), lambda p, c, o, m: (0, p)),
                pl.BlockSpec((1, rows, firsts.shape[2]), lambda p, c, o, m: (lax.div(o[m[0] * pairs + p], pairs), 0, 0)),
            ],
            out_specs=[
                pl.BlockSpec((rows, LANES), lambda p, c, o, m: (0, p)),
                pl.BlockSpec((rows, LANES), lambda p, c, o, m: (0, p)),
            ],
            scratch_shapes=[pltpu.VMEM((rows, LANES), BF16)],
        ),
        out_shape=[
            jax.ShapeDtypeStruct((rows, pairs * LANES), BF16),
            jax.ShapeDtypeStruct((rows, pairs * LANES), F32),
        ],
        cost_estimate=pl.CostEstimate(
            flops=rows * 1024 * 256 * 4 * pairs, bytes_accessed=8 << 20, transcendentals=rows * 2048
        ),
        name="attend_forward",
    )(lengths, owner, place, packed, firsts)


def attend_backward(lengths, owner, place, packed, firsts, grad, totals):
    rows, pairs = packed.shape[0], packed.shape[1] // (3 * LANES)
    return pl.pallas_call(
        functools.partial(attend_backward_kernel, pairs),
        grid_spec=pltpu.PrefetchScalarGridSpec(
            num_scalar_prefetch=3,
            grid=(pairs,),
            in_specs=[
                pl.BlockSpec((rows, 3 * LANES), lambda p, c, o, m: (0, p)),
                pl.BlockSpec((1, rows, firsts.shape[2]), lambda p, c, o, m: (lax.div(o[m[0] * pairs + p], pairs), 0, 0)),
                pl.BlockSpec((rows, LANES), lambda p, c, o, m: (0, p)),
                pl.BlockSpec((rows, LANES), lambda p, c, o, m: (0, p)),
            ],
            out_specs=pl.BlockSpec((rows, 3 * LANES), lambda p, c, o, m: (0, p)),
            scratch_shapes=[
                pltpu.VMEM((rows, LANES), F32),
                pltpu.VMEM((rows, LANES), F32),
                pltpu.VMEM((rows, LANES), BF16),
            ],
        ),
        out_shape=jax.ShapeDtypeStruct((rows, pairs * 3 * LANES), BF16),
        cost_estimate=pl.CostEstimate(
            flops=rows * 1024 * 256 * 10 * pairs, bytes_accessed=8 << 20, transcendentals=rows * 2048
        ),
        name="attend_backward",
    )(lengths, owner, place, packed, firsts, grad, totals)


def mesh_place(count):
    place = lax.axis_index("mp")
    core = lax.rem(place, 2)
    chip = lax.div(place, 2)
    chips = count // 2

    def across(step, other):
        return lax.rem(chip + step + chips, chips) * 2 + (1 - core if other else core)

    return place, place + 1 - 2 * core, across


def remote(source, target, sems, index, device):
    return pltpu.make_async_remote_copy(
        src_ref=source,
        dst_ref=target,
        send_sem=sems.at[(0, *index)],
        recv_sem=sems.at[(1, *index)],
        device_id={"mp": device},
        device_id_type=pl.DeviceIdType.MESH,
    )


def greet(count, copies=0):
    place, partner, across = mesh_place(count)
    barrier = pltpu.get_barrier_semaphore()
    for device in [partner] + [across(step, False) for step in range(1, count // 2)]:
        pl.semaphore_signal(
            barrier, inc=1, device_id={"mp": device}, device_id_type=pl.DeviceIdType.MESH
        )
    others = DpPlace(copies).greet(barrier) if copies else 0
    pl.semaphore_wait(barrier, count // 2 + others)


def each(count, step):
    def run(index, carried):
        step(index)
        return carried

    lax.fori_loop(0, count, run, 0)


class Gather:
    def __init__(self, count, out_ref, chunk, near, far, passed):
        self.count, self.out, self.chunk = count, out_ref, chunk
        self.near, self.far, self.passed = near, far, passed
        self.place, self.partner, self.across = mesh_place(count)

    def part(self, owner, index):
        return self.out.at[owner, pl.ds(pl.multiple_of(index * self.chunk, self.chunk), self.chunk), :]

    def send(self, index):
        own = self.part(self.place, index)
        for step in range(1, self.count // 2):
            remote(own, own, self.far, (step - 1, index), self.across(step, False)).start()
        remote(own, own, self.near, (index,), self.partner).start()

    def hand_on(self, index):
        for step in range(1, self.count // 2):
            got = self.part(self.across(-step, False), index)
            remote(got, got, self.far, (step - 1, index), self.across(step, False)).wait_recv()
            remote(got, got, self.passed, (step - 1, index), self.partner).start()

    def finish(self, index):
        own = self.part(self.place, index)
        near = self.part(self.partner, index)
        remote(own, near, self.near, (index,), self.partner).wait()
        for step in range(1, self.count // 2):
            remote(own, own, self.far, (step - 1, index), self.across(step, False)).wait_send()
            got = self.part(self.across(-step, True), index)
            remote(got, got, self.passed, (step - 1, index), self.partner).wait()


def gather_sems(count, chunks):
    far = max(count // 2 - 1, 1)
    return [
        pltpu.SemaphoreType.DMA((2, chunks)),
        pltpu.SemaphoreType.DMA((2, far, chunks)),
        pltpu.SemaphoreType.DMA((2, far, chunks)),
    ]


class RowSum:
    def __init__(self, count, rows, chunk, left, weight, flipped, buffers):
        self.count, self.rows, self.chunk = count, rows, chunk
        self.left, self.weight, self.flipped = left, weight, flipped
        (self.pair_out, self.pair_in, self.far_out, self.far_in, self.near_out, self.near_in) = buffers[:6]
        self.pair, self.far, self.near = buffers[6:]
        self.place, self.partner, self.across = mesh_place(count)

    def product(self, owner, index):
        at = pl.multiple_of(owner * self.rows + index * self.chunk, self.chunk)
        rows = self.left[pl.ds(at, self.chunk), :]
        return (back_product if self.flipped else product)(rows, self.weight[...])

    def pair_copy(self, step, index):
        return remote(
            self.pair_out.at[step - 1, index], self.pair_in.at[step - 1, index],
            self.pair, (step - 1, index), self.partner,
        )

    def far_copy(self, step, index):
        return remote(
            self.far_out.at[step - 1, index], self.far_in.at[step - 1, index],
            self.far, (step - 1, index), self.across(step, False),
        )

    def near_copy(self, index):
        return remote(self.near_out.at[index], self.near_in.at[index], self.near, (index,), self.partner)

    def send(self):
        chunks = self.rows // self.chunk

        def pair(index):
            for step in range(1, self.count // 2):
                self.pair_out[step - 1, index] = self.product(self.across(step, True), index).astype(BF16)
                self.pair_copy(step, index).start()

        def far(index):
            for step in range(1, self.count // 2):
                own = self.product(self.across(step, False), index)
                self.pair_copy(step, index).wait_recv()
                self.far_out[step - 1, index] = (own + self.pair_in[step - 1, index].astype(F32)).astype(BF16)
                self.far_copy(step, index).start()

        def near(index):
            self.near_out[index] = self.product(self.partner, index).astype(BF16)
            self.near_copy(index).start()

        each(chunks, pair)
        each(chunks, far)
        each(chunks, near)

    def total(self, index):
        rows = self.product(self.place, index)
        self.near_copy(index).wait_recv()
        rows = rows + self.near_in[index].astype(F32)
        for step in range(1, self.count // 2):
            self.far_copy(step, index).wait_recv()
            rows = rows + self.far_in[step - 1, index].astype(F32)
        return rows

    def finish(self, index):
        self.near_copy(index).wait_send()
        for step in range(1, self.count // 2):
            self.pair_copy(step, index).wait_send()
            self.far_copy(step, index).wait_send()


def split_copies(copies):
    inner = 1
    while (2 * inner) ** 2 <= copies:
        inner *= 2
    return copies // inner, inner


def dp_copy(source, target, send_sem, recv_sem, device):
    return pltpu.make_async_remote_copy(
        src_ref=source, dst_ref=target, send_sem=send_sem, recv_sem=recv_sem,
        device_id={"dp": device}, device_id_type=pl.DeviceIdType.MESH,
    )


class DpPlace:
    def __init__(self, copies):
        self.outer, self.inner = split_copies(copies)
        here = lax.axis_index("dp")
        self.z, self.y = lax.div(here, self.inner), lax.rem(here, self.inner)

    def along_y(self, step):
        return lax.rem(self.y + step + self.inner, self.inner)

    def along_z(self, step):
        return lax.rem(self.z + step + self.outer, self.outer)

    def device(self, z, y):
        return z * self.inner + y

    def greet(self, barrier):
        for step in range(1, self.inner):
            pl.semaphore_signal(
                barrier, inc=1, device_id={"dp": self.device(self.z, self.along_y(step))},
                device_id_type=pl.DeviceIdType.MESH,
            )
        for step in range(1, self.outer):
            pl.semaphore_signal(
                barrier, inc=1, device_id={"dp": self.device(self.along_z(step), self.y)},
                device_id_type=pl.DeviceIdType.MESH,
            )
        return self.inner + self.outer - 2


class DpReduce:
    def __init__(self, copies, source, y_in, z_out, z_in, y_sems, z_sems):
        self.at = DpPlace(copies)
        self.source, self.y_in, self.z_out, self.z_in = source, y_in, z_out, z_in
        self.y_sems, self.z_sems = y_sems, z_sems

    def y_copy(self, step, z):
        peer = self.at.along_y(step)
        return dp_copy(
            self.source.at[z, peer], self.y_in.at[step - 1, z],
            self.y_sems.at[0, step - 1, z], self.y_sems.at[1, step - 1, z], self.at.device(self.at.z, peer),
        )

    def z_copy(self, step):
        peer = self.at.along_z(step + 1)
        return dp_copy(
            self.z_out.at[step], self.z_in.at[step],
            self.z_sems.at[0, step], self.z_sems.at[1, step], self.at.device(peer, self.at.y),
        )

    def send(self):
        def start(step):
            for y_step in range(1, self.at.inner):
                self.y_copy(y_step, self.at.along_z(step + 1)).start()

        each(self.at.outer, start)

    def y_total(self, z):
        total = self.source[z, self.at.y].astype(F32)
        for y_step in range(1, self.at.inner):
            self.y_copy(y_step, z).wait_recv()
            total = total + self.y_in[y_step - 1, z].astype(F32)
        return total

    def pass_on(self, step):
        @pl.when(step < self.at.outer - 1)
        def _():
            self.z_out[step] = self.y_total(self.at.along_z(step + 1)).astype(BF16)
            self.z_copy(step).start()

    def total(self):
        total = self.y_total(self.at.z)
        for step in range(self.at.outer - 1):
            self.z_copy(step).wait_recv()
            total = total + self.z_in[step].astype(F32)
        for step in range(self.at.outer - 1):
            self.z_copy(step).wait_send()
        for y_step in range(1, self.at.inner):
            for z in range(self.at.outer):
                self.y_copy(y_step, z).wait_send()
        return total


def reduce_scratch(copies, array):
    outer, inner = split_copies(copies)
    slab = array.shape[2:]
    return [
        pltpu.VMEM((inner - 1, outer, *slab), BF16),
        pltpu.VMEM((outer - 1, *slab), BF16),
        pltpu.VMEM((outer - 1, *slab), BF16),
        pltpu.SemaphoreType.DMA((2, inner - 1, outer)),
        pltpu.SemaphoreType.DMA((2, outer - 1)),
    ]


class DpGather:
    def __init__(self, copies, slab, held, z_sems, y_sems):
        self.at = DpPlace(copies)
        self.slab, self.held, self.z_sems, self.y_sems = slab, held, z_sems, y_sems

    def z_copy(self, step, z):
        here = self.held.at[z, self.at.y]
        peer = self.at.device(self.at.along_z(step + 1), self.at.y)
        return dp_copy(here, here, self.z_sems.at[0, step], self.z_sems.at[1, step], peer)

    def y_copy(self, y_step, slot, z, y):
        here = self.held.at[z, y]
        peer = self.at.device(self.at.z, self.at.along_y(y_step))
        return dp_copy(
            here, here, self.y_sems.at[0, y_step - 1, slot], self.y_sems.at[1, y_step - 1, slot], peer
        )

    def send(self):
        self.held[self.at.z, self.at.y] = self.slab[...]
        for step in range(self.at.outer - 1):
            self.z_copy(step, self.at.z).start()
        for y_step in range(1, self.at.inner):
            self.y_copy(y_step, self.at.outer - 1, self.at.z, self.at.y).start()

    def pass_on(self, step):
        @pl.when(step < self.at.outer - 1)
        def _():
            source = self.at.along_z(-step - 1)
            self.z_copy(step, source).wait_recv()
            for y_step in range(1, self.at.inner):
                self.y_copy(y_step, step, source, self.at.y).start()

    def finish(self):
        for step in range(self.at.outer - 1):
            self.z_copy(step, self.at.z).wait_send()
        for y_step in range(1, self.at.inner):
            sender = self.at.along_y(-y_step)
            for slot in range(self.at.outer):
                source = self.at.along_z(-slot - 1)
                self.y_copy(y_step, slot, source, sender).wait_recv()
                self.y_copy(y_step, slot, source, self.at.y).wait_send()


def gather_scratch(copies, array):
    outer, inner = split_copies(copies)
    return [
        pltpu.VMEM(array.shape, BF16),
        pltpu.SemaphoreType.DMA((2, outer - 1)),
        pltpu.SemaphoreType.DMA((2, inner - 1, outer)),
    ]


def widen(source, target, outer):
    def one(z):
        for y in range(source.shape[1]):
            target[z, y] = source[z, y].astype(F32)

    each(outer, one)


def spread(index, chunks, copies, steps):
    outer = split_copies(copies)[0]
    turns = -(-outer // chunks)

    def turn(sub):
        for step in steps:
            step(index * turns + sub)

    each(turns, turn)


def row_sum_scratch(count, rows, chunk, width):
    far, chunks = max(count // 2 - 1, 1), rows // chunk
    wide = pltpu.VMEM((far, chunks, chunk, width), BF16)
    slim = pltpu.VMEM((chunks, chunk, width), BF16)
    return [
        wide, wide, wide, wide, slim, slim,
        pltpu.SemaphoreType.DMA((2, far, chunks)),
        pltpu.SemaphoreType.DMA((2, far, chunks)),
        pltpu.SemaphoreType.DMA((2, chunks)),
    ]


def rows_at(index, chunk):
    return pl.ds(pl.multiple_of(index * chunk, chunk), chunk)


def standardize(values):
    average = jnp.mean(values, axis=-1, keepdims=True)
    centered = values - average
    spread = lax.rsqrt(jnp.mean(centered * centered, axis=-1, keepdims=True) + EPSILON)
    return centered * spread, spread


def norm_backward(values, grad, gain):
    normed, spread = standardize(values)
    scaled = grad * gain
    inner = jnp.mean(scaled * normed, axis=-1, keepdims=True)
    back = (scaled - jnp.mean(scaled, axis=-1, keepdims=True) - normed * inner) * spread
    return back, grad * normed


def column_sum(values):
    return jnp.sum(values, axis=0, keepdims=True)


def open_kernel(count, chunk, x_ref, gain_ref, shift_ref, first_ref, rows_ref, all_ref, *sems):
    rows = x_ref.shape[0]
    place, _, _ = mesh_place(count)
    greet(count)
    chunks = rows // chunk
    main = Gather(count, rows_ref, chunk, *sems[:3])
    side_chunk = first_ref.shape[0] // 2
    side = Gather(count, all_ref, side_chunk, *sems[3:])

    def start(index):
        values = x_ref[rows_at(index, chunk), :].astype(F32)
        normed = standardize(values)[0] * gain_ref[...] + shift_ref[...]
        rows_ref[place, rows_at(index, chunk), :] = normed.astype(BF16)
        main.send(index)

    each(chunks, start)

    def side_start(index):
        all_ref[place, rows_at(index, side_chunk), :] = first_ref[rows_at(index, side_chunk), :]
        side.send(index)

    each(2, side_start)
    each(chunks, main.hand_on)
    each(2, side.hand_on)
    each(chunks, main.finish)
    each(2, side.finish)


def attend_out_kernel(
    count, chunk, left, weight, x_ref, bias_ref, gain_ref, shift_ref, rows_ref, residual_ref, *scratch
):
    rows = x_ref.shape[0]
    place, _, _ = mesh_place(count)
    greet(count)
    chunks = rows // chunk
    summed = RowSum(count, rows, chunk, left, weight, False, scratch[:9])
    main = Gather(count, rows_ref, chunk, *scratch[9:])
    summed.send()

    def close(index):
        at = rows_at(index, chunk)
        values = x_ref[at, :].astype(F32) + summed.total(index) + bias_ref[...]
        residual_ref[at, :] = values
        normed = standardize(values)[0] * gain_ref[...] + shift_ref[...]
        rows_ref[place, at, :] = normed.astype(BF16)
        main.send(index)

    each(chunks, close)
    each(chunks, main.hand_on)
    each(chunks, main.finish)
    each(chunks, summed.finish)


def mlp_back_kernel(
    count, copies, chunk, left, weight, residual_ref, dy_ref, gain_ref, up_ref, down_ref,
    rows_ref, grad_ref, sums_ref, up_slab, down_slab, *scratch
):
    rows = residual_ref.shape[0]
    place, _, _ = mesh_place(count)
    greet(count, copies)
    chunks = rows // chunk
    summed = RowSum(count, rows, chunk, left, weight, True, scratch[:9])
    main = Gather(count, rows_ref, chunk, *scratch[9:12])
    up = DpReduce(copies, up_ref, *scratch[12:17])
    down = DpReduce(copies, down_ref, *scratch[17:22])
    down.send()
    up.send()
    sums_ref[...] = jnp.zeros_like(sums_ref)
    summed.send()

    def close(index):
        at = rows_at(index, chunk)
        total = summed.total(index)
        dy = dy_ref[at, :].astype(F32)
        back, per_gain = norm_backward(residual_ref[at, :], total, gain_ref[...])
        grad = dy + back
        grad_ref[at, :] = grad
        rows_ref[place, at, :] = grad.astype(BF16)
        main.send(index)
        sums_ref[0:1, :] += column_sum(per_gain)
        sums_ref[1:2, :] += column_sum(total)
        sums_ref[2:3, :] += column_sum(grad)
        sums_ref[3:4, :] += column_sum(dy)
        spread(index, chunks, copies, [down.pass_on])

    def hand_on(index):
        main.hand_on(index)
        spread(index, chunks, copies, [up.pass_on])

    each(chunks, close)
    each(chunks, hand_on)
    down_slab[...] = down.total().astype(BF16)
    each(chunks, main.finish)
    each(chunks, summed.finish)
    up_slab[...] = up.total().astype(BF16)


def input_back_kernel(
    count, copies, chunk, left, weight, x_ref, grad_ref, gain_ref, skip_ref, up_slab, down_slab, qkv_ref, outw_ref,
    out_ref, all_ref, sums_ref, up_ref, down_ref, qkv_slab, outw_slab, *scratch
):
    rows = x_ref.shape[0]
    place, _, _ = mesh_place(count)
    greet(count, copies)
    chunks = rows // chunk
    summed = RowSum(count, rows, chunk, left, weight, True, scratch[:9])
    side_chunk = skip_ref.shape[0] // 2
    side = Gather(count, all_ref, side_chunk, *scratch[9:12])
    outw = DpReduce(copies, outw_ref, *scratch[12:17])
    qkv = DpReduce(copies, qkv_ref, *scratch[17:22])
    up = DpGather(copies, up_slab, *scratch[22:25])
    down = DpGather(copies, down_slab, *scratch[25:28])
    qkv.send()
    outw.send()
    down.send()
    up.send()
    sums_ref[...] = jnp.zeros_like(sums_ref)
    summed.send()

    def side_start(index):
        all_ref[place, rows_at(index, side_chunk), :] = skip_ref[rows_at(index, side_chunk), :]
        side.send(index)

    each(2, side_start)

    def close(index):
        at = rows_at(index, chunk)
        total = summed.total(index)
        back, per_gain = norm_backward(x_ref[at, :].astype(F32), total, gain_ref[...])
        out_ref[at, :] = (grad_ref[at, :] + back).astype(BF16)
        sums_ref[0:1, :] += column_sum(per_gain)
        sums_ref[1:2, :] += column_sum(total)
        spread(index, chunks, copies, [qkv.pass_on, outw.pass_on, down.pass_on, up.pass_on])

    each(chunks, close)
    each(2, side.hand_on)
    qkv_slab[...] = qkv.total().astype(BF16)
    outw_slab[...] = outw.total().astype(BF16)
    down.finish()
    widen(down.held, down_ref, down.at.outer)
    each(2, side.finish)
    each(chunks, summed.finish)
    up.finish()
    widen(up.held, up_ref, up.at.outer)


def mlp_out_kernel(
    count, copies, chunk, shared, left, weight, residual_ref, bias_ref, small_ref, qkv_slab, outw_slab,
    out_ref, small_out, qkv_ref, outw_ref, *scratch
):
    rows = residual_ref.shape[0]
    copy, place = lax.axis_index("dp"), lax.axis_index("mp")
    barrier = pltpu.get_barrier_semaphore()
    for step in range(1, copies):
        pl.semaphore_signal(
            barrier, inc=1, device_id={"dp": lax.rem(copy + step, copies)}, device_id_type=pl.DeviceIdType.MESH
        )
    for step in range(1, count):
        pl.semaphore_signal(
            barrier, inc=1, device_id={"mp": lax.rem(place + step, count)}, device_id_type=pl.DeviceIdType.MESH
        )
    pl.semaphore_wait(barrier, copies + count - 2)
    chunks = rows // chunk
    summed = RowSum(count, rows, chunk, left, weight, False, scratch[:9])
    qkv = DpGather(copies, qkv_slab, *scratch[9:12])
    outw = DpGather(copies, outw_slab, *scratch[12:15])
    copy_in, part_in, part_out, copy_sems, part_sems = scratch[15:]

    def small_copy(axis, own, size, source, slots, sems, step, slot):
        return pltpu.make_async_remote_copy(
            src_ref=source, dst_ref=slots.at[slot], send_sem=sems.at[0, step], recv_sem=sems.at[1, slot],
            device_id={axis: lax.rem(own + step, size)}, device_id_type=pl.DeviceIdType.MESH,
        )

    def small_start(axis, own, size, source, slots, sems):
        slots[own] = source[...]
        for step in range(1, size):
            small_copy(axis, own, size, source, slots, sems, step, own).start()

    def small_total(axis, own, size, source, slots, sems):
        for step in range(1, size):
            slot = lax.rem(own + size - step, size)
            small_copy(axis, own, size, source, slots, sems, step, slot).wait_recv()
            small_copy(axis, own, size, source, slots, sems, step, own).wait_send()
        total = slots[0]
        for slot in range(1, size):
            total = total + slots[slot]
        return total

    over_copies = ("dp", copy, copies, small_ref, copy_in, copy_sems)
    over_parts = ("mp", place, count, part_out, part_in, part_sems)
    small_start(*over_copies)
    qkv.send()
    outw.send()
    summed.send()
    part_out[...] = small_total(*over_copies)
    small_start(*over_parts)

    def close(index):
        at = rows_at(index, chunk)
        out_ref[at, :] = (residual_ref[at, :] + summed.total(index) + bias_ref[...]).astype(BF16)
        spread(index, chunks, copies, [qkv.pass_on, outw.pass_on])

    each(chunks, close)
    every = small_total(*over_parts)
    row = lax.broadcasted_iota(jnp.int32, every.shape, 0)
    small_out[...] = jnp.where(row < shared, every, part_out[...])
    qkv.finish()
    widen(qkv.held, qkv_ref, qkv.at.outer)
    outw.finish()
    widen(outw.held, outw_ref, outw.at.outer)
    each(chunks, summed.finish)


def call(kernel, name, number, inputs, outputs, scratch, flops):
    moved = sum(a.size * a.dtype.itemsize for a in (*inputs, *outputs))
    return pl.pallas_call(
        kernel,
        out_shape=outputs,
        in_specs=[pl.BlockSpec(memory_space=pltpu.VMEM)] * len(inputs),
        out_specs=[pl.BlockSpec(memory_space=pltpu.VMEM)] * len(outputs),
        scratch_shapes=scratch,
        compiler_params=pltpu.CompilerParams(collective_id=number, has_side_effects=True),
        cost_estimate=pl.CostEstimate(flops=flops, bytes_accessed=moved, transcendentals=0),
        name=name,
    )(*inputs)


def like(shape, kind):
    return jax.ShapeDtypeStruct(shape, kind)


def body(
    inputs,
    first_values,
    cotangent,
    seq_lengths,
    value_owner,
    attn_norm_gain,
    attn_norm_bias,
    qkv_weight,
    qv_bias,
    out_weight,
    out_bias,
    mlp_norm_gain,
    mlp_norm_bias,
    up_weight,
    up_bias,
    down_weight,
    down_bias,
):
    local_rows, model_width = inputs.shape
    group_rows = local_rows * lax.axis_size("mp")
    pairs_dev, head_size = qkv_weight.shape[1], qkv_weight.shape[3]
    all_pairs = value_owner.shape[0]
    seats = (seq_lengths, value_owner, lax.axis_index("mp").reshape(1).astype(jnp.int32))
    copies = lax.axis_size("dp")

    qkv_pack = jnp.pad(qkv_weight, ((0, 0), (0, 0), (0, 1), (0, 0)))
    qkv_pack = qkv_pack.reshape(model_width, pairs_dev * PACK * head_size)
    bias_pack = jnp.concatenate(
        [qv_bias[:, 0:2], jnp.zeros_like(qv_bias[:, 0:2]), qv_bias[:, 2:3], jnp.zeros_like(qv_bias[:, 2:3])],
        axis=1,
    ).reshape(1, pairs_dev * PACK * head_size)
    out_flat = out_weight.reshape(pairs_dev * 2 * head_size, model_width)

    count = lax.axis_size("mp")
    chunk = min(128, local_rows)
    chunks = local_rows // chunk
    row = (1, model_width)
    whole = (count, local_rows, model_width)
    slim = pairs_dev * head_size
    sum_scratch = row_sum_scratch(count, local_rows, chunk, model_width)
    main_sems, side_sems = gather_sems(count, chunks), gather_sems(count, 2)
    dense = 2 * group_rows * model_width

    rows_one, all_first = call(
        functools.partial(open_kernel, count, chunk), "open_rows", 0,
        (inputs, attn_norm_gain.reshape(row), attn_norm_bias.reshape(row), first_values.reshape(group_rows, slim)),
        [like(whole, BF16), like((count, group_rows, slim), BF16)],
        main_sems + side_sems, dense * 100,
    )
    rows_one = rows_one.reshape(group_rows, model_width)
    packed = (product(rows_one, qkv_pack) + bias_pack).astype(BF16)
    cotangent_late = lax.optimization_barrier((cotangent, rows_one))[0]
    with jax.named_scope("gradrows"):
        grad_rows = lax.all_gather(cotangent_late, "mp", axis=0, tiled=True)
    mixed, totals = attend_forward(*seats, packed, all_first)
    rows_two, residual = call(
        functools.partial(attend_out_kernel, count, chunk), "attend_out", 1,
        (mixed, out_flat, inputs, out_bias.reshape(row), mlp_norm_gain.reshape(row), mlp_norm_bias.reshape(row)),
        [like(whole, BF16), like(inputs.shape, F32)],
        sum_scratch + main_sems, dense * 256,
    )
    rows_two = rows_two.reshape(group_rows, model_width)
    hidden_pre = product(rows_two, up_weight) + up_bias
    hidden = gelu_tanh(hidden_pre).astype(BF16)
    grad_hidden = back_product(grad_rows, down_weight)
    grad_pre = jax.vjp(gelu_tanh, hidden_pre)[1](grad_hidden)[0].astype(BF16)
    grad_down_weight = rows_product(hidden, grad_rows).astype(BF16)
    grad_up_weight = rows_product(rows_two, grad_pre).astype(BF16)
    grad_up_bias = jnp.sum(grad_pre.astype(F32), axis=0)
    outer, inner = split_copies(copies)

    def sliced(values):
        return values.reshape(outer, inner, values.shape[0] // copies, values.shape[1])

    grad_up_weight, grad_down_weight = sliced(grad_up_weight), sliced(grad_down_weight)
    up_slab, down_slab = (like(part.shape[2:], BF16) for part in (grad_up_weight, grad_down_weight))
    resid_rows, grad_residual, sums_two, up_slab, down_slab = call(
        functools.partial(mlp_back_kernel, count, copies, chunk), "mlp_back", 2,
        (grad_pre, up_weight, residual, cotangent, mlp_norm_gain.reshape(row), grad_up_weight, grad_down_weight),
        [like(whole, BF16), like(inputs.shape, F32), like((8, model_width), F32), up_slab, down_slab],
        sum_scratch + main_sems + reduce_scratch(copies, grad_up_weight) + reduce_scratch(copies, grad_down_weight),
        dense * up_bias.shape[0],
    )
    resid_rows = resid_rows.reshape(group_rows, model_width)
    grad_mixed = back_product(resid_rows, out_flat).astype(BF16)
    grad_out_weight = rows_product(mixed, resid_rows).astype(BF16)
    grad_flat = attend_backward(*seats, packed, all_first, grad_mixed, totals)
    grad_pack = grad_flat.reshape(group_rows, pairs_dev, PACK, head_size)
    pack_sums = jnp.sum(grad_flat.astype(F32), axis=0).reshape(pairs_dev, PACK, head_size)
    grad_qv_bias = jnp.concatenate([pack_sums[:, 0:2], pack_sums[:, 4:5]], axis=1)
    grad_qkv_weight = sliced(rows_product(rows_one, grad_flat).astype(BF16))
    grad_out_weight = sliced(grad_out_weight)
    grad_inputs, every_skip, sums_one, up_sum, down_sum, qkv_slab, out_slab = call(
        functools.partial(input_back_kernel, count, copies, chunk), "input_back", 3,
        (grad_flat, qkv_pack, inputs, grad_residual, attn_norm_gain.reshape(row),
         grad_pack[:, :, 5].reshape(group_rows, slim), up_slab, down_slab, grad_qkv_weight, grad_out_weight),
        [like(inputs.shape, BF16), like((count, group_rows, slim), BF16), like((8, model_width), F32),
         like(grad_up_weight.shape, F32), like(grad_down_weight.shape, F32),
         like(grad_qkv_weight.shape[2:], BF16), like(grad_out_weight.shape[2:], BF16)],
        sum_scratch + side_sems + reduce_scratch(copies, grad_out_weight) + reduce_scratch(copies, grad_qkv_weight)
        + gather_scratch(copies, grad_up_weight) + gather_scratch(copies, grad_down_weight),
        dense * pairs_dev * PACK * head_size,
    )
    wide_bias = jnp.pad(grad_up_bias, (0, model_width - grad_up_bias.shape[0])).reshape(row)
    slim_bias = jnp.pad(grad_qv_bias.reshape(-1), (0, model_width - grad_qv_bias.size)).reshape(row)
    own_sums = jnp.concatenate([sums_two[0:4], sums_one[0:2], wide_bias, slim_bias], axis=0)
    block = pltpu.VMEM(own_sums.shape, F32)
    output, small, qkv_sum, out_sum = call(
        functools.partial(mlp_out_kernel, count, copies, chunk, 6), "mlp_out", 4,
        (hidden, down_weight, residual, down_bias.reshape(row), own_sums, qkv_slab, out_slab),
        [like(inputs.shape, BF16), like(own_sums.shape, F32),
         like(grad_qkv_weight.shape, F32), like(grad_out_weight.shape, F32)],
        sum_scratch + gather_scratch(copies, grad_qkv_weight) + gather_scratch(copies, grad_out_weight)
        + [pltpu.VMEM((copies, *own_sums.shape), F32), pltpu.VMEM((count, *own_sums.shape), F32), block,
           pltpu.SemaphoreType.DMA((2, copies)), pltpu.SemaphoreType.DMA((2, count))],
        dense * up_bias.shape[0],
    )
    qkv_sum = qkv_sum.reshape(model_width, pairs_dev, PACK, head_size)[:, :, 0:5]
    late_sums = (up_sum.reshape(up_weight.shape), down_sum.reshape(down_weight.shape), out_sum.reshape(out_weight.shape))
    owned = lax.axis_index("mp") * pairs_dev + jnp.arange(pairs_dev, dtype=jnp.int32)
    every_pair = jnp.arange(all_pairs, dtype=jnp.int32)
    inverse = jnp.sum(
        jnp.where(value_owner[None, :] == owned[:, None], every_pair[None, :], 0), axis=1
    )
    every_skip = every_skip.reshape(count, group_rows, pairs_dev, head_size)
    grad_first = jnp.stack(
        [every_skip[inverse[p] // pairs_dev, :, inverse[p] % pairs_dev] for p in range(pairs_dev)], axis=1
    )
    norm_sums = (small[4], small[5], small[2], small[0], small[1], small[3])
    bias_sums = (small[7, : grad_qv_bias.size].reshape(qv_bias.shape), small[6, : grad_up_bias.shape[0]])

    return (
        output,
        grad_inputs,
        grad_first,
        norm_sums[0],
        norm_sums[1],
        qkv_sum,
        bias_sums[0],
        late_sums[2],
        norm_sums[2],
        norm_sums[3],
        norm_sums[4],
        late_sums[0],
        bias_sums[1],
        late_sums[1],
        norm_sums[5],
    )


def solution(mesh):
    return jax.shard_map(
        body,
        mesh=mesh,
        in_specs=(
            P(("dp", "mp"), None),
            P("dp", "mp", None),
            P(("dp", "mp"), None),
            P("dp"),
            P(),
            P(),
            P(),
            P(None, "mp", None, None),
            P("mp", None, None),
            P("mp", None, None, None),
            P(),
            P(),
            P(),
            P(None, "mp"),
            P("mp"),
            P("mp", None),
            P(),
        ),
        out_specs=(
            P(("dp", "mp"), None),
            P(("dp", "mp"), None),
            P("dp", "mp", None),
            P(),
            P(),
            P(None, "mp", None, None),
            P("mp", None, None),
            P("mp", None, None, None),
            P(),
            P(),
            P(),
            P(None, "mp"),
            P("mp"),
            P("mp", None),
            P(),
        ),
        check_vma=False,
    )
```

```python
import functools

import jax
import jax.numpy as jnp
from jax import lax
from jax.experimental import pallas as pl
from jax.experimental.pallas import tpu as pltpu
from jax.sharding import PartitionSpec as P


SHORT = 512
QROWS = 256
LANES = 128
PACK = 6

EPSILON = 1e-05
MASKED = -1e30
GELU_C = 0.7978845608028654
BF16 = jnp.bfloat16
F32 = jnp.float32


def gelu_tanh(values):
    return 0.5 * values * (1.0 + jnp.tanh(GELU_C * (values + 0.044715 * values * values * values)))


def rows_product(left, right):
    return lax.dot_general(left, right, (((0,), (0,)), ((), ())), preferred_element_type=F32)


def back_product(left, weight):
    return lax.dot_general(left, weight, (((1,), (1,)), ((), ())), preferred_element_type=F32)


def product(left, right):
    return jnp.dot(left, right, preferred_element_type=F32)


def opens_at(lengths, row):
    begin, opens = jnp.int32(0), jnp.int32(0)
    for slot in range(lengths.shape[0]):
        opens = jnp.maximum(opens, jnp.where(begin == row, 1, 0))
        begin = begin + lengths[slot]
    return opens


def head_lanes(head):
    lane = lax.broadcasted_iota(jnp.int32, (1, LANES), 1)
    return (lane < LANES // 2) if head == 0 else (lane >= LANES // 2)


def causal_tile():
    row = lax.broadcasted_iota(jnp.int32, (QROWS, QROWS), 0)
    column = lax.broadcasted_iota(jnp.int32, (QROWS, QROWS), 1)
    return column <= row


def pick_values(half, qkv_ref, first_ref, value_ref):
    held = first_ref[0]
    if held.shape[1] < LANES:
        turned = jnp.concatenate([held, held], axis=1)
    else:
        turned = jnp.concatenate([held[:, LANES // 2 :], held[:, : LANES // 2]], axis=1)
        turned = jnp.where(half == 1, held, turned)
    value_ref[...] = jnp.where(head_lanes(0), qkv_ref[:, 2 * LANES : 3 * LANES], turned)


def attend_forward_kernel(pairs, lengths, owner, place, qkv_ref, first_ref, mixed_ref, totals_ref, value_ref):
    pick_values(lax.rem(owner[place[0] * pairs + pl.program_id(0)], pairs), qkv_ref, first_ref, value_ref)
    blocks = qkv_ref.shape[0] // SHORT
    scale = (LANES // 2) ** (-0.5)

    def block(index, carried):
        base = pl.multiple_of(index * SHORT, SHORT)
        for half in range(SHORT // QROWS):
            first = base + half * QROWS

            def attend(with_previous):
                query = qkv_ref[pl.ds(first, QROWS), 0:LANES] * jnp.asarray(scale, BF16)
                spans = []
                if with_previous:
                    spans.append((base - SHORT, SHORT))
                if half:
                    spans.append((base, half * QROWS))
                spans.append((first, QROWS))
                mixed = jnp.zeros((QROWS, LANES), F32)
                totals = []
                for head in range(2):
                    chosen = head_lanes(head)
                    query_head = jnp.where(chosen, query, jnp.zeros_like(query))
                    scores = [
                        back_product(query_head, qkv_ref[pl.ds(at, size), LANES : 2 * LANES])
                        for at, size in spans
                    ]
                    scores[-1] = jnp.where(causal_tile(), scores[-1], MASKED)
                    top = scores[0].max(axis=1, keepdims=True)
                    for part in scores[1:]:
                        top = jnp.maximum(top, part.max(axis=1, keepdims=True))
                    total = jnp.zeros((QROWS, 1), F32)
                    gathered = jnp.zeros((QROWS, LANES), F32)
                    for (at, size), part in zip(spans, scores):
                        weights = jnp.exp(part - top)
                        total = total + weights.sum(axis=1, keepdims=True)
                        values = value_ref[pl.ds(at, size), :]
                        values = jnp.where(chosen, values, jnp.zeros_like(values))
                        gathered = gathered + product(weights.astype(BF16), values)
                    mixed = mixed + gathered / total
                    totals.append(top + jnp.log(total))
                mixed_ref[pl.ds(first, QROWS), :] = mixed.astype(BF16)
                totals_ref[pl.ds(first, QROWS), :] = jnp.where(
                    head_lanes(0), totals[0], totals[1]
                )

            @pl.when(opens_at(lengths, base) == 0)
            def _():
                attend(True)

            @pl.when(opens_at(lengths, base) == 1)
            def _():
                attend(False)

        return carried

    lax.fori_loop(0, blocks, block, 0)


def attend_backward_kernel(
    pairs, lengths, owner, place, qkv_ref, first_ref, grad_ref, totals_ref, out_ref, key_sum, value_sum, value_ref
):
    pick_values(lax.rem(owner[place[0] * pairs + pl.program_id(0)], pairs), qkv_ref, first_ref, value_ref)
    blocks = qkv_ref.shape[0] // SHORT
    scale = (LANES // 2) ** (-0.5)
    key_sum[...] = jnp.zeros_like(key_sum)
    value_sum[...] = jnp.zeros_like(value_sum)

    def block(index, carried):
        base = pl.multiple_of(index * SHORT, SHORT)
        for half in range(SHORT // QROWS):
            first = base + half * QROWS

            def attend(with_previous):
                query = qkv_ref[pl.ds(first, QROWS), 0:LANES] * jnp.asarray(scale, BF16)
                grad = grad_ref[pl.ds(first, QROWS), :]
                spans = []
                if with_previous:
                    spans.append((base - SHORT, SHORT))
                if half:
                    spans.append((base, half * QROWS))
                spans.append((first, QROWS))
                grad_query = jnp.zeros((QROWS, LANES), F32)
                for head in range(2):
                    chosen = head_lanes(head)
                    query_head = jnp.where(chosen, query, jnp.zeros_like(query))
                    grad_head = jnp.where(chosen, grad, jnp.zeros_like(grad))
                    at_lane = head * (LANES // 2)
                    totals = totals_ref[pl.ds(first, QROWS), at_lane : at_lane + 1]
                    probs, grads = [], []
                    inner = jnp.zeros((QROWS, 1), F32)
                    for at, size in spans:
                        keys = qkv_ref[pl.ds(at, size), LANES : 2 * LANES]
                        part = jnp.exp(back_product(query_head, keys) - totals)
                        if at is first:
                            part = jnp.where(causal_tile(), part, 0.0)
                        values = value_ref[pl.ds(at, size), :]
                        weighted = part * back_product(grad_head, values)
                        inner = inner + weighted.sum(axis=1, keepdims=True)
                        probs.append(part)
                        grads.append(weighted)
                    for (at, size), part, weighted in zip(spans, probs, grads):
                        keys = qkv_ref[pl.ds(at, size), LANES : 2 * LANES]
                        keys = jnp.where(chosen, keys, jnp.zeros_like(keys))
                        grad_scores = (weighted - part * inner).astype(BF16)
                        grad_query = grad_query + product(grad_scores, keys)
                        key_sum[pl.ds(at, size), :] += rows_product(grad_scores, query_head)
                        value_sum[pl.ds(at, size), :] += rows_product(part.astype(BF16), grad_head)
                out_ref[pl.ds(first, QROWS), 0:LANES] = (grad_query * scale).astype(BF16)

            @pl.when(opens_at(lengths, base) == 0)
            def _():
                attend(True)

            @pl.when(opens_at(lengths, base) == 1)
            def _():
                attend(False)

        return carried

    lax.fori_loop(0, blocks, block, 0)
    out_ref[:, LANES : 2 * LANES] = key_sum[...].astype(BF16)
    out_ref[:, 2 * LANES : 3 * LANES] = value_sum[...].astype(BF16)


def attend_forward(lengths, owner, place, packed, firsts):
    rows, pairs = packed.shape[0], packed.shape[1] // (3 * LANES)
    return pl.pallas_call(
        functools.partial(attend_forward_kernel, pairs),
        grid_spec=pltpu.PrefetchScalarGridSpec(
            num_scalar_prefetch=3,
            grid=(pairs,),
            in_specs=[
                pl.BlockSpec((rows, 3 * LANES), lambda p, c, o, m: (0, p)),
                pl.BlockSpec((1, rows, firsts.shape[2]), lambda p, c, o, m: (lax.div(o[m[0] * pairs + p], pairs), 0, 0)),
            ],
            out_specs=[
                pl.BlockSpec((rows, LANES), lambda p, c, o, m: (0, p)),
                pl.BlockSpec((rows, LANES), lambda p, c, o, m: (0, p)),
            ],
            scratch_shapes=[pltpu.VMEM((rows, LANES), BF16)],
        ),
        out_shape=[
            jax.ShapeDtypeStruct((rows, pairs * LANES), BF16),
            jax.ShapeDtypeStruct((rows, pairs * LANES), F32),
        ],
        cost_estimate=pl.CostEstimate(
            flops=rows * 1024 * 256 * 4 * pairs, bytes_accessed=8 << 20, transcendentals=rows * 2048
        ),
        name="attend_forward",
    )(lengths, owner, place, packed, firsts)


def attend_backward(lengths, owner, place, packed, firsts, grad, totals):
    rows, pairs = packed.shape[0], packed.shape[1] // (3 * LANES)
    return pl.pallas_call(
        functools.partial(attend_backward_kernel, pairs),
        grid_spec=pltpu.PrefetchScalarGridSpec(
            num_scalar_prefetch=3,
            grid=(pairs,),
            in_specs=[
                pl.BlockSpec((rows, 3 * LANES), lambda p, c, o, m: (0, p)),
                pl.BlockSpec((1, rows, firsts.shape[2]), lambda p, c, o, m: (lax.div(o[m[0] * pairs + p], pairs), 0, 0)),
                pl.BlockSpec((rows, LANES), lambda p, c, o, m: (0, p)),
                pl.BlockSpec((rows, LANES), lambda p, c, o, m: (0, p)),
            ],
            out_specs=pl.BlockSpec((rows, 3 * LANES), lambda p, c, o, m: (0, p)),
            scratch_shapes=[
                pltpu.VMEM((rows, LANES), F32),
                pltpu.VMEM((rows, LANES), F32),
                pltpu.VMEM((rows, LANES), BF16),
            ],
        ),
        out_shape=jax.ShapeDtypeStruct((rows, pairs * 3 * LANES), BF16),
        cost_estimate=pl.CostEstimate(
            flops=rows * 1024 * 256 * 10 * pairs, bytes_accessed=8 << 20, transcendentals=rows * 2048
        ),
        name="attend_backward",
    )(lengths, owner, place, packed, firsts, grad, totals)


def mesh_place(count):
    place = lax.axis_index("mp")
    core = lax.rem(place, 2)
    chip = lax.div(place, 2)
    chips = count // 2

    def across(step, other):
        return lax.rem(chip + step + chips, chips) * 2 + (1 - core if other else core)

    return place, place + 1 - 2 * core, across


def remote(source, target, sems, index, device):
    return pltpu.make_async_remote_copy(
        src_ref=source,
        dst_ref=target,
        send_sem=sems.at[(0, *index)],
        recv_sem=sems.at[(1, *index)],
        device_id={"mp": device},
        device_id_type=pl.DeviceIdType.MESH,
    )


def greet(count, copies=0):
    _, partner, across = mesh_place(count)
    barrier = pltpu.get_barrier_semaphore()
    for device in [partner] + [across(step, False) for step in range(1, count // 2)]:
        pl.semaphore_signal(
            barrier, inc=1, device_id={"mp": device}, device_id_type=pl.DeviceIdType.MESH
        )
    others = DpPlace(copies).greet(barrier) if copies else 0
    pl.semaphore_wait(barrier, count // 2 + others)


def each(count, step):
    def run(index, carried):
        step(index)
        return carried

    lax.fori_loop(0, count, run, 0)


class Gather:
    def __init__(self, count, out_ref, chunk, near, far, passed):
        self.count, self.out, self.chunk = count, out_ref, chunk
        self.near, self.far, self.passed = near, far, passed
        self.place, self.partner, self.across = mesh_place(count)

    def part(self, owner, index):
        return self.out.at[owner, pl.ds(pl.multiple_of(index * self.chunk, self.chunk), self.chunk), :]

    def send(self, index):
        own = self.part(self.place, index)
        for step in range(1, self.count // 2):
            remote(own, own, self.far, (step - 1, index), self.across(step, False)).start()
        remote(own, own, self.near, (index,), self.partner).start()

    def hand_on(self, index):
        for step in range(1, self.count // 2):
            got = self.part(self.across(-step, False), index)
            remote(got, got, self.far, (step - 1, index), self.across(step, False)).wait_recv()
            remote(got, got, self.passed, (step - 1, index), self.partner).start()

    def finish(self, index):
        own = self.part(self.place, index)
        near = self.part(self.partner, index)
        remote(own, near, self.near, (index,), self.partner).wait()
        for step in range(1, self.count // 2):
            remote(own, own, self.far, (step - 1, index), self.across(step, False)).wait_send()
            got = self.part(self.across(-step, True), index)
            remote(got, got, self.passed, (step - 1, index), self.partner).wait()


def gather_sems(count, chunks):
    far = max(count // 2 - 1, 1)
    return [
        pltpu.SemaphoreType.DMA((2, chunks)),
        pltpu.SemaphoreType.DMA((2, far, chunks)),
        pltpu.SemaphoreType.DMA((2, far, chunks)),
    ]


class RowSum:
    def __init__(self, count, rows, chunk, left, weight, flipped, buffers):
        self.count, self.rows, self.chunk = count, rows, chunk
        self.left, self.weight, self.flipped = left, weight, flipped
        (self.pair_out, self.pair_in, self.far_out, self.far_in, self.near_out, self.near_in, self.own) = buffers[:7]
        self.pair, self.far, self.near = buffers[7:]
        self.place, self.partner, self.across = mesh_place(count)

    def product(self, owner, index):
        at = pl.multiple_of(owner * self.rows + index * self.chunk, self.chunk)
        rows = self.left[pl.ds(at, self.chunk), :]
        return (back_product if self.flipped else product)(rows, self.weight[...])

    def pair_copy(self, step, index):
        return remote(
            self.pair_out.at[step - 1, index], self.pair_in.at[step - 1, index],
            self.pair, (step - 1, index), self.partner,
        )

    def far_copy(self, step, index):
        return remote(
            self.far_out.at[step - 1, index], self.far_in.at[step - 1, index],
            self.far, (step - 1, index), self.across(step, False),
        )

    def near_copy(self, index):
        return remote(self.near_out.at[index], self.near_in.at[index], self.near, (index,), self.partner)

    def send(self):
        chunks, far = self.rows // self.chunk, self.count // 2 - 1
        core = lax.rem(self.place, 2)

        def turn(number):
            kind, index = lax.div(number, chunks), lax.rem(number, chunks)
            step = lax.rem(kind, max(far, 1)) + 1
            owner = lax.rem(lax.div(self.place, 2) + step, self.count // 2) * 2
            owner = owner + jnp.where(kind < far, 1 - core, core)
            owner = jnp.where(kind == 2 * far, self.partner, owner)
            owner = jnp.where(kind > 2 * far, self.place, owner)
            rows = self.product(owner, index)

            @pl.when(kind < far)
            def _():
                self.pair_out[step - 1, index] = rows.astype(BF16)
                self.pair_copy(step, index).start()

            @pl.when((kind >= far) & (kind < 2 * far))
            def _():
                self.pair_copy(step, index).wait_recv()
                self.far_out[step - 1, index] = (rows + self.pair_in[step - 1, index].astype(F32)).astype(BF16)
                self.far_copy(step, index).start()

            @pl.when(kind == 2 * far)
            def _():
                self.near_out[index] = rows.astype(BF16)
                self.near_copy(index).start()

            @pl.when(kind > 2 * far)
            def _():
                self.own[index] = rows

        each((2 * far + 2) * chunks, turn)

    def total(self, index):
        self.near_copy(index).wait_recv()
        rows = self.own[index] + self.near_in[index].astype(F32)
        for step in range(1, self.count // 2):
            self.far_copy(step, index).wait_recv()
            rows = rows + self.far_in[step - 1, index].astype(F32)
        return rows

    def finish(self, index):
        self.near_copy(index).wait_send()
        for step in range(1, self.count // 2):
            self.pair_copy(step, index).wait_send()
            self.far_copy(step, index).wait_send()


def split_copies(copies):
    inner = 1
    while (2 * inner) ** 2 <= copies:
        inner *= 2
    return copies // inner, inner


def dp_copy(source, target, send_sem, recv_sem, device):
    return pltpu.make_async_remote_copy(
        src_ref=source, dst_ref=target, send_sem=send_sem, recv_sem=recv_sem,
        device_id={"dp": device}, device_id_type=pl.DeviceIdType.MESH,
    )


class DpPlace:
    def __init__(self, copies):
        self.outer, self.inner = split_copies(copies)
        here = lax.axis_index("dp")
        self.z, self.y = lax.div(here, self.inner), lax.rem(here, self.inner)

    def along_y(self, step):
        return lax.rem(self.y + step + self.inner, self.inner)

    def along_z(self, step):
        return lax.rem(self.z + step + self.outer, self.outer)

    def device(self, z, y):
        return z * self.inner + y

    def greet(self, barrier):
        for step in range(1, self.inner):
            pl.semaphore_signal(
                barrier, inc=1, device_id={"dp": self.device(self.z, self.along_y(step))},
                device_id_type=pl.DeviceIdType.MESH,
            )
        for step in range(1, self.outer):
            pl.semaphore_signal(
                barrier, inc=1, device_id={"dp": self.device(self.along_z(step), self.y)},
                device_id_type=pl.DeviceIdType.MESH,
            )
        return self.inner + self.outer - 2


class DpReduce:
    def __init__(self, copies, source, y_in, z_out, z_in, y_sems, z_sems):
        self.at = DpPlace(copies)
        self.source, self.y_in, self.z_out, self.z_in = source, y_in, z_out, z_in
        self.y_sems, self.z_sems = y_sems, z_sems

    def y_copy(self, step, z):
        peer = self.at.along_y(step)
        return dp_copy(
            self.source.at[z, peer], self.y_in.at[step - 1, z],
            self.y_sems.at[0, step - 1, z], self.y_sems.at[1, step - 1, z], self.at.device(self.at.z, peer),
        )

    def z_copy(self, step):
        peer = self.at.along_z(step + 1)
        return dp_copy(
            self.z_out.at[step], self.z_in.at[step],
            self.z_sems.at[0, step], self.z_sems.at[1, step], self.at.device(peer, self.at.y),
        )

    def send(self):
        def start(step):
            for y_step in range(1, self.at.inner):
                self.y_copy(y_step, self.at.along_z(step + 1)).start()

        each(self.at.outer, start)

    def y_total(self, z):
        total = self.source[z, self.at.y].astype(F32)
        for y_step in range(1, self.at.inner):
            self.y_copy(y_step, z).wait_recv()
            total = total + self.y_in[y_step - 1, z].astype(F32)
        return total

    def pass_on(self, step):
        @pl.when(step < self.at.outer - 1)
        def _():
            self.z_out[step] = self.y_total(self.at.along_z(step + 1)).astype(BF16)
            self.z_copy(step).start()

    def total(self):
        total = self.y_total(self.at.z)
        for step in range(self.at.outer - 1):
            self.z_copy(step).wait_recv()
            total = total + self.z_in[step].astype(F32)
        for step in range(self.at.outer - 1):
            self.z_copy(step).wait_send()
        for y_step in range(1, self.at.inner):
            for z in range(self.at.outer):
                self.y_copy(y_step, z).wait_send()
        return total


def reduce_scratch(copies, array):
    outer, inner = split_copies(copies)
    slab = array.shape[2:]
    return [
        pltpu.VMEM((inner - 1, outer, *slab), BF16),
        pltpu.VMEM((outer - 1, *slab), BF16),
        pltpu.VMEM((outer - 1, *slab), BF16),
        pltpu.SemaphoreType.DMA((2, inner - 1, outer)),
        pltpu.SemaphoreType.DMA((2, outer - 1)),
    ]


class DpGather:
    def __init__(self, copies, slab, held, z_sems, y_sems):
        self.at = DpPlace(copies)
        self.slab, self.held, self.z_sems, self.y_sems = slab, held, z_sems, y_sems

    def z_copy(self, step, z):
        here = self.held.at[z, self.at.y]
        peer = self.at.device(self.at.along_z(step + 1), self.at.y)
        return dp_copy(here, here, self.z_sems.at[0, step], self.z_sems.at[1, step], peer)

    def y_copy(self, y_step, slot, z, y):
        here = self.held.at[z, y]
        peer = self.at.device(self.at.z, self.at.along_y(y_step))
        return dp_copy(
            here, here, self.y_sems.at[0, y_step - 1, slot], self.y_sems.at[1, y_step - 1, slot], peer
        )

    def send(self):
        self.held[self.at.z, self.at.y] = self.slab[...]
        for step in range(self.at.outer - 1):
            self.z_copy(step, self.at.z).start()
        for y_step in range(1, self.at.inner):
            self.y_copy(y_step, self.at.outer - 1, self.at.z, self.at.y).start()

    def pass_on(self, step):
        @pl.when(step < self.at.outer - 1)
        def _():
            source = self.at.along_z(-step - 1)
            self.z_copy(step, source).wait_recv()
            for y_step in range(1, self.at.inner):
                self.y_copy(y_step, step, source, self.at.y).start()

    def finish(self):
        for step in range(self.at.outer - 1):
            self.z_copy(step, self.at.z).wait_send()
        for y_step in range(1, self.at.inner):
            sender = self.at.along_y(-y_step)
            for slot in range(self.at.outer):
                source = self.at.along_z(-slot - 1)
                self.y_copy(y_step, slot, source, sender).wait_recv()
                self.y_copy(y_step, slot, source, self.at.y).wait_send()


def gather_scratch(copies):
    outer, inner = split_copies(copies)
    return [pltpu.SemaphoreType.DMA((2, outer - 1)), pltpu.SemaphoreType.DMA((2, inner - 1, outer))]


def spread(index, chunks, copies, steps):
    outer = split_copies(copies)[0]
    turns = -(-outer // chunks)

    def turn(sub):
        for step in steps:
            step(index * turns + sub)

    each(turns, turn)


def row_sum_scratch(count, rows, chunk, width):
    far, chunks = max(count // 2 - 1, 1), rows // chunk
    wide = pltpu.VMEM((far, chunks, chunk, width), BF16)
    slim = pltpu.VMEM((chunks, chunk, width), BF16)
    return [
        wide, wide, wide, wide, slim, slim, pltpu.VMEM((chunks, chunk, width), F32),
        pltpu.SemaphoreType.DMA((2, far, chunks)),
        pltpu.SemaphoreType.DMA((2, far, chunks)),
        pltpu.SemaphoreType.DMA((2, chunks)),
    ]


def rows_at(index, chunk):
    return pl.ds(pl.multiple_of(index * chunk, chunk), chunk)


def standardize(values):
    average = jnp.mean(values, axis=-1, keepdims=True)
    centered = values - average
    spread = lax.rsqrt(jnp.mean(centered * centered, axis=-1, keepdims=True) + EPSILON)
    return centered * spread, spread


def norm_backward(values, grad, gain):
    normed, spread = standardize(values)
    scaled = grad * gain
    inner = jnp.mean(scaled * normed, axis=-1, keepdims=True)
    back = (scaled - jnp.mean(scaled, axis=-1, keepdims=True) - normed * inner) * spread
    return back, grad * normed


def column_sum(values):
    return jnp.sum(values, axis=0, keepdims=True)


def open_kernel(count, chunk, x_ref, gain_ref, shift_ref, first_ref, rows_ref, all_ref, *sems):
    rows = x_ref.shape[0]
    place, _, _ = mesh_place(count)
    greet(count)
    chunks = rows // chunk
    main = Gather(count, rows_ref, chunk, *sems[:3])
    side_chunk = first_ref.shape[0] // 2
    side = Gather(count, all_ref, side_chunk, *sems[3:])

    def start(index):
        values = x_ref[rows_at(index, chunk), :].astype(F32)
        normed = standardize(values)[0] * gain_ref[...] + shift_ref[...]
        rows_ref[place, rows_at(index, chunk), :] = normed.astype(BF16)
        main.send(index)

    each(chunks, start)

    def side_start(index):
        all_ref[place, rows_at(index, side_chunk), :] = first_ref[rows_at(index, side_chunk), :]
        side.send(index)

    each(2, side_start)
    each(chunks, main.hand_on)
    each(2, side.hand_on)
    each(chunks, main.finish)
    each(2, side.finish)


def attend_out_kernel(
    count, chunk, left, weight, x_ref, bias_ref, gain_ref, shift_ref, rows_ref, residual_ref, *scratch
):
    rows = x_ref.shape[0]
    place, _, _ = mesh_place(count)
    greet(count)
    chunks = rows // chunk
    summed = RowSum(count, rows, chunk, left, weight, False, scratch[:10])
    main = Gather(count, rows_ref, chunk, *scratch[10:])
    summed.send()

    def close(index):
        at = rows_at(index, chunk)
        values = x_ref[at, :].astype(F32) + summed.total(index) + bias_ref[...]
        residual_ref[at, :] = values
        normed = standardize(values)[0] * gain_ref[...] + shift_ref[...]
        rows_ref[place, at, :] = normed.astype(BF16)
        main.send(index)

    each(chunks, close)
    each(chunks, main.hand_on)
    each(chunks, main.finish)
    each(chunks, summed.finish)


def mlp_back_kernel(
    count, chunk, left, weight, residual_ref, dy_ref, gain_ref, rows_ref, grad_ref, sums_ref, *scratch
):
    rows = residual_ref.shape[0]
    place, _, _ = mesh_place(count)
    greet(count)
    chunks = rows // chunk
    summed = RowSum(count, rows, chunk, left, weight, True, scratch[:10])
    main = Gather(count, rows_ref, chunk, *scratch[10:])
    sums_ref[...] = jnp.zeros_like(sums_ref)
    summed.send()

    def close(index):
        at = rows_at(index, chunk)
        total = summed.total(index)
        dy = dy_ref[at, :].astype(F32)
        back, per_gain = norm_backward(residual_ref[at, :], total, gain_ref[...])
        grad = dy + back
        grad_ref[at, :] = grad
        rows_ref[place, at, :] = grad.astype(BF16)
        main.send(index)
        sums_ref[0:1, :] += column_sum(per_gain)
        sums_ref[1:2, :] += column_sum(total)
        sums_ref[2:3, :] += column_sum(grad)
        sums_ref[3:4, :] += column_sum(dy)

    each(chunks, close)
    each(chunks, main.hand_on)
    each(chunks, main.finish)
    each(chunks, summed.finish)


def input_back_kernel(
    count, copies, chunk, left, weight, x_ref, grad_ref, gain_ref, skip_ref, qkv_ref, outw_ref,
    out_ref, all_ref, sums_ref, qkv_slab, outw_slab, *scratch
):
    rows = x_ref.shape[0]
    place, _, _ = mesh_place(count)
    greet(count, copies)
    chunks = rows // chunk
    summed = RowSum(count, rows, chunk, left, weight, True, scratch[:10])
    side_chunk = skip_ref.shape[0] // 2
    side = Gather(count, all_ref, side_chunk, *scratch[10:13])
    outw = DpReduce(copies, outw_ref, *scratch[13:18])
    qkv = DpReduce(copies, qkv_ref, *scratch[18:23])
    qkv.send()
    outw.send()
    sums_ref[...] = jnp.zeros_like(sums_ref)
    summed.send()

    def side_start(index):
        all_ref[place, rows_at(index, side_chunk), :] = skip_ref[rows_at(index, side_chunk), :]
        side.send(index)

    each(2, side_start)

    def close(index):
        at = rows_at(index, chunk)
        total = summed.total(index)
        back, per_gain = norm_backward(x_ref[at, :].astype(F32), total, gain_ref[...])
        out_ref[at, :] = (grad_ref[at, :] + back).astype(BF16)
        sums_ref[0:1, :] += column_sum(per_gain)
        sums_ref[1:2, :] += column_sum(total)
        spread(index, chunks, copies, [qkv.pass_on, outw.pass_on])

    each(chunks, close)
    each(2, side.hand_on)
    qkv_slab[...] = qkv.total().astype(BF16)
    outw_slab[...] = outw.total().astype(BF16)
    each(2, side.finish)
    each(chunks, summed.finish)


def mlp_out_kernel(
    count, copies, chunk, shared, left, weight, residual_ref, bias_ref, small_ref, qkv_slab, outw_slab,
    out_ref, small_out, qkv_ref, outw_ref, *scratch
):
    rows = residual_ref.shape[0]
    copy, place = lax.axis_index("dp"), lax.axis_index("mp")
    barrier = pltpu.get_barrier_semaphore()
    for step in range(1, copies):
        pl.semaphore_signal(
            barrier, inc=1, device_id={"dp": lax.rem(copy + step, copies)}, device_id_type=pl.DeviceIdType.MESH
        )
    for step in range(1, count):
        pl.semaphore_signal(
            barrier, inc=1, device_id={"mp": lax.rem(place + step, count)}, device_id_type=pl.DeviceIdType.MESH
        )
    pl.semaphore_wait(barrier, copies + count - 2)
    chunks = rows // chunk
    summed = RowSum(count, rows, chunk, left, weight, False, scratch[:10])
    qkv = DpGather(copies, qkv_slab, qkv_ref, *scratch[10:12])
    outw = DpGather(copies, outw_slab, outw_ref, *scratch[12:14])
    copy_in, part_in, part_out, copy_sems, part_sems = scratch[14:]

    def small_copy(axis, own, size, source, slots, sems, step, slot):
        return pltpu.make_async_remote_copy(
            src_ref=source, dst_ref=slots.at[slot], send_sem=sems.at[0, step], recv_sem=sems.at[1, slot],
            device_id={axis: lax.rem(own + step, size)}, device_id_type=pl.DeviceIdType.MESH,
        )

    def small_start(axis, own, size, source, slots, sems):
        slots[own] = source[...]
        for step in range(1, size):
            small_copy(axis, own, size, source, slots, sems, step, own).start()

    def small_total(axis, own, size, source, slots, sems):
        for step in range(1, size):
            slot = lax.rem(own + size - step, size)
            small_copy(axis, own, size, source, slots, sems, step, slot).wait_recv()
            small_copy(axis, own, size, source, slots, sems, step, own).wait_send()
        total = slots[0]
        for slot in range(1, size):
            total = total + slots[slot]
        return total

    over_copies = ("dp", copy, copies, small_ref, copy_in, copy_sems)
    over_parts = ("mp", place, count, part_out, part_in, part_sems)
    small_start(*over_copies)
    qkv.send()
    outw.send()
    summed.send()
    part_out[...] = small_total(*over_copies)
    small_start(*over_parts)

    def close(index):
        at = rows_at(index, chunk)
        out_ref[at, :] = (residual_ref[at, :] + summed.total(index) + bias_ref[...]).astype(BF16)
        spread(index, chunks, copies, [qkv.pass_on, outw.pass_on])

    each(chunks, close)
    every = small_total(*over_parts)
    row = lax.broadcasted_iota(jnp.int32, every.shape, 0)
    small_out[...] = jnp.where(row < shared, every, part_out[...])
    qkv.finish()
    outw.finish()
    each(chunks, summed.finish)


def user_of(owner, head):
    user = jnp.int32(0)
    for pair in range(owner.shape[0]):
        user = user + jnp.where(owner[pair] == head, pair, 0)
    return user


def pick_gradient(owner, place, every, pairs):
    _, rows, slim = every.shape
    width = slim // pairs

    def kernel(owner, place, *refs):
        for slot in range(pairs):
            held = refs[slot][0]
            user = lax.rem(user_of(owner, place[0] * pairs + slot), pairs)
            value = held[:, 0:width]
            for part in range(1, pairs):
                value = jnp.where(user == part, held[:, part * width : (part + 1) * width], value)
            refs[-1][:, slot * width : (slot + 1) * width] = value

    def block(slot):
        return pl.BlockSpec(
            (1, rows // 4, slim),
            lambda g, o, m: (lax.div(user_of(o, m[0] * pairs + slot), pairs), g, 0),
        )

    return pl.pallas_call(
        kernel,
        grid_spec=pltpu.PrefetchScalarGridSpec(
            num_scalar_prefetch=2,
            grid=(4,),
            in_specs=[block(slot) for slot in range(pairs)],
            out_specs=pl.BlockSpec((rows // 4, slim), lambda g, o, m: (g, 0)),
        ),
        out_shape=jax.ShapeDtypeStruct((rows, slim), BF16),
        name="pick_gradient",
    )(owner, place, *([every] * pairs))


def call(kernel, number, inputs, outputs, scratch, flops):
    moved = sum(a.size * a.dtype.itemsize for a in (*inputs, *outputs))
    return pl.pallas_call(
        kernel,
        out_shape=outputs,
        in_specs=[pl.BlockSpec(memory_space=pltpu.VMEM)] * len(inputs),
        out_specs=[pl.BlockSpec(memory_space=pltpu.VMEM)] * len(outputs),
        scratch_shapes=scratch,
        compiler_params=pltpu.CompilerParams(collective_id=number, has_side_effects=True),
        cost_estimate=pl.CostEstimate(flops=flops, bytes_accessed=moved, transcendentals=0),
    )(*inputs)


def like(shape, kind):
    return jax.ShapeDtypeStruct(shape, kind)


def body(
    inputs,
    first_values,
    cotangent,
    seq_lengths,
    value_owner,
    attn_norm_gain,
    attn_norm_bias,
    qkv_weight,
    qv_bias,
    out_weight,
    out_bias,
    mlp_norm_gain,
    mlp_norm_bias,
    up_weight,
    up_bias,
    down_weight,
    down_bias,
):
    local_rows, model_width = inputs.shape
    group_rows = local_rows * lax.axis_size("mp")
    pairs_dev, head_size = qkv_weight.shape[1], qkv_weight.shape[3]
    seats = (seq_lengths, value_owner, lax.axis_index("mp").reshape(1).astype(jnp.int32))
    copies = lax.axis_size("dp")

    qkv_pack = jnp.pad(qkv_weight, ((0, 0), (0, 0), (0, 1), (0, 0)))
    qkv_pack = qkv_pack.reshape(model_width, pairs_dev * PACK * head_size)
    bias_pack = jnp.concatenate(
        [qv_bias[:, 0:2], jnp.zeros_like(qv_bias[:, 0:2]), qv_bias[:, 2:3], jnp.zeros_like(qv_bias[:, 2:3])],
        axis=1,
    ).reshape(1, pairs_dev * PACK * head_size)
    out_flat = out_weight.reshape(pairs_dev * 2 * head_size, model_width)

    count = lax.axis_size("mp")
    chunk = min(128, local_rows)
    chunks = local_rows // chunk
    row = (1, model_width)
    whole = (count, local_rows, model_width)
    slim = pairs_dev * head_size
    sum_scratch = row_sum_scratch(count, local_rows, chunk, model_width)
    main_sems, side_sems = gather_sems(count, chunks), gather_sems(count, 2)
    dense = 2 * group_rows * model_width

    rows_one, all_first = call(
        functools.partial(open_kernel, count, chunk), 0,
        (inputs, attn_norm_gain.reshape(row), attn_norm_bias.reshape(row), first_values.reshape(group_rows, slim)),
        [like(whole, BF16), like((count, group_rows, slim), BF16)],
        main_sems + side_sems, dense * 100,
    )
    rows_one = rows_one.reshape(group_rows, model_width)
    packed = (product(rows_one, qkv_pack) + bias_pack).astype(BF16)
    cotangent_late = lax.optimization_barrier((cotangent, rows_one))[0]
    grad_rows = lax.all_gather(cotangent_late, "mp", axis=0, tiled=True)
    mixed, totals = attend_forward(*seats, packed, all_first)
    rows_two, residual = call(
        functools.partial(attend_out_kernel, count, chunk), 1,
        (mixed, out_flat, inputs, out_bias.reshape(row), mlp_norm_gain.reshape(row), mlp_norm_bias.reshape(row)),
        [like(whole, BF16), like(inputs.shape, F32)],
        sum_scratch + main_sems, dense * 256,
    )
    rows_two = rows_two.reshape(group_rows, model_width)
    hidden_pre = product(rows_two, up_weight) + up_bias
    hidden = gelu_tanh(hidden_pre).astype(BF16)
    grad_hidden = back_product(grad_rows, down_weight)
    grad_pre = jax.vjp(gelu_tanh, hidden_pre)[1](grad_hidden)[0].astype(BF16)
    grad_down_weight = rows_product(hidden, grad_rows).astype(BF16)
    grad_up_weight = rows_product(rows_two, grad_pre).astype(BF16)
    grad_up_bias = jnp.sum(grad_pre.astype(F32), axis=0)
    outer, inner = split_copies(copies)

    def sliced(values):
        return values.reshape(outer, inner, values.shape[0] // copies, values.shape[1])

    late = (grad_up_weight, grad_down_weight)
    grad_pre, late = lax.optimization_barrier((grad_pre, late))
    late_sums = lax.psum(late, "dp")
    resid_rows, grad_residual, sums_two = call(
        functools.partial(mlp_back_kernel, count, chunk), 2,
        (grad_pre, up_weight, residual, cotangent, mlp_norm_gain.reshape(row)),
        [like(whole, BF16), like(inputs.shape, F32), like((8, model_width), F32)],
        sum_scratch + main_sems, dense * up_bias.shape[0],
    )
    resid_rows = resid_rows.reshape(group_rows, model_width)
    grad_mixed = back_product(resid_rows, out_flat).astype(BF16)
    grad_out_weight = rows_product(mixed, resid_rows).astype(BF16)
    grad_flat = attend_backward(*seats, packed, all_first, grad_mixed, totals)
    grad_pack = grad_flat.reshape(group_rows, pairs_dev, PACK, head_size)
    pack_sums = jnp.sum(grad_flat.astype(F32), axis=0).reshape(pairs_dev, PACK, head_size)
    grad_qv_bias = jnp.concatenate([pack_sums[:, 0:2], pack_sums[:, 4:5]], axis=1)
    grad_qkv_weight = sliced(rows_product(rows_one, grad_flat).astype(BF16))
    grad_out_weight = sliced(grad_out_weight)
    grad_inputs, every_skip, sums_one, qkv_slab, out_slab = call(
        functools.partial(input_back_kernel, count, copies, chunk), 3,
        (grad_flat, qkv_pack, inputs, grad_residual, attn_norm_gain.reshape(row),
         grad_pack[:, :, 5].reshape(group_rows, slim), grad_qkv_weight, grad_out_weight),
        [like(inputs.shape, BF16), like((count, group_rows, slim), BF16), like((8, model_width), F32),
         like(grad_qkv_weight.shape[2:], BF16), like(grad_out_weight.shape[2:], BF16)],
        sum_scratch + side_sems + reduce_scratch(copies, grad_out_weight) + reduce_scratch(copies, grad_qkv_weight),
        dense * pairs_dev * PACK * head_size,
    )
    wide_bias = jnp.pad(grad_up_bias, (0, model_width - grad_up_bias.shape[0])).reshape(row)
    slim_bias = jnp.pad(grad_qv_bias.reshape(-1), (0, model_width - grad_qv_bias.size)).reshape(row)
    own_sums = jnp.concatenate([sums_two[0:4], sums_one[0:2], wide_bias, slim_bias], axis=0)
    block = pltpu.VMEM(own_sums.shape, F32)
    output, small, qkv_sum, out_sum = call(
        functools.partial(mlp_out_kernel, count, copies, chunk, 6), 4,
        (hidden, down_weight, residual, down_bias.reshape(row), own_sums, qkv_slab, out_slab),
        [like(inputs.shape, BF16), like(own_sums.shape, F32),
         like(grad_qkv_weight.shape, BF16), like(grad_out_weight.shape, BF16)],
        sum_scratch + gather_scratch(copies) + gather_scratch(copies)
        + [pltpu.VMEM((copies, *own_sums.shape), F32), pltpu.VMEM((count, *own_sums.shape), F32), block,
           pltpu.SemaphoreType.DMA((2, copies)), pltpu.SemaphoreType.DMA((2, count))],
        dense * up_bias.shape[0],
    )
    qkv_sum = qkv_sum.reshape(model_width, pairs_dev, PACK, head_size)[:, :, 0:5].astype(F32)
    late_sums = (*(part.astype(F32) for part in late_sums), out_sum.reshape(out_weight.shape).astype(F32))
    grad_first = pick_gradient(*seats[1:], every_skip, pairs_dev).reshape(group_rows, pairs_dev, head_size)
    norm_sums = (small[4], small[5], small[2], small[0], small[1], small[3])
    bias_sums = (small[7, : grad_qv_bias.size].reshape(qv_bias.shape), small[6, : grad_up_bias.shape[0]])

    return (
        output,
        grad_inputs,
        grad_first,
        norm_sums[0],
        norm_sums[1],
        qkv_sum,
        bias_sums[0],
        late_sums[2],
        norm_sums[2],
        norm_sums[3],
        norm_sums[4],
        late_sums[0],
        bias_sums[1],
        late_sums[1],
        norm_sums[5],
    )


def solution(mesh):
    return jax.shard_map(
        body,
        mesh=mesh,
        in_specs=(
            P(("dp", "mp"), None),
            P("dp", "mp", None),
            P(("dp", "mp"), None),
            P("dp"),
            P(),
            P(),
            P(),
            P(None, "mp", None, None),
            P("mp", None, None),
            P("mp", None, None, None),
            P(),
            P(),
            P(),
            P(None, "mp"),
            P("mp"),
            P("mp", None),
            P(),
        ),
        out_specs=(
            P(("dp", "mp"), None),
            P(("dp", "mp"), None),
            P("dp", "mp", None),
            P(),
            P(),
            P(None, "mp", None, None),
            P("mp", None, None),
            P("mp", None, None, None),
            P(),
            P(),
            P(),
            P(None, "mp"),
            P("mp"),
            P("mp", None),
            P(),
        ),
        check_vma=False,
    )
```

```python
import functools

import jax
import jax.numpy as jnp
from jax import lax
from jax.experimental import pallas as pl
from jax.experimental.pallas import tpu as pltpu
from jax.sharding import PartitionSpec as P


SHORT = 512
QROWS = 256
LANES = 128
PACK = 6

EPSILON = 1e-05
MASKED = -1e30
GELU_C = 0.7978845608028654
BF16 = jnp.bfloat16
F32 = jnp.float32


def gelu_tanh(values):
    return 0.5 * values * (1.0 + jnp.tanh(GELU_C * (values + 0.044715 * values * values * values)))


def rows_product(left, right):
    return lax.dot_general(left, right, (((0,), (0,)), ((), ())), preferred_element_type=F32)


def back_product(left, weight):
    return lax.dot_general(left, weight, (((1,), (1,)), ((), ())), preferred_element_type=F32)


def product(left, right):
    return jnp.dot(left, right, preferred_element_type=F32)


def opens_at(lengths, row):
    begin, opens = jnp.int32(0), jnp.int32(0)
    for slot in range(lengths.shape[0]):
        opens = jnp.maximum(opens, jnp.where(begin == row, 1, 0))
        begin = begin + lengths[slot]
    return opens


def head_lanes(head):
    lane = lax.broadcasted_iota(jnp.int32, (1, LANES), 1)
    return (lane < LANES // 2) if head == 0 else (lane >= LANES // 2)


def causal_tile():
    row = lax.broadcasted_iota(jnp.int32, (QROWS, QROWS), 0)
    column = lax.broadcasted_iota(jnp.int32, (QROWS, QROWS), 1)
    return column <= row


def pick_values(half, fresh, held, value_ref):
    if held.shape[1] < LANES:
        turned = jnp.concatenate([held, held], axis=1)
    else:
        turned = jnp.concatenate([held[:, LANES // 2 :], held[:, : LANES // 2]], axis=1)
        turned = jnp.where(half == 1, held, turned)
    value_ref[...] = jnp.where(head_lanes(0), fresh, turned)


def attend_forward_kernel(pairs, lengths, owner, place, qkv_ref, first_ref, mixed_ref, totals_ref, value_ref):
    half = lax.rem(owner[place[0] * pairs + pl.program_id(0)], pairs)
    pick_values(half, qkv_ref[:, 2 * LANES : 3 * LANES], first_ref[0], value_ref)
    blocks = qkv_ref.shape[0] // SHORT
    scale = (LANES // 2) ** (-0.5)

    def block(index, carried):
        base = pl.multiple_of(index * SHORT, SHORT)
        for half in range(SHORT // QROWS):
            first = base + half * QROWS

            def attend(with_previous):
                query = qkv_ref[pl.ds(first, QROWS), 0:LANES] * jnp.asarray(scale, BF16)
                spans = []
                if with_previous:
                    spans.append((base - SHORT, SHORT))
                if half:
                    spans.append((base, half * QROWS))
                spans.append((first, QROWS))
                mixed = jnp.zeros((QROWS, LANES), F32)
                totals = []
                for head in range(2):
                    chosen = head_lanes(head)
                    query_head = jnp.where(chosen, query, jnp.zeros_like(query))
                    scores = [
                        back_product(query_head, qkv_ref[pl.ds(at, size), LANES : 2 * LANES])
                        for at, size in spans
                    ]
                    scores[-1] = jnp.where(causal_tile(), scores[-1], MASKED)
                    top = scores[0].max(axis=1, keepdims=True)
                    for part in scores[1:]:
                        top = jnp.maximum(top, part.max(axis=1, keepdims=True))
                    total = jnp.zeros((QROWS, 1), F32)
                    gathered = jnp.zeros((QROWS, LANES), F32)
                    for (at, size), part in zip(spans, scores):
                        weights = jnp.exp(part - top)
                        total = total + weights.sum(axis=1, keepdims=True)
                        values = value_ref[pl.ds(at, size), :]
                        values = jnp.where(chosen, values, jnp.zeros_like(values))
                        gathered = gathered + product(weights.astype(BF16), values)
                    mixed = mixed + gathered / total
                    totals.append(top + jnp.log(total))
                mixed_ref[pl.ds(first, QROWS), :] = mixed.astype(BF16)
                totals_ref[pl.ds(first, QROWS), :] = jnp.where(
                    head_lanes(0), totals[0], totals[1]
                )

            @pl.when(opens_at(lengths, base) == 0)
            def _():
                attend(True)

            @pl.when(opens_at(lengths, base) == 1)
            def _():
                attend(False)

        return carried

    lax.fori_loop(0, blocks, block, 0)


def attend_backward_kernel(
    count, chunk, pairs, lengths, owner, qkv_ref, first_ref, grad_ref, totals_ref, left, weight, residual_ref, shift_ref,
    out_ref, skip_ref, sums_ref, layer_ref, key_sum, value_sum, value_ref, *scratch
):
    blocks = qkv_ref.shape[0] // SHORT
    scale = (LANES // 2) ** (-0.5)
    place, _, _ = mesh_place(count)
    greet(count)
    rows = residual_ref.shape[0]
    chunks = rows // chunk
    summed = RowSum(count, rows, chunk, left, weight, False, scratch)
    sums_ref[...] = jnp.zeros_like(sums_ref)
    summed.send()

    def one_pair(pair):
        column = pl.multiple_of(pair * 3 * LANES, LANES)
        side = pl.multiple_of(pair * LANES, LANES)
        query_at, key_at, fresh_at = (pl.ds(column + part * LANES, LANES) for part in range(3))
        used = owner[place * pairs + pair]
        held = first_ref[lax.div(used, pairs)]
        pick_values(lax.rem(used, pairs), qkv_ref[:, fresh_at], held, value_ref)
        key_sum[...] = jnp.zeros_like(key_sum)
        value_sum[...] = jnp.zeros_like(value_sum)

        def block(index):
            base = pl.multiple_of(index * SHORT, SHORT)
            joined = opens_at(lengths, base) == 0

            def attend(half, with_previous):
                first = base + half * QROWS
                query = qkv_ref[pl.ds(first, QROWS), query_at] * jnp.asarray(scale, BF16)
                grad = grad_ref[pl.ds(first, QROWS), pl.ds(side, LANES)]
                spans = []
                if with_previous:
                    spans.append((base - SHORT, SHORT))
                if half:
                    spans.append((base, half * QROWS))
                spans.append((first, QROWS))
                grad_query = jnp.zeros((QROWS, LANES), F32)
                both = totals_ref[pl.ds(first, QROWS), pl.ds(side, LANES)]
                for head in range(2):
                    chosen = head_lanes(head)
                    query_head = jnp.where(chosen, query, jnp.zeros_like(query))
                    grad_head = jnp.where(chosen, grad, jnp.zeros_like(grad))
                    at_lane = head * (LANES // 2)
                    totals = both[:, at_lane : at_lane + 1]
                    probs, grads = [], []
                    inner = jnp.zeros((QROWS, 1), F32)
                    for number, (at, size) in enumerate(spans):
                        keys = qkv_ref[pl.ds(at, size), key_at]
                        part = jnp.exp(back_product(query_head, keys) - totals)
                        if number == len(spans) - 1:
                            part = jnp.where(causal_tile(), part, 0.0)
                        elif with_previous and number == 0:
                            part = jnp.where(joined, part, 0.0)
                        values = value_ref[pl.ds(at, size), :]
                        weighted = part * back_product(grad_head, values)
                        inner = inner + weighted.sum(axis=1, keepdims=True)
                        probs.append(part)
                        grads.append(weighted)
                    for (at, size), part, weighted in zip(spans, probs, grads):
                        keys = qkv_ref[pl.ds(at, size), key_at]
                        keys = jnp.where(chosen, keys, jnp.zeros_like(keys))
                        grad_scores = (weighted - part * inner).astype(BF16)
                        grad_query = grad_query + product(grad_scores, keys)
                        key_sum[pl.ds(at, size), :] += rows_product(grad_scores, query_head)
                        value_sum[pl.ds(at, size), :] += rows_product(part.astype(BF16), grad_head)
                out_ref[pl.ds(first, QROWS), query_at] = (grad_query * scale).astype(BF16)

            for half in range(SHORT // QROWS):

                @pl.when(index > 0)
                def _():
                    attend(half, True)

                @pl.when(index == 0)
                def _():
                    attend(half, False)

        each(blocks, block)
        out_ref[:, key_at] = key_sum[...].astype(BF16)
        out_ref[:, fresh_at] = value_sum[...].astype(BF16)
        for slot in range(pairs):

            @pl.when(pair == slot)
            def _():
                width = LANES // 2
                skip_ref[:, slot * width : (slot + 1) * width] = value_sum[:, width:].astype(BF16)

        for at in (query_at, fresh_at):
            sums_ref[0:1, at] = column_sum(out_ref[:, at].astype(F32))

    each(pairs, one_pair)

    def close(index):
        at = rows_at(index, chunk)
        layer_ref[at, :] = (residual_ref[at, :] + summed.total(index) + shift_ref[...]).astype(BF16)

    each(chunks, close)
    each(chunks, summed.finish)


def attend_forward(lengths, owner, place, packed, firsts):
    rows, pairs = packed.shape[0], packed.shape[1] // (3 * LANES)
    return pl.pallas_call(
        functools.partial(attend_forward_kernel, pairs),
        grid_spec=pltpu.PrefetchScalarGridSpec(
            num_scalar_prefetch=3,
            grid=(pairs,),
            in_specs=[
                pl.BlockSpec((rows, 3 * LANES), lambda p, c, o, m: (0, p)),
                pl.BlockSpec((1, rows, firsts.shape[2]), lambda p, c, o, m: (lax.div(o[m[0] * pairs + p], pairs), 0, 0)),
            ],
            out_specs=[
                pl.BlockSpec((rows, LANES), lambda p, c, o, m: (0, p)),
                pl.BlockSpec((rows, LANES), lambda p, c, o, m: (0, p)),
            ],
            scratch_shapes=[pltpu.VMEM((rows, LANES), BF16)],
        ),
        out_shape=[
            jax.ShapeDtypeStruct((rows, pairs * LANES), BF16),
            jax.ShapeDtypeStruct((rows, pairs * LANES), F32),
        ],
        cost_estimate=pl.CostEstimate(
            flops=rows * 1024 * 256 * 4 * pairs, bytes_accessed=8 << 20, transcendentals=rows * 2048
        ),
        name="attend_forward",
    )(lengths, owner, place, packed, firsts)


def mesh_place(count):
    place = lax.axis_index("mp")
    core = lax.rem(place, 2)
    chip = lax.div(place, 2)
    chips = count // 2

    def across(step, other):
        return lax.rem(chip + step + chips, chips) * 2 + (1 - core if other else core)

    return place, place + 1 - 2 * core, across


def remote(source, target, sems, index, device):
    return pltpu.make_async_remote_copy(
        src_ref=source,
        dst_ref=target,
        send_sem=sems.at[(0, *index)],
        recv_sem=sems.at[(1, *index)],
        device_id={"mp": device},
        device_id_type=pl.DeviceIdType.MESH,
    )


def greet(count, copies=0):
    _, partner, across = mesh_place(count)
    barrier = pltpu.get_barrier_semaphore()
    for device in [partner] + [across(step, False) for step in range(1, count // 2)]:
        pl.semaphore_signal(
            barrier, inc=1, device_id={"mp": device}, device_id_type=pl.DeviceIdType.MESH
        )
    others = DpPlace(copies).greet(barrier) if copies else 0
    pl.semaphore_wait(barrier, count // 2 + others)


def each(count, step):
    def run(index, carried):
        step(index)
        return carried

    lax.fori_loop(0, count, run, 0)


class Gather:
    def __init__(self, count, out_ref, chunk, near, far, passed):
        self.count, self.out, self.chunk = count, out_ref, chunk
        self.near, self.far, self.passed = near, far, passed
        self.place, self.partner, self.across = mesh_place(count)

    def part(self, owner, index):
        return self.out.at[owner, pl.ds(pl.multiple_of(index * self.chunk, self.chunk), self.chunk), :]

    def send(self, index):
        own = self.part(self.place, index)
        for step in range(1, self.count // 2):
            remote(own, own, self.far, (step - 1, index), self.across(step, False)).start()
        remote(own, own, self.near, (index,), self.partner).start()

    def hand_on(self, index):
        for step in range(1, self.count // 2):
            got = self.part(self.across(-step, False), index)
            remote(got, got, self.far, (step - 1, index), self.across(step, False)).wait_recv()
            remote(got, got, self.passed, (step - 1, index), self.partner).start()

    def finish(self, index):
        own = self.part(self.place, index)
        near = self.part(self.partner, index)
        remote(own, near, self.near, (index,), self.partner).wait()
        for step in range(1, self.count // 2):
            remote(own, own, self.far, (step - 1, index), self.across(step, False)).wait_send()
            got = self.part(self.across(-step, True), index)
            remote(got, got, self.passed, (step - 1, index), self.partner).wait()


def gather_sems(count, chunks):
    far = max(count // 2 - 1, 1)
    return [
        pltpu.SemaphoreType.DMA((2, chunks)),
        pltpu.SemaphoreType.DMA((2, far, chunks)),
        pltpu.SemaphoreType.DMA((2, far, chunks)),
    ]


class RowSum:
    def __init__(self, count, rows, chunk, left, weight, flipped, buffers):
        self.count, self.rows, self.chunk = count, rows, chunk
        self.left, self.weight, self.flipped = left, weight, flipped
        (self.pair_out, self.pair_in, self.far_out, self.far_in, self.near_out, self.near_in, self.own) = buffers[:7]
        self.pair, self.far, self.near = buffers[7:]
        self.place, self.partner, self.across = mesh_place(count)

    def product(self, owner, index):
        at = pl.multiple_of(owner * self.rows + index * self.chunk, self.chunk)
        rows = self.left[pl.ds(at, self.chunk), :]
        return (back_product if self.flipped else product)(rows, self.weight[...])

    def pair_copy(self, step, index):
        return remote(
            self.pair_out.at[step - 1, index], self.pair_in.at[step - 1, index],
            self.pair, (step - 1, index), self.partner,
        )

    def far_copy(self, step, index):
        return remote(
            self.far_out.at[step - 1, index], self.far_in.at[step - 1, index],
            self.far, (step - 1, index), self.across(step, False),
        )

    def near_copy(self, index):
        return remote(self.near_out.at[index], self.near_in.at[index], self.near, (index,), self.partner)

    def send(self):
        chunks, far = self.rows // self.chunk, self.count // 2 - 1
        core = lax.rem(self.place, 2)

        def turn(number):
            kind, index = lax.div(number, chunks), lax.rem(number, chunks)
            step = lax.rem(kind, max(far, 1)) + 1
            owner = lax.rem(lax.div(self.place, 2) + step, self.count // 2) * 2
            owner = owner + jnp.where(kind < far, 1 - core, core)
            owner = jnp.where(kind == 2 * far, self.partner, owner)
            owner = jnp.where(kind > 2 * far, self.place, owner)
            rows = self.product(owner, index)

            @pl.when(kind < far)
            def _():
                self.pair_out[step - 1, index] = rows.astype(BF16)
                self.pair_copy(step, index).start()

            @pl.when((kind >= far) & (kind < 2 * far))
            def _():
                self.pair_copy(step, index).wait_recv()
                self.far_out[step - 1, index] = (rows + self.pair_in[step - 1, index].astype(F32)).astype(BF16)
                self.far_copy(step, index).start()

            @pl.when(kind == 2 * far)
            def _():
                self.near_out[index] = rows.astype(BF16)
                self.near_copy(index).start()

            @pl.when(kind > 2 * far)
            def _():
                self.own[index] = rows

        each((2 * far + 2) * chunks, turn)

    def total(self, index):
        self.near_copy(index).wait_recv()
        rows = self.own[index] + self.near_in[index].astype(F32)
        for step in range(1, self.count // 2):
            self.far_copy(step, index).wait_recv()
            rows = rows + self.far_in[step - 1, index].astype(F32)
        return rows

    def finish(self, index):
        self.near_copy(index).wait_send()
        for step in range(1, self.count // 2):
            self.pair_copy(step, index).wait_send()
            self.far_copy(step, index).wait_send()


def split_copies(copies):
    inner = 1
    while (2 * inner) ** 2 <= copies:
        inner *= 2
    return copies // inner, inner


def dp_copy(source, target, send_sem, recv_sem, device):
    return pltpu.make_async_remote_copy(
        src_ref=source, dst_ref=target, send_sem=send_sem, recv_sem=recv_sem,
        device_id={"dp": device}, device_id_type=pl.DeviceIdType.MESH,
    )


class DpPlace:
    def __init__(self, copies):
        self.outer, self.inner = split_copies(copies)
        here = lax.axis_index("dp")
        self.z, self.y = lax.div(here, self.inner), lax.rem(here, self.inner)

    def along_y(self, step):
        return lax.rem(self.y + step + self.inner, self.inner)

    def along_z(self, step):
        return lax.rem(self.z + step + self.outer, self.outer)

    def device(self, z, y):
        return z * self.inner + y

    def greet(self, barrier):
        for step in range(1, self.inner):
            pl.semaphore_signal(
                barrier, inc=1, device_id={"dp": self.device(self.z, self.along_y(step))},
                device_id_type=pl.DeviceIdType.MESH,
            )
        for step in range(1, self.outer):
            pl.semaphore_signal(
                barrier, inc=1, device_id={"dp": self.device(self.along_z(step), self.y)},
                device_id_type=pl.DeviceIdType.MESH,
            )
        return self.inner + self.outer - 2


class DpReduce:
    def __init__(self, copies, source, y_in, z_out, z_in, y_sems, z_sems):
        self.at = DpPlace(copies)
        self.source, self.y_in, self.z_out, self.z_in = source, y_in, z_out, z_in
        self.y_sems, self.z_sems = y_sems, z_sems

    def y_copy(self, step, z):
        peer = self.at.along_y(step)
        return dp_copy(
            self.source.at[z, peer], self.y_in.at[step - 1, z],
            self.y_sems.at[0, step - 1, z], self.y_sems.at[1, step - 1, z], self.at.device(self.at.z, peer),
        )

    def z_copy(self, step):
        peer = self.at.along_z(step + 1)
        return dp_copy(
            self.z_out.at[step], self.z_in.at[step],
            self.z_sems.at[0, step], self.z_sems.at[1, step], self.at.device(peer, self.at.y),
        )

    def send(self):
        def start(step):
            for y_step in range(1, self.at.inner):
                self.y_copy(y_step, self.at.along_z(step + 1)).start()

        each(self.at.outer, start)

    def y_total(self, z):
        total = self.source[z, self.at.y].astype(F32)
        for y_step in range(1, self.at.inner):
            self.y_copy(y_step, z).wait_recv()
            total = total + self.y_in[y_step - 1, z].astype(F32)
        return total

    def pass_on(self, step):
        @pl.when(step < self.at.outer - 1)
        def _():
            self.z_out[step] = self.y_total(self.at.along_z(step + 1)).astype(BF16)
            self.z_copy(step).start()

    def total(self):
        total = self.y_total(self.at.z)
        for step in range(self.at.outer - 1):
            self.z_copy(step).wait_recv()
            total = total + self.z_in[step].astype(F32)
        for step in range(self.at.outer - 1):
            self.z_copy(step).wait_send()
        for y_step in range(1, self.at.inner):
            for z in range(self.at.outer):
                self.y_copy(y_step, z).wait_send()
        return total


def reduce_scratch(copies, array):
    outer, inner = split_copies(copies)
    slab = array.shape[2:]
    return [
        pltpu.VMEM((inner - 1, outer, *slab), BF16),
        pltpu.VMEM((outer - 1, *slab), BF16),
        pltpu.VMEM((outer - 1, *slab), BF16),
        pltpu.SemaphoreType.DMA((2, inner - 1, outer)),
        pltpu.SemaphoreType.DMA((2, outer - 1)),
    ]


class DpGather:
    def __init__(self, copies, slab, held, z_sems, y_sems):
        self.at = DpPlace(copies)
        self.slab, self.held, self.z_sems, self.y_sems = slab, held, z_sems, y_sems

    def z_copy(self, step, z):
        here = self.held.at[z, self.at.y]
        peer = self.at.device(self.at.along_z(step + 1), self.at.y)
        return dp_copy(here, here, self.z_sems.at[0, step], self.z_sems.at[1, step], peer)

    def y_copy(self, y_step, slot, z, y):
        here = self.held.at[z, y]
        peer = self.at.device(self.at.z, self.at.along_y(y_step))
        return dp_copy(
            here, here, self.y_sems.at[0, y_step - 1, slot], self.y_sems.at[1, y_step - 1, slot], peer
        )

    def send(self):
        self.held[self.at.z, self.at.y] = self.slab[...]
        for step in range(self.at.outer - 1):
            self.z_copy(step, self.at.z).start()
        for y_step in range(1, self.at.inner):
            self.y_copy(y_step, self.at.outer - 1, self.at.z, self.at.y).start()

    def pass_on(self, step):
        @pl.when(step < self.at.outer - 1)
        def _():
            source = self.at.along_z(-step - 1)
            self.z_copy(step, source).wait_recv()
            for y_step in range(1, self.at.inner):
                self.y_copy(y_step, step, source, self.at.y).start()

    def finish(self):
        for step in range(self.at.outer - 1):
            self.z_copy(step, self.at.z).wait_send()
        for y_step in range(1, self.at.inner):
            sender = self.at.along_y(-y_step)
            for slot in range(self.at.outer):
                source = self.at.along_z(-slot - 1)
                self.y_copy(y_step, slot, source, sender).wait_recv()
                self.y_copy(y_step, slot, source, self.at.y).wait_send()


def gather_scratch(copies):
    outer, inner = split_copies(copies)
    return [pltpu.SemaphoreType.DMA((2, outer - 1)), pltpu.SemaphoreType.DMA((2, inner - 1, outer))]


def spread(index, chunks, copies, steps):
    outer = split_copies(copies)[0]
    turns = -(-outer // chunks)

    def turn(sub):
        for step in steps:
            step(index * turns + sub)

    each(turns, turn)


def row_sum_scratch(count, rows, chunk, width):
    far, chunks = max(count // 2 - 1, 1), rows // chunk
    wide = pltpu.VMEM((far, chunks, chunk, width), BF16)
    slim = pltpu.VMEM((chunks, chunk, width), BF16)
    return [
        wide, wide, wide, wide, slim, slim, pltpu.VMEM((chunks, chunk, width), F32),
        pltpu.SemaphoreType.DMA((2, far, chunks)),
        pltpu.SemaphoreType.DMA((2, far, chunks)),
        pltpu.SemaphoreType.DMA((2, chunks)),
    ]


def rows_at(index, chunk):
    return pl.ds(pl.multiple_of(index * chunk, chunk), chunk)


def standardize(values):
    average = jnp.mean(values, axis=-1, keepdims=True)
    centered = values - average
    spread = lax.rsqrt(jnp.mean(centered * centered, axis=-1, keepdims=True) + EPSILON)
    return centered * spread, spread


def norm_backward(values, grad, gain):
    normed, spread = standardize(values)
    scaled = grad * gain
    inner = jnp.mean(scaled * normed, axis=-1, keepdims=True)
    back = (scaled - jnp.mean(scaled, axis=-1, keepdims=True) - normed * inner) * spread
    return back, grad * normed


def column_sum(values):
    return jnp.sum(values, axis=0, keepdims=True)


def open_kernel(count, chunk, x_ref, gain_ref, shift_ref, first_ref, rows_ref, all_ref, *sems):
    rows = x_ref.shape[0]
    place, _, _ = mesh_place(count)
    greet(count)
    chunks = rows // chunk
    main = Gather(count, rows_ref, chunk, *sems[:3])
    side_chunk = first_ref.shape[0] // 2
    side = Gather(count, all_ref, side_chunk, *sems[3:])

    def start(index):
        values = x_ref[rows_at(index, chunk), :].astype(F32)
        normed = standardize(values)[0] * gain_ref[...] + shift_ref[...]
        rows_ref[place, rows_at(index, chunk), :] = normed.astype(BF16)
        main.send(index)

    each(chunks, start)

    def side_start(index):
        all_ref[place, rows_at(index, side_chunk), :] = first_ref[rows_at(index, side_chunk), :]
        side.send(index)

    each(2, side_start)
    each(chunks, main.hand_on)
    each(2, side.hand_on)
    each(chunks, main.finish)
    each(2, side.finish)


def attend_out_kernel(
    count, chunk, left, weight, x_ref, bias_ref, gain_ref, shift_ref, rows_ref, residual_ref, *scratch
):
    rows = x_ref.shape[0]
    place, _, _ = mesh_place(count)
    greet(count)
    chunks = rows // chunk
    summed = RowSum(count, rows, chunk, left, weight, False, scratch[:10])
    main = Gather(count, rows_ref, chunk, *scratch[10:])
    summed.send()

    def close(index):
        at = rows_at(index, chunk)
        values = x_ref[at, :].astype(F32) + summed.total(index) + bias_ref[...]
        residual_ref[at, :] = values
        normed = standardize(values)[0] * gain_ref[...] + shift_ref[...]
        rows_ref[place, at, :] = normed.astype(BF16)
        main.send(index)

    each(chunks, close)
    each(chunks, main.hand_on)
    each(chunks, main.finish)
    each(chunks, summed.finish)


def mlp_back_kernel(
    count, chunk, left, weight, residual_ref, dy_ref, gain_ref, rows_ref, grad_ref, sums_ref, *scratch
):
    rows = residual_ref.shape[0]
    place, _, _ = mesh_place(count)
    greet(count)
    chunks = rows // chunk
    summed = RowSum(count, rows, chunk, left, weight, True, scratch[:10])
    main = Gather(count, rows_ref, chunk, *scratch[10:])
    sums_ref[...] = jnp.zeros_like(sums_ref)
    summed.send()

    def close(index):
        at = rows_at(index, chunk)
        total = summed.total(index)
        dy = dy_ref[at, :].astype(F32)
        back, per_gain = norm_backward(residual_ref[at, :], total, gain_ref[...])
        grad = dy + back
        grad_ref[at, :] = grad
        rows_ref[place, at, :] = grad.astype(BF16)
        main.send(index)
        sums_ref[0:1, :] += column_sum(per_gain)
        sums_ref[1:2, :] += column_sum(total)
        sums_ref[2:3, :] += column_sum(grad)
        sums_ref[3:4, :] += column_sum(dy)

    each(chunks, close)
    each(chunks, main.hand_on)
    each(chunks, main.finish)
    each(chunks, summed.finish)


def input_back_kernel(
    count, copies, chunk, left, weight, x_ref, grad_ref, gain_ref, qkv_ref, outw_ref,
    out_ref, sums_ref, qkv_slab, outw_slab, *scratch
):
    rows = x_ref.shape[0]
    greet(count, copies)
    chunks = rows // chunk
    summed = RowSum(count, rows, chunk, left, weight, True, scratch[:10])
    outw = DpReduce(copies, outw_ref, *scratch[10:15])
    qkv = DpReduce(copies, qkv_ref, *scratch[15:20])
    qkv.send()
    outw.send()
    sums_ref[...] = jnp.zeros_like(sums_ref)
    summed.send()

    def close(index):
        at = rows_at(index, chunk)
        total = summed.total(index)
        back, per_gain = norm_backward(x_ref[at, :].astype(F32), total, gain_ref[...])
        out_ref[at, :] = (grad_ref[at, :] + back).astype(BF16)
        sums_ref[0:1, :] += column_sum(per_gain)
        sums_ref[1:2, :] += column_sum(total)
        spread(index, chunks, copies, [qkv.pass_on, outw.pass_on])

    each(chunks, close)
    qkv_slab[...] = qkv.total().astype(BF16)
    outw_slab[...] = outw.total().astype(BF16)
    each(chunks, summed.finish)


def closing_kernel(
    count, copies, shared, small_ref, skip_ref, qkv_slab, outw_slab,
    small_out, all_ref, qkv_ref, outw_ref, *scratch
):
    copy, place = lax.axis_index("dp"), lax.axis_index("mp")
    barrier = pltpu.get_barrier_semaphore()
    for step in range(1, copies):
        pl.semaphore_signal(
            barrier, inc=1, device_id={"dp": lax.rem(copy + step, copies)}, device_id_type=pl.DeviceIdType.MESH
        )
    for step in range(1, count):
        pl.semaphore_signal(
            barrier, inc=1, device_id={"mp": lax.rem(place + step, count)}, device_id_type=pl.DeviceIdType.MESH
        )
    pl.semaphore_wait(barrier, copies + count - 2)
    side_chunk = skip_ref.shape[0] // 2
    side = Gather(count, all_ref, side_chunk, *scratch[0:3])
    qkv = DpGather(copies, qkv_slab, qkv_ref, *scratch[3:5])
    outw = DpGather(copies, outw_slab, outw_ref, *scratch[5:7])
    copy_in, part_in, part_out, copy_sems, part_sems = scratch[7:]

    def small_copy(axis, own, size, source, slots, sems, step, slot):
        return pltpu.make_async_remote_copy(
            src_ref=source, dst_ref=slots.at[slot], send_sem=sems.at[0, step], recv_sem=sems.at[1, slot],
            device_id={axis: lax.rem(own + step, size)}, device_id_type=pl.DeviceIdType.MESH,
        )

    def small_start(axis, own, size, source, slots, sems):
        slots[own] = source[...]
        for step in range(1, size):
            small_copy(axis, own, size, source, slots, sems, step, own).start()

    def small_total(axis, own, size, source, slots, sems):
        for step in range(1, size):
            slot = lax.rem(own + size - step, size)
            small_copy(axis, own, size, source, slots, sems, step, slot).wait_recv()
            small_copy(axis, own, size, source, slots, sems, step, own).wait_send()
        total = slots[0]
        for slot in range(1, size):
            total = total + slots[slot]
        return total

    over_copies = ("dp", copy, copies, small_ref, copy_in, copy_sems)
    over_parts = ("mp", place, count, part_out, part_in, part_sems)
    small_start(*over_copies)
    qkv.send()
    outw.send()

    def side_start(index):
        all_ref[place, rows_at(index, side_chunk), :] = skip_ref[rows_at(index, side_chunk), :]
        side.send(index)

    each(2, side_start)
    part_out[...] = small_total(*over_copies)
    small_start(*over_parts)
    every = small_total(*over_parts)
    row = lax.broadcasted_iota(jnp.int32, every.shape, 0)
    small_out[...] = jnp.where(row < shared, every, part_out[...])

    def pass_on(index):
        qkv.pass_on(index)
        outw.pass_on(index)

    each(qkv.at.outer, pass_on)
    each(2, side.hand_on)
    outw.finish()
    qkv.finish()
    each(2, side.finish)


def user_of(owner, head):
    user = jnp.int32(0)
    for pair in range(owner.shape[0]):
        user = user + jnp.where(owner[pair] == head, pair, 0)
    return user


def pick_gradient(owner, place, every, pairs):
    _, rows, slim = every.shape
    width = slim // pairs

    def kernel(owner, place, *refs):
        for slot in range(pairs):
            held = refs[slot][0]
            user = lax.rem(user_of(owner, place[0] * pairs + slot), pairs)
            value = held[:, 0:width]
            for part in range(1, pairs):
                value = jnp.where(user == part, held[:, part * width : (part + 1) * width], value)
            refs[-1][:, slot * width : (slot + 1) * width] = value

    def block(slot):
        return pl.BlockSpec(
            (1, rows // 4, slim),
            lambda g, o, m: (lax.div(user_of(o, m[0] * pairs + slot), pairs), g, 0),
        )

    return pl.pallas_call(
        kernel,
        grid_spec=pltpu.PrefetchScalarGridSpec(
            num_scalar_prefetch=2,
            grid=(4,),
            in_specs=[block(slot) for slot in range(pairs)],
            out_specs=pl.BlockSpec((rows // 4, slim), lambda g, o, m: (g, 0)),
        ),
        out_shape=jax.ShapeDtypeStruct((rows, slim), BF16),
        name="pick_gradient",
    )(owner, place, *([every] * pairs))


def call(kernel, number, inputs, outputs, scratch, flops, scalars=0):
    moved = sum(a.size * a.dtype.itemsize for a in (*inputs, *outputs))
    return pl.pallas_call(
        kernel,
        out_shape=outputs,
        in_specs=[pl.BlockSpec(memory_space=pltpu.SMEM)] * scalars
        + [pl.BlockSpec(memory_space=pltpu.VMEM)] * (len(inputs) - scalars),
        out_specs=[pl.BlockSpec(memory_space=pltpu.VMEM)] * len(outputs),
        scratch_shapes=scratch,
        compiler_params=pltpu.CompilerParams(collective_id=number, has_side_effects=True),
        cost_estimate=pl.CostEstimate(flops=flops, bytes_accessed=moved, transcendentals=0),
    )(*inputs)


def like(shape, kind):
    return jax.ShapeDtypeStruct(shape, kind)


def body(
    inputs,
    first_values,
    cotangent,
    seq_lengths,
    value_owner,
    attn_norm_gain,
    attn_norm_bias,
    qkv_weight,
    qv_bias,
    out_weight,
    out_bias,
    mlp_norm_gain,
    mlp_norm_bias,
    up_weight,
    up_bias,
    down_weight,
    down_bias,
):
    local_rows, model_width = inputs.shape
    group_rows = local_rows * lax.axis_size("mp")
    pairs_dev, head_size = qkv_weight.shape[1], qkv_weight.shape[3]
    seats = (seq_lengths, value_owner, lax.axis_index("mp").reshape(1).astype(jnp.int32))
    copies = lax.axis_size("dp")

    qkv_pack = jnp.pad(qkv_weight, ((0, 0), (0, 0), (0, 1), (0, 0)))
    qkv_pack = qkv_pack.reshape(model_width, pairs_dev * PACK * head_size)
    bias_pack = jnp.concatenate(
        [qv_bias[:, 0:2], jnp.zeros_like(qv_bias[:, 0:2]), qv_bias[:, 2:3], jnp.zeros_like(qv_bias[:, 2:3])],
        axis=1,
    ).reshape(1, pairs_dev * PACK * head_size)
    out_flat = out_weight.reshape(pairs_dev * 2 * head_size, model_width)

    count = lax.axis_size("mp")
    chunk = min(128, local_rows)
    chunks = local_rows // chunk
    row = (1, model_width)
    whole = (count, local_rows, model_width)
    slim = pairs_dev * head_size
    sum_scratch = row_sum_scratch(count, local_rows, chunk, model_width)
    main_sems, side_sems = gather_sems(count, chunks), gather_sems(count, 2)
    dense = 2 * group_rows * model_width

    rows_one, all_first = call(
        functools.partial(open_kernel, count, chunk), 0,
        (inputs, attn_norm_gain.reshape(row), attn_norm_bias.reshape(row), first_values.reshape(group_rows, slim)),
        [like(whole, BF16), like((count, group_rows, slim), BF16)],
        main_sems + side_sems, dense * 100,
    )
    rows_one = rows_one.reshape(group_rows, model_width)
    packed = (product(rows_one, qkv_pack) + bias_pack).astype(BF16)
    cotangent_late = lax.optimization_barrier((cotangent, rows_one))[0]
    grad_rows = lax.all_gather(cotangent_late, "mp", axis=0, tiled=True)
    mixed, totals = attend_forward(*seats, packed, all_first)
    rows_two, residual = call(
        functools.partial(attend_out_kernel, count, chunk), 1,
        (mixed, out_flat, inputs, out_bias.reshape(row), mlp_norm_gain.reshape(row), mlp_norm_bias.reshape(row)),
        [like(whole, BF16), like(inputs.shape, F32)],
        sum_scratch + main_sems, dense * 256,
    )
    rows_two = rows_two.reshape(group_rows, model_width)
    hidden_pre = product(rows_two, up_weight) + up_bias
    hidden = gelu_tanh(hidden_pre).astype(BF16)
    grad_hidden = back_product(grad_rows, down_weight)
    grad_pre = jax.vjp(gelu_tanh, hidden_pre)[1](grad_hidden)[0].astype(BF16)
    grad_down_weight = rows_product(hidden, grad_rows).astype(BF16)
    grad_up_weight = rows_product(rows_two, grad_pre).astype(BF16)
    grad_up_bias = jnp.sum(grad_pre.astype(F32), axis=0)
    outer, inner = split_copies(copies)

    def sliced(values):
        return values.reshape(outer, inner, values.shape[0] // copies, values.shape[1])

    late = (grad_up_weight, grad_down_weight)
    grad_pre, late = lax.optimization_barrier((grad_pre, late))
    late_sums = lax.psum(late, "dp")
    resid_rows, grad_residual, sums_two = call(
        functools.partial(mlp_back_kernel, count, chunk), 2,
        (grad_pre, up_weight, residual, cotangent, mlp_norm_gain.reshape(row)),
        [like(whole, BF16), like(inputs.shape, F32), like((8, model_width), F32)],
        sum_scratch + main_sems, dense * up_bias.shape[0],
    )
    resid_rows = resid_rows.reshape(group_rows, model_width)
    grad_mixed = back_product(resid_rows, out_flat).astype(BF16)
    grad_out_weight = rows_product(mixed, resid_rows).astype(BF16)
    packs = pairs_dev * PACK * head_size
    grad_flat, grad_skip, pack_sums, output = call(
        functools.partial(attend_backward_kernel, count, chunk, pairs_dev), 5,
        (seq_lengths, value_owner, packed, all_first, grad_mixed, totals, hidden, down_weight, residual,
         down_bias.reshape(row)),
        [like((group_rows, packs), BF16), like((group_rows, slim), BF16), like((8, packs), F32),
         like(inputs.shape, BF16)],
        [pltpu.VMEM((group_rows, LANES), F32), pltpu.VMEM((group_rows, LANES), F32),
         pltpu.VMEM((group_rows, LANES), BF16)] + sum_scratch,
        group_rows * 1024 * 256 * 10 * pairs_dev, scalars=2,
    )
    pack_sums = pack_sums[0].reshape(pairs_dev, PACK, head_size)
    grad_qv_bias = jnp.concatenate([pack_sums[:, 0:2], pack_sums[:, 4:5]], axis=1)
    grad_qkv_weight = sliced(rows_product(rows_one, grad_flat).astype(BF16))
    grad_out_weight = sliced(grad_out_weight)
    grad_inputs, sums_one, qkv_slab, out_slab = call(
        functools.partial(input_back_kernel, count, copies, chunk), 3,
        (grad_flat, qkv_pack, inputs, grad_residual, attn_norm_gain.reshape(row), grad_qkv_weight, grad_out_weight),
        [like(inputs.shape, BF16), like((8, model_width), F32),
         like(grad_qkv_weight.shape[2:], BF16), like(grad_out_weight.shape[2:], BF16)],
        sum_scratch + reduce_scratch(copies, grad_out_weight) + reduce_scratch(copies, grad_qkv_weight),
        dense * packs,
    )
    wide_bias = jnp.pad(grad_up_bias, (0, model_width - grad_up_bias.shape[0])).reshape(row)
    slim_bias = jnp.pad(grad_qv_bias.reshape(-1), (0, model_width - grad_qv_bias.size)).reshape(row)
    own_sums = jnp.concatenate([sums_two[0:4], sums_one[0:2], wide_bias, slim_bias], axis=0)
    block = pltpu.VMEM(own_sums.shape, F32)
    small, every_skip, qkv_sum, out_sum = call(
        functools.partial(closing_kernel, count, copies, 6), 4,
        (own_sums, grad_skip, qkv_slab, out_slab),
        [like(own_sums.shape, F32), like((count, group_rows, slim), BF16),
         like(grad_qkv_weight.shape, BF16), like(grad_out_weight.shape, BF16)],
        side_sems + gather_scratch(copies) + gather_scratch(copies)
        + [pltpu.VMEM((copies, *own_sums.shape), F32), pltpu.VMEM((count, *own_sums.shape), F32), block,
           pltpu.SemaphoreType.DMA((2, copies)), pltpu.SemaphoreType.DMA((2, count))],
        own_sums.size * (copies + count),
    )
    qkv_sum = qkv_sum.reshape(model_width, pairs_dev, PACK, head_size)[:, :, 0:5].astype(F32)
    late_sums = (*(part.astype(F32) for part in late_sums), out_sum.reshape(out_weight.shape).astype(F32))
    grad_first = pick_gradient(*seats[1:], every_skip, pairs_dev).reshape(group_rows, pairs_dev, head_size)
    norm_sums = (small[4], small[5], small[2], small[0], small[1], small[3])
    bias_sums = (small[7, : grad_qv_bias.size].reshape(qv_bias.shape), small[6, : grad_up_bias.shape[0]])

    return (
        output,
        grad_inputs,
        grad_first,
        norm_sums[0],
        norm_sums[1],
        qkv_sum,
        bias_sums[0],
        late_sums[2],
        norm_sums[2],
        norm_sums[3],
        norm_sums[4],
        late_sums[0],
        bias_sums[1],
        late_sums[1],
        norm_sums[5],
    )


def solution(mesh):
    return jax.shard_map(
        body,
        mesh=mesh,
        in_specs=(
            P(("dp", "mp"), None),
            P("dp", "mp", None),
            P(("dp", "mp"), None),
            P("dp"),
            P(),
            P(),
            P(),
            P(None, "mp", None, None),
            P("mp", None, None),
            P("mp", None, None, None),
            P(),
            P(),
            P(),
            P(None, "mp"),
            P("mp"),
            P("mp", None),
            P(),
        ),
        out_specs=(
            P(("dp", "mp"), None),
            P(("dp", "mp"), None),
            P("dp", "mp", None),
            P(),
            P(),
            P(None, "mp", None, None),
            P("mp", None, None),
            P("mp", None, None, None),
            P(),
            P(),
            P(),
            P(None, "mp"),
            P("mp"),
            P("mp", None),
            P(),
        ),
        check_vma=False,
    )
```

```python
import functools

import jax
import jax.numpy as jnp
from jax import lax
from jax.experimental import pallas as pl
from jax.experimental.pallas import tpu as pltpu
from jax.sharding import PartitionSpec as P


SHORT = 512
QROWS = 256
LANES = 128
PACK = 6

EPSILON = 1e-05
MASKED = -1e30
GELU_C = 0.7978845608028654
BF16 = jnp.bfloat16
F32 = jnp.float32


def gelu_tanh(values):
    return 0.5 * values * (1.0 + jnp.tanh(GELU_C * (values + 0.044715 * values * values * values)))


def rows_product(left, right):
    return lax.dot_general(left, right, (((0,), (0,)), ((), ())), preferred_element_type=F32)


def back_product(left, weight):
    return lax.dot_general(left, weight, (((1,), (1,)), ((), ())), preferred_element_type=F32)


def product(left, right):
    return jnp.dot(left, right, preferred_element_type=F32)


def opens_at(lengths, row):
    begin, opens = jnp.int32(0), jnp.int32(0)
    for slot in range(lengths.shape[0]):
        opens = jnp.maximum(opens, jnp.where(begin == row, 1, 0))
        begin = begin + lengths[slot]
    return opens


def head_lanes(head):
    lane = lax.broadcasted_iota(jnp.int32, (1, LANES), 1)
    return (lane < LANES // 2) if head == 0 else (lane >= LANES // 2)


def causal_tile():
    row = lax.broadcasted_iota(jnp.int32, (QROWS, QROWS), 0)
    column = lax.broadcasted_iota(jnp.int32, (QROWS, QROWS), 1)
    return column <= row


def pick_values(half, fresh, held, value_ref):
    if held.shape[1] < LANES:
        turned = jnp.concatenate([held, held], axis=1)
    else:
        turned = jnp.concatenate([held[:, LANES // 2 :], held[:, : LANES // 2]], axis=1)
        turned = jnp.where(half == 1, held, turned)
    value_ref[...] = jnp.where(head_lanes(0), fresh, turned)


def attend_forward_kernel(pairs, lengths, owner, place, qkv_ref, first_ref, mixed_ref, totals_ref, value_ref):
    half = lax.rem(owner[place[0] * pairs + pl.program_id(0)], pairs)
    pick_values(half, qkv_ref[:, 2 * LANES : 3 * LANES], first_ref[0], value_ref)
    blocks = qkv_ref.shape[0] // SHORT
    scale = (LANES // 2) ** (-0.5)

    def block(index, carried):
        base = pl.multiple_of(index * SHORT, SHORT)
        for half in range(SHORT // QROWS):
            first = base + half * QROWS

            def attend(with_previous):
                query = qkv_ref[pl.ds(first, QROWS), 0:LANES] * jnp.asarray(scale, BF16)
                spans = []
                if with_previous:
                    spans.append((base - SHORT, SHORT))
                if half:
                    spans.append((base, half * QROWS))
                spans.append((first, QROWS))
                mixed = jnp.zeros((QROWS, LANES), F32)
                totals = []
                for head in range(2):
                    chosen = head_lanes(head)
                    query_head = jnp.where(chosen, query, jnp.zeros_like(query))
                    scores = [
                        back_product(query_head, qkv_ref[pl.ds(at, size), LANES : 2 * LANES])
                        for at, size in spans
                    ]
                    scores[-1] = jnp.where(causal_tile(), scores[-1], MASKED)
                    top = scores[0].max(axis=1, keepdims=True)
                    for part in scores[1:]:
                        top = jnp.maximum(top, part.max(axis=1, keepdims=True))
                    total = jnp.zeros((QROWS, 1), F32)
                    gathered = jnp.zeros((QROWS, LANES), F32)
                    for (at, size), part in zip(spans, scores):
                        weights = jnp.exp(part - top)
                        total = total + weights.sum(axis=1, keepdims=True)
                        values = value_ref[pl.ds(at, size), :]
                        values = jnp.where(chosen, values, jnp.zeros_like(values))
                        gathered = gathered + product(weights.astype(BF16), values)
                    mixed = mixed + gathered / total
                    totals.append(top + jnp.log(total))
                mixed_ref[pl.ds(first, QROWS), :] = mixed.astype(BF16)
                totals_ref[pl.ds(first, QROWS), :] = jnp.where(
                    head_lanes(0), totals[0], totals[1]
                )

            @pl.when(opens_at(lengths, base) == 0)
            def _():
                attend(True)

            @pl.when(opens_at(lengths, base) == 1)
            def _():
                attend(False)

        return carried

    lax.fori_loop(0, blocks, block, 0)


def attend_backward_kernel(
    count, chunk, pairs, lengths, owner, qkv_ref, first_ref, grad_ref, totals_ref, left, weight, residual_ref, shift_ref,
    out_ref, skip_ref, sums_ref, layer_ref, key_sum, value_sum, value_ref, *scratch
):
    blocks = qkv_ref.shape[0] // SHORT
    scale = (LANES // 2) ** (-0.5)
    place, _, _ = mesh_place(count)
    greet(count)
    rows = residual_ref.shape[0]
    chunks = rows // chunk
    summed = RowSum(count, rows, chunk, left, weight, False, scratch)
    sums_ref[...] = jnp.zeros_like(sums_ref)
    summed.send()

    def one_pair(pair):
        column = pl.multiple_of(pair * 3 * LANES, LANES)
        side = pl.multiple_of(pair * LANES, LANES)
        query_at, key_at, fresh_at = (pl.ds(column + part * LANES, LANES) for part in range(3))
        used = owner[place * pairs + pair]
        held = first_ref[lax.div(used, pairs)]
        pick_values(lax.rem(used, pairs), qkv_ref[:, fresh_at], held, value_ref)
        key_sum[...] = jnp.zeros_like(key_sum)
        value_sum[...] = jnp.zeros_like(value_sum)

        def block(index):
            base = pl.multiple_of(index * SHORT, SHORT)
            joined = opens_at(lengths, base) == 0

            def attend(half, with_previous):
                first = base + half * QROWS
                query = qkv_ref[pl.ds(first, QROWS), query_at] * jnp.asarray(scale, BF16)
                grad = grad_ref[pl.ds(first, QROWS), pl.ds(side, LANES)]
                spans = []
                if with_previous:
                    spans.append((base - SHORT, SHORT))
                if half:
                    spans.append((base, half * QROWS))
                spans.append((first, QROWS))
                grad_query = jnp.zeros((QROWS, LANES), F32)
                both = totals_ref[pl.ds(first, QROWS), pl.ds(side, LANES)]
                for head in range(2):
                    chosen = head_lanes(head)
                    query_head = jnp.where(chosen, query, jnp.zeros_like(query))
                    grad_head = jnp.where(chosen, grad, jnp.zeros_like(grad))
                    at_lane = head * (LANES // 2)
                    totals = both[:, at_lane : at_lane + 1]
                    probs, grads = [], []
                    inner = jnp.zeros((QROWS, 1), F32)
                    for number, (at, size) in enumerate(spans):
                        keys = qkv_ref[pl.ds(at, size), key_at]
                        part = jnp.exp(back_product(query_head, keys) - totals)
                        if number == len(spans) - 1:
                            part = jnp.where(causal_tile(), part, 0.0)
                        elif with_previous and number == 0:
                            part = jnp.where(joined, part, 0.0)
                        values = value_ref[pl.ds(at, size), :]
                        weighted = part * back_product(grad_head, values)
                        inner = inner + weighted.sum(axis=1, keepdims=True)
                        probs.append(part)
                        grads.append(weighted)
                    for (at, size), part, weighted in zip(spans, probs, grads):
                        keys = qkv_ref[pl.ds(at, size), key_at]
                        keys = jnp.where(chosen, keys, jnp.zeros_like(keys))
                        grad_scores = (weighted - part * inner).astype(BF16)
                        grad_query = grad_query + product(grad_scores, keys)
                        key_sum[pl.ds(at, size), :] += rows_product(grad_scores, query_head)
                        value_sum[pl.ds(at, size), :] += rows_product(part.astype(BF16), grad_head)
                out_ref[pl.ds(first, QROWS), query_at] = (grad_query * scale).astype(BF16)

            for half in range(SHORT // QROWS):

                @pl.when(index > 0)
                def _():
                    attend(half, True)

                @pl.when(index == 0)
                def _():
                    attend(half, False)

        each(blocks, block)
        out_ref[:, key_at] = key_sum[...].astype(BF16)
        out_ref[:, fresh_at] = value_sum[...].astype(BF16)
        for slot in range(pairs):

            @pl.when(pair == slot)
            def _():
                width = LANES // 2
                skip_ref[:, slot * width : (slot + 1) * width] = value_sum[:, width:].astype(BF16)

        for at in (query_at, fresh_at):
            sums_ref[0:1, at] = column_sum(out_ref[:, at].astype(F32))

    each(pairs, one_pair)

    def close(index):
        at = rows_at(index, chunk)
        layer_ref[at, :] = (residual_ref[at, :] + summed.total(index) + shift_ref[...]).astype(BF16)

    each(chunks, close)
    each(chunks, summed.finish)


def attend_forward(lengths, owner, place, packed, firsts):
    rows, pairs = packed.shape[0], packed.shape[1] // (3 * LANES)
    return pl.pallas_call(
        functools.partial(attend_forward_kernel, pairs),
        grid_spec=pltpu.PrefetchScalarGridSpec(
            num_scalar_prefetch=3,
            grid=(pairs,),
            in_specs=[
                pl.BlockSpec((rows, 3 * LANES), lambda p, c, o, m: (0, p)),
                pl.BlockSpec((1, rows, firsts.shape[2]), lambda p, c, o, m: (lax.div(o[m[0] * pairs + p], pairs), 0, 0)),
            ],
            out_specs=[
                pl.BlockSpec((rows, LANES), lambda p, c, o, m: (0, p)),
                pl.BlockSpec((rows, LANES), lambda p, c, o, m: (0, p)),
            ],
            scratch_shapes=[pltpu.VMEM((rows, LANES), BF16)],
        ),
        out_shape=[
            jax.ShapeDtypeStruct((rows, pairs * LANES), BF16),
            jax.ShapeDtypeStruct((rows, pairs * LANES), F32),
        ],
        cost_estimate=pl.CostEstimate(
            flops=rows * 1024 * 256 * 4 * pairs, bytes_accessed=8 << 20, transcendentals=rows * 2048
        ),
        name="attend_forward",
    )(lengths, owner, place, packed, firsts)


def mesh_place(count):
    place = lax.axis_index("mp")
    core = lax.rem(place, 2)
    chip = lax.div(place, 2)
    chips = count // 2

    def across(step, other):
        return lax.rem(chip + step + chips, chips) * 2 + (1 - core if other else core)

    return place, place + 1 - 2 * core, across


def remote(source, target, sems, index, device):
    return pltpu.make_async_remote_copy(
        src_ref=source,
        dst_ref=target,
        send_sem=sems.at[(0, *index)],
        recv_sem=sems.at[(1, *index)],
        device_id={"mp": device},
        device_id_type=pl.DeviceIdType.MESH,
    )


def greet(count, copies=0):
    _, partner, across = mesh_place(count)
    barrier = pltpu.get_barrier_semaphore()
    for device in [partner] + [across(step, False) for step in range(1, count // 2)]:
        pl.semaphore_signal(
            barrier, inc=1, device_id={"mp": device}, device_id_type=pl.DeviceIdType.MESH
        )
    others = DpPlace(copies).greet(barrier) if copies else 0
    pl.semaphore_wait(barrier, count // 2 + others)


def each(count, step):
    def run(index, carried):
        step(index)
        return carried

    lax.fori_loop(0, count, run, 0)


class Gather:
    def __init__(self, count, out_ref, chunk, near, far, passed):
        self.count, self.out, self.chunk = count, out_ref, chunk
        self.near, self.far, self.passed = near, far, passed
        self.place, self.partner, self.across = mesh_place(count)

    def part(self, owner, index):
        return self.out.at[owner, pl.ds(pl.multiple_of(index * self.chunk, self.chunk), self.chunk), :]

    def send(self, index):
        own = self.part(self.place, index)
        for step in range(1, self.count // 2):
            remote(own, own, self.far, (step - 1, index), self.across(step, False)).start()
        remote(own, own, self.near, (index,), self.partner).start()

    def hand_on(self, index):
        for step in range(1, self.count // 2):
            got = self.part(self.across(-step, False), index)
            remote(got, got, self.far, (step - 1, index), self.across(step, False)).wait_recv()
            remote(got, got, self.passed, (step - 1, index), self.partner).start()

    def consume(self, chunks, use):
        far = self.count // 2 - 1
        chip, core = lax.div(self.place, 2), lax.rem(self.place, 2)

        def turn(number):
            kind, index = lax.div(number, chunks), lax.rem(number, chunks)
            step = lax.rem(kind + 2 * far - 2, max(far, 1)) + 1
            owner = lax.rem(chip - step + self.count // 2, self.count // 2) * 2
            owner = owner + jnp.where(kind < far + 2, core, 1 - core)
            owner = jnp.where(kind == 0, self.place, jnp.where(kind == 1, self.partner, owner))
            got = self.part(owner, index)

            @pl.when(kind == 1)
            def _():
                remote(got, got, self.near, (index,), self.partner).wait_recv()

            @pl.when((kind >= 2) & (kind < far + 2))
            def _():
                remote(got, got, self.far, (step - 1, index), self.across(step, False)).wait_recv()
                remote(got, got, self.passed, (step - 1, index), self.partner).start()

            @pl.when(kind >= far + 2)
            def _():
                remote(got, got, self.passed, (step - 1, index), self.partner).wait_recv()

            use(owner, index)

        each((2 * far + 2) * chunks, turn)

    def sent(self, index):
        own = self.part(self.place, index)
        remote(own, own, self.near, (index,), self.partner).wait_send()
        for step in range(1, self.count // 2):
            remote(own, own, self.far, (step - 1, index), self.across(step, False)).wait_send()
            got = self.part(self.across(-step, False), index)
            remote(got, got, self.passed, (step - 1, index), self.partner).wait_send()

    def finish(self, index):
        own = self.part(self.place, index)
        near = self.part(self.partner, index)
        remote(own, near, self.near, (index,), self.partner).wait()
        for step in range(1, self.count // 2):
            remote(own, own, self.far, (step - 1, index), self.across(step, False)).wait_send()
            got = self.part(self.across(-step, True), index)
            remote(got, got, self.passed, (step - 1, index), self.partner).wait()


def gather_sems(count, chunks):
    far = max(count // 2 - 1, 1)
    return [
        pltpu.SemaphoreType.DMA((2, chunks)),
        pltpu.SemaphoreType.DMA((2, far, chunks)),
        pltpu.SemaphoreType.DMA((2, far, chunks)),
    ]


class RowSum:
    def __init__(self, count, rows, chunk, left, weight, flipped, buffers):
        self.count, self.rows, self.chunk = count, rows, chunk
        self.left, self.weight, self.flipped = left, weight, flipped
        (self.pair_out, self.pair_in, self.far_out, self.far_in, self.near_out, self.near_in, self.own) = buffers[:7]
        self.pair, self.far, self.near = buffers[7:]
        self.place, self.partner, self.across = mesh_place(count)

    def product(self, owner, index):
        at = pl.multiple_of(owner * self.rows + index * self.chunk, self.chunk)
        rows = self.left[pl.ds(at, self.chunk), :]
        return (back_product if self.flipped else product)(rows, self.weight[...])

    def pair_copy(self, step, index):
        return remote(
            self.pair_out.at[step - 1, index], self.pair_in.at[step - 1, index],
            self.pair, (step - 1, index), self.partner,
        )

    def far_copy(self, step, index):
        return remote(
            self.far_out.at[step - 1, index], self.far_in.at[step - 1, index],
            self.far, (step - 1, index), self.across(step, False),
        )

    def near_copy(self, index):
        return remote(self.near_out.at[index], self.near_in.at[index], self.near, (index,), self.partner)

    def send(self):
        chunks, far = self.rows // self.chunk, self.count // 2 - 1
        core = lax.rem(self.place, 2)

        def turn(number):
            kind, index = lax.div(number, chunks), lax.rem(number, chunks)
            step = lax.rem(kind, max(far, 1)) + 1
            owner = lax.rem(lax.div(self.place, 2) + step, self.count // 2) * 2
            owner = owner + jnp.where(kind < far, 1 - core, core)
            owner = jnp.where(kind == 2 * far, self.partner, owner)
            owner = jnp.where(kind > 2 * far, self.place, owner)
            rows = self.product(owner, index)

            @pl.when(kind < far)
            def _():
                self.pair_out[step - 1, index] = rows.astype(BF16)
                self.pair_copy(step, index).start()

            @pl.when((kind >= far) & (kind < 2 * far))
            def _():
                self.pair_copy(step, index).wait_recv()
                self.far_out[step - 1, index] = (rows + self.pair_in[step - 1, index].astype(F32)).astype(BF16)
                self.far_copy(step, index).start()

            @pl.when(kind == 2 * far)
            def _():
                self.near_out[index] = rows.astype(BF16)
                self.near_copy(index).start()

            @pl.when(kind > 2 * far)
            def _():
                self.own[index] = rows

        each((2 * far + 2) * chunks, turn)

    def total(self, index):
        self.near_copy(index).wait_recv()
        rows = self.own[index] + self.near_in[index].astype(F32)
        for step in range(1, self.count // 2):
            self.far_copy(step, index).wait_recv()
            rows = rows + self.far_in[step - 1, index].astype(F32)
        return rows

    def finish(self, index):
        self.near_copy(index).wait_send()
        for step in range(1, self.count // 2):
            self.pair_copy(step, index).wait_send()
            self.far_copy(step, index).wait_send()


def split_copies(copies):
    inner = 1
    while (2 * inner) ** 2 <= copies:
        inner *= 2
    return copies // inner, inner


def dp_copy(source, target, send_sem, recv_sem, device):
    return pltpu.make_async_remote_copy(
        src_ref=source, dst_ref=target, send_sem=send_sem, recv_sem=recv_sem,
        device_id={"dp": device}, device_id_type=pl.DeviceIdType.MESH,
    )


class DpPlace:
    def __init__(self, copies):
        self.outer, self.inner = split_copies(copies)
        here = lax.axis_index("dp")
        self.z, self.y = lax.div(here, self.inner), lax.rem(here, self.inner)

    def along_y(self, step):
        return lax.rem(self.y + step + self.inner, self.inner)

    def along_z(self, step):
        return lax.rem(self.z + step + self.outer, self.outer)

    def device(self, z, y):
        return z * self.inner + y

    def greet(self, barrier):
        for step in range(1, self.inner):
            pl.semaphore_signal(
                barrier, inc=1, device_id={"dp": self.device(self.z, self.along_y(step))},
                device_id_type=pl.DeviceIdType.MESH,
            )
        for step in range(1, self.outer):
            pl.semaphore_signal(
                barrier, inc=1, device_id={"dp": self.device(self.along_z(step), self.y)},
                device_id_type=pl.DeviceIdType.MESH,
            )
        return self.inner + self.outer - 2


class DpReduce:
    def __init__(self, copies, source, y_in, z_out, z_in, y_sems, z_sems):
        self.at = DpPlace(copies)
        self.source, self.y_in, self.z_out, self.z_in = source, y_in, z_out, z_in
        self.y_sems, self.z_sems = y_sems, z_sems

    def y_copy(self, step, z):
        peer = self.at.along_y(step)
        return dp_copy(
            self.source.at[z, peer], self.y_in.at[step - 1, z],
            self.y_sems.at[0, step - 1, z], self.y_sems.at[1, step - 1, z], self.at.device(self.at.z, peer),
        )

    def z_copy(self, step):
        peer = self.at.along_z(step + 1)
        return dp_copy(
            self.z_out.at[step], self.z_in.at[step],
            self.z_sems.at[0, step], self.z_sems.at[1, step], self.at.device(peer, self.at.y),
        )

    def send(self):
        def start(step):
            for y_step in range(1, self.at.inner):
                self.y_copy(y_step, self.at.along_z(step + 1)).start()

        each(self.at.outer, start)

    def y_total(self, z):
        total = self.source[z, self.at.y].astype(F32)
        for y_step in range(1, self.at.inner):
            self.y_copy(y_step, z).wait_recv()
            total = total + self.y_in[y_step - 1, z].astype(F32)
        return total

    def pass_on(self, step):
        @pl.when(step < self.at.outer - 1)
        def _():
            self.z_out[step] = self.y_total(self.at.along_z(step + 1)).astype(BF16)
            self.z_copy(step).start()

    def total(self):
        total = self.y_total(self.at.z)
        for step in range(self.at.outer - 1):
            self.z_copy(step).wait_recv()
            total = total + self.z_in[step].astype(F32)
        for step in range(self.at.outer - 1):
            self.z_copy(step).wait_send()
        for y_step in range(1, self.at.inner):
            for z in range(self.at.outer):
                self.y_copy(y_step, z).wait_send()
        return total


def reduce_scratch(copies, array):
    outer, inner = split_copies(copies)
    slab = array.shape[2:]
    return [
        pltpu.VMEM((inner - 1, outer, *slab), BF16),
        pltpu.VMEM((outer - 1, *slab), BF16),
        pltpu.VMEM((outer - 1, *slab), BF16),
        pltpu.SemaphoreType.DMA((2, inner - 1, outer)),
        pltpu.SemaphoreType.DMA((2, outer - 1)),
    ]


class DpGather:
    def __init__(self, copies, slab, held, z_sems, y_sems):
        self.at = DpPlace(copies)
        self.slab, self.held, self.z_sems, self.y_sems = slab, held, z_sems, y_sems

    def z_copy(self, step, z):
        here = self.held.at[z, self.at.y]
        peer = self.at.device(self.at.along_z(step + 1), self.at.y)
        return dp_copy(here, here, self.z_sems.at[0, step], self.z_sems.at[1, step], peer)

    def y_copy(self, y_step, slot, z, y):
        here = self.held.at[z, y]
        peer = self.at.device(self.at.z, self.at.along_y(y_step))
        return dp_copy(
            here, here, self.y_sems.at[0, y_step - 1, slot], self.y_sems.at[1, y_step - 1, slot], peer
        )

    def send(self):
        self.held[self.at.z, self.at.y] = self.slab[...]
        for step in range(self.at.outer - 1):
            self.z_copy(step, self.at.z).start()
        for y_step in range(1, self.at.inner):
            self.y_copy(y_step, self.at.outer - 1, self.at.z, self.at.y).start()

    def pass_on(self, step):
        @pl.when(step < self.at.outer - 1)
        def _():
            source = self.at.along_z(-step - 1)
            self.z_copy(step, source).wait_recv()
            for y_step in range(1, self.at.inner):
                self.y_copy(y_step, step, source, self.at.y).start()

    def finish(self):
        for step in range(self.at.outer - 1):
            self.z_copy(step, self.at.z).wait_send()
        for y_step in range(1, self.at.inner):
            sender = self.at.along_y(-y_step)
            for slot in range(self.at.outer):
                source = self.at.along_z(-slot - 1)
                self.y_copy(y_step, slot, source, sender).wait_recv()
                self.y_copy(y_step, slot, source, self.at.y).wait_send()


def gather_scratch(copies):
    outer, inner = split_copies(copies)
    return [pltpu.SemaphoreType.DMA((2, outer - 1)), pltpu.SemaphoreType.DMA((2, inner - 1, outer))]


def spread(index, chunks, copies, steps):
    outer = split_copies(copies)[0]
    turns = -(-outer // chunks)

    def turn(sub):
        for step in steps:
            step(index * turns + sub)

    each(turns, turn)


def row_sum_scratch(count, rows, chunk, width):
    far, chunks = max(count // 2 - 1, 1), rows // chunk
    wide = pltpu.VMEM((far, chunks, chunk, width), BF16)
    slim = pltpu.VMEM((chunks, chunk, width), BF16)
    return [
        wide, wide, wide, wide, slim, slim, pltpu.VMEM((chunks, chunk, width), F32),
        pltpu.SemaphoreType.DMA((2, far, chunks)),
        pltpu.SemaphoreType.DMA((2, far, chunks)),
        pltpu.SemaphoreType.DMA((2, chunks)),
    ]


def rows_at(index, chunk):
    return pl.ds(pl.multiple_of(index * chunk, chunk), chunk)


def standardize(values):
    average = jnp.mean(values, axis=-1, keepdims=True)
    centered = values - average
    spread = lax.rsqrt(jnp.mean(centered * centered, axis=-1, keepdims=True) + EPSILON)
    return centered * spread, spread


def norm_backward(values, grad, gain):
    normed, spread = standardize(values)
    scaled = grad * gain
    inner = jnp.mean(scaled * normed, axis=-1, keepdims=True)
    back = (scaled - jnp.mean(scaled, axis=-1, keepdims=True) - normed * inner) * spread
    return back, grad * normed


def column_sum(values):
    return jnp.sum(values, axis=0, keepdims=True)


def open_kernel(
    count, chunk, x_ref, gain_ref, shift_ref, first_ref, weight, bias_ref, rows_ref, all_ref, packed_ref, *sems
):
    rows = x_ref.shape[0]
    place, _, _ = mesh_place(count)
    greet(count)
    chunks = rows // chunk
    main = Gather(count, rows_ref, chunk, *sems[:3])
    side_chunk = first_ref.shape[0] // 2
    side = Gather(count, all_ref, side_chunk, *sems[3:])

    def start(index):
        values = x_ref[rows_at(index, chunk), :].astype(F32)
        normed = standardize(values)[0] * gain_ref[...] + shift_ref[...]
        rows_ref[place, rows_at(index, chunk), :] = normed.astype(BF16)
        main.send(index)

    each(chunks, start)

    def side_start(index):
        all_ref[place, rows_at(index, side_chunk), :] = first_ref[rows_at(index, side_chunk), :]
        side.send(index)

    each(2, side_start)

    def use(owner, index):
        got = rows_ref[owner, rows_at(index, chunk), :]
        at = pl.ds(pl.multiple_of(owner * rows + index * chunk, chunk), chunk)
        packed_ref[at, :] = (back_product(got, weight[...]) + bias_ref[...]).astype(BF16)

    main.consume(chunks, use)
    each(2, side.hand_on)
    each(chunks, main.sent)
    each(2, side.finish)


def attend_out_kernel(
    count, chunk, left, weight, x_ref, bias_ref, gain_ref, shift_ref, up_ref, up_bias_ref,
    rows_ref, residual_ref, pre_ref, hidden_ref, *scratch
):
    rows = x_ref.shape[0]
    place, _, _ = mesh_place(count)
    greet(count)
    chunks = rows // chunk
    summed = RowSum(count, rows, chunk, left, weight, False, scratch[:10])
    main = Gather(count, rows_ref, chunk, *scratch[10:])
    summed.send()

    def close(index):
        at = rows_at(index, chunk)
        values = x_ref[at, :].astype(F32) + summed.total(index) + bias_ref[...]
        residual_ref[at, :] = values
        normed = standardize(values)[0] * gain_ref[...] + shift_ref[...]
        rows_ref[place, at, :] = normed.astype(BF16)
        main.send(index)

    each(chunks, close)

    def use(owner, index):
        got = rows_ref[owner, rows_at(index, chunk), :]
        at = pl.ds(pl.multiple_of(owner * rows + index * chunk, chunk), chunk)
        pre = product(got, up_ref[...]) + up_bias_ref[...]
        pre_ref[at, :] = pre
        hidden_ref[at, :] = gelu_tanh(pre).astype(BF16)

    main.consume(chunks, use)
    each(chunks, main.sent)
    each(chunks, summed.finish)


def mlp_back_kernel(
    count, chunk, left, weight, residual_ref, dy_ref, gain_ref, out_weight_ref, mixed_ref,
    grad_ref, sums_ref, mixed_grad_ref, weight_grad_ref, rows_ref, weight_sum, *scratch
):
    rows = residual_ref.shape[0]
    place, _, _ = mesh_place(count)
    greet(count)
    chunks = rows // chunk
    summed = RowSum(count, rows, chunk, left, weight, True, scratch[:10])
    main = Gather(count, rows_ref, chunk, *scratch[10:])
    sums_ref[...] = jnp.zeros_like(sums_ref)
    summed.send()

    def close(index):
        at = rows_at(index, chunk)
        total = summed.total(index)
        dy = dy_ref[at, :].astype(F32)
        back, per_gain = norm_backward(residual_ref[at, :], total, gain_ref[...])
        grad = dy + back
        grad_ref[at, :] = grad
        rows_ref[place, at, :] = grad.astype(BF16)
        main.send(index)
        sums_ref[0:1, :] += column_sum(per_gain)
        sums_ref[1:2, :] += column_sum(total)
        sums_ref[2:3, :] += column_sum(grad)
        sums_ref[3:4, :] += column_sum(dy)

    each(chunks, close)
    weight_sum[...] = jnp.zeros_like(weight_sum)

    def use(owner, index):
        got = rows_ref[owner, rows_at(index, chunk), :]
        at = pl.ds(pl.multiple_of(owner * rows + index * chunk, chunk), chunk)
        mixed_grad_ref[at, :] = back_product(got, out_weight_ref[...]).astype(BF16)
        weight_sum[...] += rows_product(mixed_ref[at, :], got)

    main.consume(chunks, use)
    weight_grad_ref[...] = weight_sum[...].astype(BF16)
    each(chunks, main.sent)
    each(chunks, summed.finish)


def input_back_kernel(
    count, copies, chunk, left, weight, x_ref, grad_ref, gain_ref, qkv_ref, outw_ref,
    out_ref, sums_ref, qkv_slab, outw_slab, *scratch
):
    rows = x_ref.shape[0]
    greet(count, copies)
    chunks = rows // chunk
    summed = RowSum(count, rows, chunk, left, weight, False, scratch[:10])
    outw = DpReduce(copies, outw_ref, *scratch[10:15])
    qkv = DpReduce(copies, qkv_ref, *scratch[15:20])
    qkv.send()
    outw.send()
    sums_ref[...] = jnp.zeros_like(sums_ref)
    summed.send()

    def close(index):
        at = rows_at(index, chunk)
        total = summed.total(index)
        back, per_gain = norm_backward(x_ref[at, :].astype(F32), total, gain_ref[...])
        out_ref[at, :] = (grad_ref[at, :] + back).astype(BF16)
        sums_ref[0:1, :] += column_sum(per_gain)
        sums_ref[1:2, :] += column_sum(total)
        spread(index, chunks, copies, [qkv.pass_on, outw.pass_on])

    each(chunks, close)
    qkv_slab[...] = qkv.total().astype(BF16)
    outw_slab[...] = outw.total().astype(BF16)
    each(chunks, summed.finish)


def closing_kernel(
    count, copies, shared, pairs, owner, small_ref, skip_ref, qkv_slab, outw_slab,
    small_out, first_ref, qkv_ref, outw_ref, all_ref, *scratch
):
    copy, place = lax.axis_index("dp"), lax.axis_index("mp")
    barrier = pltpu.get_barrier_semaphore()
    for step in range(1, copies):
        pl.semaphore_signal(
            barrier, inc=1, device_id={"dp": lax.rem(copy + step, copies)}, device_id_type=pl.DeviceIdType.MESH
        )
    for step in range(1, count):
        pl.semaphore_signal(
            barrier, inc=1, device_id={"mp": lax.rem(place + step, count)}, device_id_type=pl.DeviceIdType.MESH
        )
    pl.semaphore_wait(barrier, copies + count - 2)
    side_chunk = skip_ref.shape[0] // 2
    side = Gather(count, all_ref, side_chunk, *scratch[0:3])
    qkv = DpGather(copies, qkv_slab, qkv_ref, *scratch[3:5])
    outw = DpGather(copies, outw_slab, outw_ref, *scratch[5:7])
    copy_in, part_in, part_out, copy_sems, part_sems = scratch[7:]

    def small_copy(axis, own, size, source, slots, sems, step, slot):
        return pltpu.make_async_remote_copy(
            src_ref=source, dst_ref=slots.at[slot], send_sem=sems.at[0, step], recv_sem=sems.at[1, slot],
            device_id={axis: lax.rem(own + step, size)}, device_id_type=pl.DeviceIdType.MESH,
        )

    def small_start(axis, own, size, source, slots, sems):
        slots[own] = source[...]
        for step in range(1, size):
            small_copy(axis, own, size, source, slots, sems, step, own).start()

    def small_total(axis, own, size, source, slots, sems):
        for step in range(1, size):
            slot = lax.rem(own + size - step, size)
            small_copy(axis, own, size, source, slots, sems, step, slot).wait_recv()
            small_copy(axis, own, size, source, slots, sems, step, own).wait_send()
        total = slots[0]
        for slot in range(1, size):
            total = total + slots[slot]
        return total

    over_copies = ("dp", copy, copies, small_ref, copy_in, copy_sems)
    over_parts = ("mp", place, count, part_out, part_in, part_sems)
    small_start(*over_copies)
    qkv.send()
    outw.send()
    part_out[...] = small_total(*over_copies)
    small_start(*over_parts)

    def side_start(index):
        all_ref[place, rows_at(index, side_chunk), :] = skip_ref[rows_at(index, side_chunk), :]
        side.send(index)

    each(2, side_start)

    def pass_on(index):
        qkv.pass_on(index)
        outw.pass_on(index)

    each(qkv.at.outer, pass_on)
    each(2, side.hand_on)
    every = small_total(*over_parts)
    row = lax.broadcasted_iota(jnp.int32, every.shape, 0)
    small_out[...] = jnp.where(row < shared, every, part_out[...])
    each(2, side.finish)
    width = skip_ref.shape[1] // pairs
    for slot in range(pairs):
        user = user_of(owner, place * pairs + slot)
        held = all_ref[lax.div(user, pairs)]
        value = held[:, 0:width]
        for part in range(1, pairs):
            value = jnp.where(lax.rem(user, pairs) == part, held[:, part * width : (part + 1) * width], value)
        first_ref[:, slot * width : (slot + 1) * width] = value
    outw.finish()
    qkv.finish()


def user_of(owner, head):
    user = jnp.int32(0)
    for pair in range(owner.shape[0]):
        user = jnp.maximum(user, jnp.where(owner[pair] == head, pair, 0))
    return user


def call(kernel, number, inputs, outputs, scratch, flops, scalars=0):
    moved = sum(a.size * a.dtype.itemsize for a in (*inputs, *outputs))
    return pl.pallas_call(
        kernel,
        out_shape=outputs,
        in_specs=[pl.BlockSpec(memory_space=pltpu.SMEM)] * scalars
        + [pl.BlockSpec(memory_space=pltpu.VMEM)] * (len(inputs) - scalars),
        out_specs=[pl.BlockSpec(memory_space=pltpu.VMEM)] * len(outputs),
        scratch_shapes=scratch,
        compiler_params=pltpu.CompilerParams(collective_id=number, has_side_effects=True),
        cost_estimate=pl.CostEstimate(flops=flops, bytes_accessed=moved, transcendentals=0),
    )(*inputs)


def like(shape, kind):
    return jax.ShapeDtypeStruct(shape, kind)


def body(
    inputs,
    first_values,
    cotangent,
    seq_lengths,
    value_owner,
    attn_norm_gain,
    attn_norm_bias,
    qkv_weight,
    qv_bias,
    out_weight,
    out_bias,
    mlp_norm_gain,
    mlp_norm_bias,
    up_weight,
    up_bias,
    down_weight,
    down_bias,
):
    local_rows, model_width = inputs.shape
    group_rows = local_rows * lax.axis_size("mp")
    pairs_dev, head_size = qkv_weight.shape[1], qkv_weight.shape[3]
    seats = (seq_lengths, value_owner, lax.axis_index("mp").reshape(1).astype(jnp.int32))
    copies = lax.axis_size("dp")

    qkv_pack = jnp.pad(jnp.transpose(qkv_weight, (1, 2, 3, 0)), ((0, 0), (0, 1), (0, 0), (0, 0)))
    qkv_pack = qkv_pack.reshape(pairs_dev * PACK * head_size, model_width)
    bias_pack = jnp.concatenate(
        [qv_bias[:, 0:2], jnp.zeros_like(qv_bias[:, 0:2]), qv_bias[:, 2:3], jnp.zeros_like(qv_bias[:, 2:3])],
        axis=1,
    ).reshape(1, pairs_dev * PACK * head_size)
    out_flat = out_weight.reshape(pairs_dev * 2 * head_size, model_width)

    count = lax.axis_size("mp")
    chunk = min(128, local_rows)
    chunks = local_rows // chunk
    row = (1, model_width)
    whole = (count, local_rows, model_width)
    slim = pairs_dev * head_size
    sum_scratch = row_sum_scratch(count, local_rows, chunk, model_width)
    main_sems, side_sems = gather_sems(count, chunks), gather_sems(count, 2)
    dense = 2 * group_rows * model_width

    packs = pairs_dev * PACK * head_size
    rows_one, all_first, packed = call(
        functools.partial(open_kernel, count, chunk), 0,
        (inputs, attn_norm_gain.reshape(row), attn_norm_bias.reshape(row), first_values.reshape(group_rows, slim),
         qkv_pack, bias_pack),
        [like(whole, BF16), like((count, group_rows, slim), BF16), like((group_rows, packs), BF16)],
        main_sems + side_sems, dense * packs,
    )
    rows_one = rows_one.reshape(group_rows, model_width)
    cotangent_late = lax.optimization_barrier((cotangent, rows_one))[0]
    grad_rows = lax.all_gather(cotangent_late, "mp", axis=0, tiled=True)
    mixed, totals = attend_forward(*seats, packed, all_first)
    units = up_bias.shape[0]
    rows_two, residual, hidden_pre, hidden = call(
        functools.partial(attend_out_kernel, count, chunk), 1,
        (mixed, out_flat, inputs, out_bias.reshape(row), mlp_norm_gain.reshape(row), mlp_norm_bias.reshape(row),
         up_weight, up_bias.reshape(1, units)),
        [like(whole, BF16), like(inputs.shape, F32), like((group_rows, units), F32), like((group_rows, units), BF16)],
        sum_scratch + main_sems, dense * (256 + units),
    )
    rows_two = rows_two.reshape(group_rows, model_width)
    grad_hidden = back_product(grad_rows, down_weight)
    grad_pre = jax.vjp(gelu_tanh, hidden_pre)[1](grad_hidden)[0].astype(BF16)
    grad_down_weight = rows_product(hidden, grad_rows).astype(BF16)
    grad_up_weight = rows_product(rows_two, grad_pre).astype(BF16)
    grad_up_bias = jnp.sum(grad_pre.astype(F32), axis=0)
    outer, inner = split_copies(copies)

    def sliced(values):
        return values.reshape(outer, inner, values.shape[0] // copies, values.shape[1])

    late = (grad_up_weight, grad_down_weight)
    grad_pre, late = lax.optimization_barrier((grad_pre, late))
    late_sums = lax.psum(late, "dp")
    grad_residual, sums_two, grad_mixed, grad_out_weight = call(
        functools.partial(mlp_back_kernel, count, chunk), 2,
        (grad_pre, up_weight, residual, cotangent, mlp_norm_gain.reshape(row), out_flat, mixed),
        [like(inputs.shape, F32), like((8, model_width), F32), like(mixed.shape, BF16), like(out_flat.shape, BF16)],
        [pltpu.VMEM(whole, BF16), pltpu.VMEM(out_flat.shape, F32)] + sum_scratch + main_sems,
        dense * up_bias.shape[0],
    )
    grad_flat, grad_skip, pack_sums, output = call(
        functools.partial(attend_backward_kernel, count, chunk, pairs_dev), 5,
        (seq_lengths, value_owner, packed, all_first, grad_mixed, totals, hidden, down_weight, residual,
         down_bias.reshape(row)),
        [like((group_rows, packs), BF16), like((group_rows, slim), BF16), like((8, packs), F32),
         like(inputs.shape, BF16)],
        [pltpu.VMEM((group_rows, LANES), F32), pltpu.VMEM((group_rows, LANES), F32),
         pltpu.VMEM((group_rows, LANES), BF16)] + sum_scratch,
        group_rows * 1024 * 256 * 10 * pairs_dev, scalars=2,
    )
    pack_sums = pack_sums[0].reshape(pairs_dev, PACK, head_size)
    grad_qv_bias = jnp.concatenate([pack_sums[:, 0:2], pack_sums[:, 4:5]], axis=1)
    grad_qkv_weight = rows_product(grad_flat, rows_one).astype(BF16)
    grad_qkv_weight = grad_qkv_weight.reshape(pairs_dev, PACK, head_size, model_width)[:, 0:5]
    grad_qkv_weight = sliced(grad_qkv_weight.reshape(pairs_dev * 5 * head_size, model_width))
    grad_out_weight = sliced(grad_out_weight)
    grad_inputs, sums_one, qkv_slab, out_slab = call(
        functools.partial(input_back_kernel, count, copies, chunk), 3,
        (grad_flat, qkv_pack, inputs, grad_residual, attn_norm_gain.reshape(row), grad_qkv_weight, grad_out_weight),
        [like(inputs.shape, BF16), like((8, model_width), F32),
         like(grad_qkv_weight.shape[2:], BF16), like(grad_out_weight.shape[2:], BF16)],
        sum_scratch + reduce_scratch(copies, grad_out_weight) + reduce_scratch(copies, grad_qkv_weight),
        dense * packs,
    )
    wide_bias = jnp.pad(grad_up_bias, (0, model_width - grad_up_bias.shape[0])).reshape(row)
    slim_bias = jnp.pad(grad_qv_bias.reshape(-1), (0, model_width - grad_qv_bias.size)).reshape(row)
    own_sums = jnp.concatenate([sums_two[0:4], sums_one[0:2], wide_bias, slim_bias], axis=0)
    block = pltpu.VMEM(own_sums.shape, F32)
    small, grad_first, qkv_sum, out_sum = call(
        functools.partial(closing_kernel, count, copies, 6, pairs_dev), 4,
        (value_owner, own_sums, grad_skip, qkv_slab, out_slab),
        [like(own_sums.shape, F32), like((group_rows, slim), BF16),
         like(grad_qkv_weight.shape, BF16), like(grad_out_weight.shape, BF16)],
        [pltpu.VMEM((count, group_rows, slim), BF16)]
        + side_sems + gather_scratch(copies) + gather_scratch(copies)
        + [pltpu.VMEM((copies, *own_sums.shape), F32), pltpu.VMEM((count, *own_sums.shape), F32), block,
           pltpu.SemaphoreType.DMA((2, copies)), pltpu.SemaphoreType.DMA((2, count))],
        own_sums.size * (copies + count), scalars=1,
    )
    qkv_sum = qkv_sum.reshape(pairs_dev, 5, head_size, model_width).astype(F32)
    qkv_sum = jnp.transpose(qkv_sum, (3, 0, 1, 2))
    late_sums = (*(part.astype(F32) for part in late_sums), out_sum.reshape(out_weight.shape).astype(F32))
    grad_first = grad_first.reshape(group_rows, pairs_dev, head_size)
    norm_sums = (small[4], small[5], small[2], small[0], small[1], small[3])
    bias_sums = (small[7, : grad_qv_bias.size].reshape(qv_bias.shape), small[6, : grad_up_bias.shape[0]])

    return (
        output,
        grad_inputs,
        grad_first,
        norm_sums[0],
        norm_sums[1],
        qkv_sum,
        bias_sums[0],
        late_sums[2],
        norm_sums[2],
        norm_sums[3],
        norm_sums[4],
        late_sums[0],
        bias_sums[1],
        late_sums[1],
        norm_sums[5],
    )


def solution(mesh):
    return jax.shard_map(
        body,
        mesh=mesh,
        in_specs=(
            P(("dp", "mp"), None),
            P("dp", "mp", None),
            P(("dp", "mp"), None),
            P("dp"),
            P(),
            P(),
            P(),
            P(None, "mp", None, None),
            P("mp", None, None),
            P("mp", None, None, None),
            P(),
            P(),
            P(),
            P(None, "mp"),
            P("mp"),
            P("mp", None),
            P(),
        ),
        out_specs=(
            P(("dp", "mp"), None),
            P(("dp", "mp"), None),
            P("dp", "mp", None),
            P(),
            P(),
            P(None, "mp", None, None),
            P("mp", None, None),
            P("mp", None, None, None),
            P(),
            P(),
            P(),
            P(None, "mp"),
            P("mp"),
            P("mp", None),
            P(),
        ),
        check_vma=False,
    )
```

```python
import functools

import jax
import jax.numpy as jnp
from jax import lax
from jax.experimental import pallas as pl
from jax.experimental.pallas import tpu as pltpu
from jax.sharding import PartitionSpec as P


SHORT = 512
QROWS = 256
LANES = 128
PACK = 6

EPSILON = 1e-05
MASKED = -1e30
GELU_C = 0.7978845608028654
BF16 = jnp.bfloat16
F32 = jnp.float32


def gelu_tanh(values):
    return 0.5 * values * (1.0 + jnp.tanh(GELU_C * (values + 0.044715 * values * values * values)))


def rows_product(left, right):
    return lax.dot_general(left, right, (((0,), (0,)), ((), ())), preferred_element_type=F32)


def back_product(left, weight):
    return lax.dot_general(left, weight, (((1,), (1,)), ((), ())), preferred_element_type=F32)


def product(left, right):
    return jnp.dot(left, right, preferred_element_type=F32)


def opens_at(lengths, row):
    begin, opens = jnp.int32(0), jnp.int32(0)
    for slot in range(lengths.shape[0]):
        opens = jnp.maximum(opens, jnp.where(begin == row, 1, 0))
        begin = begin + lengths[slot]
    return opens


def head_lanes(head):
    lane = lax.broadcasted_iota(jnp.int32, (1, LANES), 1)
    return (lane < LANES // 2) if head == 0 else (lane >= LANES // 2)


def causal_tile():
    row = lax.broadcasted_iota(jnp.int32, (QROWS, QROWS), 0)
    column = lax.broadcasted_iota(jnp.int32, (QROWS, QROWS), 1)
    return column <= row


def pick_values(half, fresh, held, value_ref):
    if held.shape[1] < LANES:
        turned = jnp.concatenate([held, held], axis=1)
    else:
        turned = jnp.concatenate([held[:, LANES // 2 :], held[:, : LANES // 2]], axis=1)
        turned = jnp.where(half == 1, held, turned)
    value_ref[...] = jnp.where(head_lanes(0), fresh, turned)


def attend_forward_kernel(pairs, lengths, owner, place, qkv_ref, first_ref, mixed_ref, totals_ref, value_ref):
    half = lax.rem(owner[place[0] * pairs + pl.program_id(0)], pairs)
    pick_values(half, qkv_ref[:, 2 * LANES : 3 * LANES], first_ref[0], value_ref)
    blocks = qkv_ref.shape[0] // SHORT
    scale = (LANES // 2) ** (-0.5)

    def block(index, carried):
        base = pl.multiple_of(index * SHORT, SHORT)
        for half in range(SHORT // QROWS):
            first = base + half * QROWS

            def attend(with_previous):
                query = qkv_ref[pl.ds(first, QROWS), 0:LANES] * jnp.asarray(scale, BF16)
                spans = []
                if with_previous:
                    spans.append((base - SHORT, SHORT))
                if half:
                    spans.append((base, half * QROWS))
                spans.append((first, QROWS))
                mixed = jnp.zeros((QROWS, LANES), F32)
                totals = []
                for head in range(2):
                    chosen = head_lanes(head)
                    query_head = jnp.where(chosen, query, jnp.zeros_like(query))
                    scores = [
                        back_product(query_head, qkv_ref[pl.ds(at, size), LANES : 2 * LANES])
                        for at, size in spans
                    ]
                    scores[-1] = jnp.where(causal_tile(), scores[-1], MASKED)
                    top = scores[0].max(axis=1, keepdims=True)
                    for part in scores[1:]:
                        top = jnp.maximum(top, part.max(axis=1, keepdims=True))
                    total = jnp.zeros((QROWS, 1), F32)
                    gathered = jnp.zeros((QROWS, LANES), F32)
                    for (at, size), part in zip(spans, scores):
                        weights = jnp.exp(part - top)
                        total = total + weights.sum(axis=1, keepdims=True)
                        values = value_ref[pl.ds(at, size), :]
                        values = jnp.where(chosen, values, jnp.zeros_like(values))
                        gathered = gathered + product(weights.astype(BF16), values)
                    mixed = mixed + gathered / total
                    totals.append(top + jnp.log(total))
                mixed_ref[pl.ds(first, QROWS), :] = mixed.astype(BF16)
                totals_ref[pl.ds(first, QROWS), :] = jnp.where(
                    head_lanes(0), totals[0], totals[1]
                )

            @pl.when(opens_at(lengths, base) == 0)
            def _():
                attend(True)

            @pl.when(opens_at(lengths, base) == 1)
            def _():
                attend(False)

        return carried

    lax.fori_loop(0, blocks, block, 0)


def attend_backward_kernel(
    count, chunk, pairs, lengths, owner, qkv_ref, first_ref, grad_ref, totals_ref, left, weight, residual_ref, shift_ref,
    out_ref, skip_ref, sums_ref, layer_ref, key_sum, value_sum, value_ref, *scratch
):
    blocks = qkv_ref.shape[0] // SHORT
    scale = (LANES // 2) ** (-0.5)
    place, _, _ = mesh_place(count)
    greet(count)
    rows = residual_ref.shape[0]
    chunks = rows // chunk
    summed = RowSum(count, rows, chunk, left, weight, False, scratch)
    sums_ref[...] = jnp.zeros_like(sums_ref)
    summed.send()

    def one_pair(pair):
        column = pl.multiple_of(pair * 3 * LANES, LANES)
        side = pl.multiple_of(pair * LANES, LANES)
        query_at, key_at, fresh_at = (pl.ds(column + part * LANES, LANES) for part in range(3))
        used = owner[place * pairs + pair]
        held = first_ref[lax.div(used, pairs)]
        pick_values(lax.rem(used, pairs), qkv_ref[:, fresh_at], held, value_ref)
        key_sum[...] = jnp.zeros_like(key_sum)
        value_sum[...] = jnp.zeros_like(value_sum)

        def block(index):
            base = pl.multiple_of(index * SHORT, SHORT)
            joined = opens_at(lengths, base) == 0

            def attend(half, with_previous):
                first = base + half * QROWS
                query = qkv_ref[pl.ds(first, QROWS), query_at] * jnp.asarray(scale, BF16)
                grad = grad_ref[pl.ds(first, QROWS), pl.ds(side, LANES)]
                spans = []
                if with_previous:
                    spans.append((base - SHORT, SHORT))
                if half:
                    spans.append((base, half * QROWS))
                spans.append((first, QROWS))
                grad_query = jnp.zeros((QROWS, LANES), F32)
                both = totals_ref[pl.ds(first, QROWS), pl.ds(side, LANES)]
                for head in range(2):
                    chosen = head_lanes(head)
                    query_head = jnp.where(chosen, query, jnp.zeros_like(query))
                    grad_head = jnp.where(chosen, grad, jnp.zeros_like(grad))
                    at_lane = head * (LANES // 2)
                    totals = both[:, at_lane : at_lane + 1]
                    probs, grads = [], []
                    inner = jnp.zeros((QROWS, 1), F32)
                    for number, (at, size) in enumerate(spans):
                        keys = qkv_ref[pl.ds(at, size), key_at]
                        part = jnp.exp(back_product(query_head, keys) - totals)
                        if number == len(spans) - 1:
                            part = jnp.where(causal_tile(), part, 0.0)
                        elif with_previous and number == 0:
                            part = jnp.where(joined, part, 0.0)
                        values = value_ref[pl.ds(at, size), :]
                        weighted = part * back_product(grad_head, values)
                        inner = inner + weighted.sum(axis=1, keepdims=True)
                        probs.append(part)
                        grads.append(weighted)
                    for (at, size), part, weighted in zip(spans, probs, grads):
                        keys = qkv_ref[pl.ds(at, size), key_at]
                        keys = jnp.where(chosen, keys, jnp.zeros_like(keys))
                        grad_scores = (weighted - part * inner).astype(BF16)
                        grad_query = grad_query + product(grad_scores, keys)
                        key_sum[pl.ds(at, size), :] += rows_product(grad_scores, query_head)
                        value_sum[pl.ds(at, size), :] += rows_product(part.astype(BF16), grad_head)
                out_ref[pl.ds(first, QROWS), query_at] = (grad_query * scale).astype(BF16)

            for half in range(SHORT // QROWS):

                @pl.when(index > 0)
                def _():
                    attend(half, True)

                @pl.when(index == 0)
                def _():
                    attend(half, False)

        each(blocks, block)
        out_ref[:, key_at] = key_sum[...].astype(BF16)
        out_ref[:, fresh_at] = value_sum[...].astype(BF16)
        for slot in range(pairs):

            @pl.when(pair == slot)
            def _():
                width = LANES // 2
                skip_ref[:, slot * width : (slot + 1) * width] = value_sum[:, width:].astype(BF16)

        for at in (query_at, fresh_at):
            sums_ref[0:1, at] = column_sum(out_ref[:, at].astype(F32))

    each(pairs, one_pair)

    def close(index):
        at = rows_at(index, chunk)
        layer_ref[at, :] = (residual_ref[at, :] + summed.total(index) + shift_ref[...]).astype(BF16)

    each(chunks, close)
    each(chunks, summed.finish)


def attend_forward(lengths, owner, place, packed, firsts):
    rows, pairs = packed.shape[0], packed.shape[1] // (3 * LANES)
    return pl.pallas_call(
        functools.partial(attend_forward_kernel, pairs),
        grid_spec=pltpu.PrefetchScalarGridSpec(
            num_scalar_prefetch=3,
            grid=(pairs,),
            in_specs=[
                pl.BlockSpec((rows, 3 * LANES), lambda p, c, o, m: (0, p)),
                pl.BlockSpec((1, rows, firsts.shape[2]), lambda p, c, o, m: (lax.div(o[m[0] * pairs + p], pairs), 0, 0)),
            ],
            out_specs=[
                pl.BlockSpec((rows, LANES), lambda p, c, o, m: (0, p)),
                pl.BlockSpec((rows, LANES), lambda p, c, o, m: (0, p)),
            ],
            scratch_shapes=[pltpu.VMEM((rows, LANES), BF16)],
        ),
        out_shape=[
            jax.ShapeDtypeStruct((rows, pairs * LANES), BF16),
            jax.ShapeDtypeStruct((rows, pairs * LANES), F32),
        ],
        cost_estimate=pl.CostEstimate(
            flops=rows * 1024 * 256 * 4 * pairs, bytes_accessed=8 << 20, transcendentals=rows * 2048
        ),
        name="attend_forward",
    )(lengths, owner, place, packed, firsts)


def mesh_place(count):
    place = lax.axis_index("mp")
    core = lax.rem(place, 2)
    chip = lax.div(place, 2)
    chips = count // 2

    def across(step, other):
        return lax.rem(chip + step + chips, chips) * 2 + (1 - core if other else core)

    return place, place + 1 - 2 * core, across


def remote(source, target, sems, index, device):
    return pltpu.make_async_remote_copy(
        src_ref=source,
        dst_ref=target,
        send_sem=sems.at[(0, *index)],
        recv_sem=sems.at[(1, *index)],
        device_id={"mp": device},
        device_id_type=pl.DeviceIdType.MESH,
    )


def greet(count, copies=0):
    _, partner, across = mesh_place(count)
    barrier = pltpu.get_barrier_semaphore()
    for device in [partner] + [across(step, False) for step in range(1, count // 2)]:
        pl.semaphore_signal(
            barrier, inc=1, device_id={"mp": device}, device_id_type=pl.DeviceIdType.MESH
        )
    others = DpPlace(copies).greet(barrier) if copies else 0
    pl.semaphore_wait(barrier, count // 2 + others)


def each(count, step):
    def run(index, carried):
        step(index)
        return carried

    lax.fori_loop(0, count, run, 0)


class Gather:
    def __init__(self, count, out_ref, chunk, near, far, passed):
        self.count, self.out, self.chunk = count, out_ref, chunk
        self.near, self.far, self.passed = near, far, passed
        self.place, self.partner, self.across = mesh_place(count)

    def part(self, owner, index):
        return self.out.at[owner, pl.ds(pl.multiple_of(index * self.chunk, self.chunk), self.chunk), :]

    def send(self, index):
        own = self.part(self.place, index)
        for step in range(1, self.count // 2):
            remote(own, own, self.far, (step - 1, index), self.across(step, False)).start()
        remote(own, own, self.near, (index,), self.partner).start()

    def hand_on(self, index):
        for step in range(1, self.count // 2):
            got = self.part(self.across(-step, False), index)
            remote(got, got, self.far, (step - 1, index), self.across(step, False)).wait_recv()
            remote(got, got, self.passed, (step - 1, index), self.partner).start()

    def consume(self, chunks, use):
        far = self.count // 2 - 1
        chip, core = lax.div(self.place, 2), lax.rem(self.place, 2)

        def turn(number):
            kind, index = lax.div(number, chunks), lax.rem(number, chunks)
            step = lax.rem(kind + 2 * far - 2, max(far, 1)) + 1
            owner = lax.rem(chip - step + self.count // 2, self.count // 2) * 2
            owner = owner + jnp.where(kind < far + 2, core, 1 - core)
            owner = jnp.where(kind == 0, self.place, jnp.where(kind == 1, self.partner, owner))
            got = self.part(owner, index)

            @pl.when(kind == 1)
            def _():
                remote(got, got, self.near, (index,), self.partner).wait_recv()

            @pl.when((kind >= 2) & (kind < far + 2))
            def _():
                remote(got, got, self.far, (step - 1, index), self.across(step, False)).wait_recv()
                remote(got, got, self.passed, (step - 1, index), self.partner).start()

            @pl.when(kind >= far + 2)
            def _():
                remote(got, got, self.passed, (step - 1, index), self.partner).wait_recv()

            use(owner, index)

        each((2 * far + 2) * chunks, turn)

    def sent(self, index):
        own = self.part(self.place, index)
        remote(own, own, self.near, (index,), self.partner).wait_send()
        for step in range(1, self.count // 2):
            remote(own, own, self.far, (step - 1, index), self.across(step, False)).wait_send()
            got = self.part(self.across(-step, False), index)
            remote(got, got, self.passed, (step - 1, index), self.partner).wait_send()

    def finish(self, index):
        own = self.part(self.place, index)
        near = self.part(self.partner, index)
        remote(own, near, self.near, (index,), self.partner).wait()
        for step in range(1, self.count // 2):
            remote(own, own, self.far, (step - 1, index), self.across(step, False)).wait_send()
            got = self.part(self.across(-step, True), index)
            remote(got, got, self.passed, (step - 1, index), self.partner).wait()


def gather_sems(count, chunks):
    far = max(count // 2 - 1, 1)
    return [
        pltpu.SemaphoreType.DMA((2, chunks)),
        pltpu.SemaphoreType.DMA((2, far, chunks)),
        pltpu.SemaphoreType.DMA((2, far, chunks)),
    ]


class RowSum:
    def __init__(self, count, rows, chunk, left, weight, flipped, buffers):
        self.count, self.rows, self.chunk = count, rows, chunk
        self.left, self.weight, self.flipped = left, weight, flipped
        (self.pair_out, self.pair_in, self.far_out, self.far_in, self.near_out, self.near_in, self.own) = buffers[:7]
        self.pair, self.far, self.near = buffers[7:]
        self.place, self.partner, self.across = mesh_place(count)

    def product(self, owner, index):
        at = pl.multiple_of(owner * self.rows + index * self.chunk, self.chunk)
        rows = self.left[pl.ds(at, self.chunk), :]
        return (back_product if self.flipped else product)(rows, self.weight[...])

    def pair_copy(self, step, index):
        return remote(
            self.pair_out.at[step - 1, index], self.pair_in.at[step - 1, index],
            self.pair, (step - 1, index), self.partner,
        )

    def far_copy(self, step, index):
        return remote(
            self.far_out.at[step - 1, index], self.far_in.at[step - 1, index],
            self.far, (step - 1, index), self.across(step, False),
        )

    def near_copy(self, index):
        return remote(self.near_out.at[index], self.near_in.at[index], self.near, (index,), self.partner)

    def send(self):
        chunks, far = self.rows // self.chunk, self.count // 2 - 1
        core = lax.rem(self.place, 2)

        def turn(number):
            kind, index = lax.div(number, chunks), lax.rem(number, chunks)
            step = lax.rem(kind, max(far, 1)) + 1
            owner = lax.rem(lax.div(self.place, 2) + step, self.count // 2) * 2
            owner = owner + jnp.where(kind < far, 1 - core, core)
            owner = jnp.where(kind == 2 * far, self.partner, owner)
            owner = jnp.where(kind > 2 * far, self.place, owner)
            rows = self.product(owner, index)

            @pl.when(kind < far)
            def _():
                self.pair_out[step - 1, index] = rows.astype(BF16)
                self.pair_copy(step, index).start()

            @pl.when((kind >= far) & (kind < 2 * far))
            def _():
                self.pair_copy(step, index).wait_recv()
                self.far_out[step - 1, index] = (rows + self.pair_in[step - 1, index].astype(F32)).astype(BF16)
                self.far_copy(step, index).start()

            @pl.when(kind == 2 * far)
            def _():
                self.near_out[index] = rows.astype(BF16)
                self.near_copy(index).start()

            @pl.when(kind > 2 * far)
            def _():
                self.own[index] = rows

        each((2 * far + 2) * chunks, turn)

    def total(self, index):
        self.near_copy(index).wait_recv()
        rows = self.own[index] + self.near_in[index].astype(F32)
        for step in range(1, self.count // 2):
            self.far_copy(step, index).wait_recv()
            rows = rows + self.far_in[step - 1, index].astype(F32)
        return rows

    def finish(self, index):
        self.near_copy(index).wait_send()
        for step in range(1, self.count // 2):
            self.pair_copy(step, index).wait_send()
            self.far_copy(step, index).wait_send()


def split_copies(copies):
    inner = 1
    while (2 * inner) ** 2 <= copies:
        inner *= 2
    return copies // inner, inner


def dp_copy(source, target, send_sem, recv_sem, device):
    return pltpu.make_async_remote_copy(
        src_ref=source, dst_ref=target, send_sem=send_sem, recv_sem=recv_sem,
        device_id={"dp": device}, device_id_type=pl.DeviceIdType.MESH,
    )


class DpPlace:
    def __init__(self, copies):
        self.outer, self.inner = split_copies(copies)
        here = lax.axis_index("dp")
        self.z, self.y = lax.div(here, self.inner), lax.rem(here, self.inner)

    def along_y(self, step):
        return lax.rem(self.y + step + self.inner, self.inner)

    def along_z(self, step):
        return lax.rem(self.z + step + self.outer, self.outer)

    def device(self, z, y):
        return z * self.inner + y

    def greet(self, barrier):
        for step in range(1, self.inner):
            pl.semaphore_signal(
                barrier, inc=1, device_id={"dp": self.device(self.z, self.along_y(step))},
                device_id_type=pl.DeviceIdType.MESH,
            )
        for step in range(1, self.outer):
            pl.semaphore_signal(
                barrier, inc=1, device_id={"dp": self.device(self.along_z(step), self.y)},
                device_id_type=pl.DeviceIdType.MESH,
            )
        return self.inner + self.outer - 2


class DpReduce:
    def __init__(self, copies, source, y_in, z_out, z_in, y_sems, z_sems):
        self.at = DpPlace(copies)
        self.source, self.y_in, self.z_out, self.z_in = source, y_in, z_out, z_in
        self.y_sems, self.z_sems = y_sems, z_sems

    def y_copy(self, step, z):
        peer = self.at.along_y(step)
        return dp_copy(
            self.source.at[z, peer], self.y_in.at[step - 1, z],
            self.y_sems.at[0, step - 1, z], self.y_sems.at[1, step - 1, z], self.at.device(self.at.z, peer),
        )

    def z_copy(self, step):
        peer = self.at.along_z(step + 1)
        return dp_copy(
            self.z_out.at[step], self.z_in.at[step],
            self.z_sems.at[0, step], self.z_sems.at[1, step], self.at.device(peer, self.at.y),
        )

    def send(self):
        def start(step):
            for y_step in range(1, self.at.inner):
                self.y_copy(y_step, self.at.along_z(step + 1)).start()

        each(self.at.outer, start)

    def y_total(self, z):
        total = self.source[z, self.at.y].astype(F32)
        for y_step in range(1, self.at.inner):
            self.y_copy(y_step, z).wait_recv()
            total = total + self.y_in[y_step - 1, z].astype(F32)
        return total

    def pass_on(self, step):
        @pl.when(step < self.at.outer - 1)
        def _():
            self.z_out[step] = self.y_total(self.at.along_z(step + 1)).astype(BF16)
            self.z_copy(step).start()

    def total(self):
        total = self.y_total(self.at.z)
        for step in range(self.at.outer - 1):
            self.z_copy(step).wait_recv()
            total = total + self.z_in[step].astype(F32)
        for step in range(self.at.outer - 1):
            self.z_copy(step).wait_send()
        for y_step in range(1, self.at.inner):
            for z in range(self.at.outer):
                self.y_copy(y_step, z).wait_send()
        return total


def reduce_scratch(copies, array):
    outer, inner = split_copies(copies)
    slab = array.shape[2:]
    return [
        pltpu.VMEM((inner - 1, outer, *slab), BF16),
        pltpu.VMEM((outer - 1, *slab), BF16),
        pltpu.VMEM((outer - 1, *slab), BF16),
        pltpu.SemaphoreType.DMA((2, inner - 1, outer)),
        pltpu.SemaphoreType.DMA((2, outer - 1)),
    ]


class DpGather:
    def __init__(self, copies, slab, held, z_sems, y_sems):
        self.at = DpPlace(copies)
        self.slab, self.held, self.z_sems, self.y_sems = slab, held, z_sems, y_sems

    def z_copy(self, step, z):
        here = self.held.at[z, self.at.y]
        peer = self.at.device(self.at.along_z(step + 1), self.at.y)
        return dp_copy(here, here, self.z_sems.at[0, step], self.z_sems.at[1, step], peer)

    def y_copy(self, y_step, slot, z, y):
        here = self.held.at[z, y]
        peer = self.at.device(self.at.z, self.at.along_y(y_step))
        return dp_copy(
            here, here, self.y_sems.at[0, y_step - 1, slot], self.y_sems.at[1, y_step - 1, slot], peer
        )

    def send(self):
        self.held[self.at.z, self.at.y] = self.slab[...]
        for step in range(self.at.outer - 1):
            self.z_copy(step, self.at.z).start()
        for y_step in range(1, self.at.inner):
            self.y_copy(y_step, self.at.outer - 1, self.at.z, self.at.y).start()

    def pass_on(self, step):
        @pl.when(step < self.at.outer - 1)
        def _():
            source = self.at.along_z(-step - 1)
            self.z_copy(step, source).wait_recv()
            for y_step in range(1, self.at.inner):
                self.y_copy(y_step, step, source, self.at.y).start()

    def finish(self):
        for step in range(self.at.outer - 1):
            self.z_copy(step, self.at.z).wait_send()
        for y_step in range(1, self.at.inner):
            sender = self.at.along_y(-y_step)
            for slot in range(self.at.outer):
                source = self.at.along_z(-slot - 1)
                self.y_copy(y_step, slot, source, sender).wait_recv()
                self.y_copy(y_step, slot, source, self.at.y).wait_send()


def gather_scratch(copies):
    outer, inner = split_copies(copies)
    return [pltpu.SemaphoreType.DMA((2, outer - 1)), pltpu.SemaphoreType.DMA((2, inner - 1, outer))]


def spread(index, chunks, copies, steps):
    outer = split_copies(copies)[0]
    turns = -(-outer // chunks)

    def turn(sub):
        for step in steps:
            step(index * turns + sub)

    each(turns, turn)


def row_sum_scratch(count, rows, chunk, width):
    far, chunks = max(count // 2 - 1, 1), rows // chunk
    wide = pltpu.VMEM((far, chunks, chunk, width), BF16)
    slim = pltpu.VMEM((chunks, chunk, width), BF16)
    return [
        wide, wide, wide, wide, slim, slim, pltpu.VMEM((chunks, chunk, width), F32),
        pltpu.SemaphoreType.DMA((2, far, chunks)),
        pltpu.SemaphoreType.DMA((2, far, chunks)),
        pltpu.SemaphoreType.DMA((2, chunks)),
    ]


def rows_at(index, chunk):
    return pl.ds(pl.multiple_of(index * chunk, chunk), chunk)


def standardize(values):
    average = jnp.mean(values, axis=-1, keepdims=True)
    centered = values - average
    spread = lax.rsqrt(jnp.mean(centered * centered, axis=-1, keepdims=True) + EPSILON)
    return centered * spread, spread


def norm_backward(values, grad, gain):
    normed, spread = standardize(values)
    scaled = grad * gain
    inner = jnp.mean(scaled * normed, axis=-1, keepdims=True)
    back = (scaled - jnp.mean(scaled, axis=-1, keepdims=True) - normed * inner) * spread
    return back, grad * normed


def column_sum(values):
    return jnp.sum(values, axis=0, keepdims=True)


def open_kernel(
    count, chunk, x_ref, gain_ref, shift_ref, first_ref, weight, bias_ref, rows_ref, all_ref, packed_ref, pack_ref, *sems
):
    rows = x_ref.shape[0]
    place, _, _ = mesh_place(count)
    greet(count)
    chunks = rows // chunk
    main = Gather(count, rows_ref, chunk, *sems[:3])
    side_chunk = first_ref.shape[0] // 2
    side = Gather(count, all_ref, side_chunk, *sems[3:])

    def start(index):
        values = x_ref[rows_at(index, chunk), :].astype(F32)
        normed = standardize(values)[0] * gain_ref[...] + shift_ref[...]
        rows_ref[place, rows_at(index, chunk), :] = normed.astype(BF16)
        main.send(index)

    each(chunks, start)

    def side_start(index):
        all_ref[place, rows_at(index, side_chunk), :] = first_ref[rows_at(index, side_chunk), :]
        side.send(index)

    each(2, side_start)

    held = weight.shape[1]
    span = pack_ref.shape[0] // weight.shape[0]
    for pair in range(weight.shape[0]):
        pack_ref[pair * span : pair * span + held, :] = weight[pair]
        pack_ref[pair * span + held : (pair + 1) * span, :] = jnp.zeros((span - held, weight.shape[2]), BF16)

    def use(owner, index):
        got = rows_ref[owner, rows_at(index, chunk), :]
        at = pl.ds(pl.multiple_of(owner * rows + index * chunk, chunk), chunk)
        packed_ref[at, :] = (back_product(got, pack_ref[...]) + bias_ref[...]).astype(BF16)

    main.consume(chunks, use)
    each(2, side.hand_on)
    each(chunks, main.sent)
    each(2, side.finish)


def attend_out_kernel(
    count, chunk, left, weight, x_ref, bias_ref, gain_ref, shift_ref, up_ref, up_bias_ref,
    rows_ref, residual_ref, pre_ref, hidden_ref, *scratch
):
    rows = x_ref.shape[0]
    place, _, _ = mesh_place(count)
    greet(count)
    chunks = rows // chunk
    summed = RowSum(count, rows, chunk, left, weight, False, scratch[:10])
    main = Gather(count, rows_ref, chunk, *scratch[10:])
    summed.send()

    def close(index):
        at = rows_at(index, chunk)
        values = x_ref[at, :].astype(F32) + summed.total(index) + bias_ref[...]
        residual_ref[at, :] = values
        normed = standardize(values)[0] * gain_ref[...] + shift_ref[...]
        rows_ref[place, at, :] = normed.astype(BF16)
        main.send(index)

    each(chunks, close)

    def use(owner, index):
        got = rows_ref[owner, rows_at(index, chunk), :]
        at = pl.ds(pl.multiple_of(owner * rows + index * chunk, chunk), chunk)
        pre = product(got, up_ref[...]) + up_bias_ref[...]
        pre_ref[at, :] = pre
        hidden_ref[at, :] = gelu_tanh(pre).astype(BF16)

    main.consume(chunks, use)
    each(chunks, main.sent)
    each(chunks, summed.finish)


def mlp_back_kernel(
    count, chunk, left, weight, residual_ref, dy_ref, gain_ref, out_weight_ref, mixed_ref,
    grad_ref, sums_ref, mixed_grad_ref, weight_grad_ref, rows_ref, weight_sum, *scratch
):
    rows = residual_ref.shape[0]
    place, _, _ = mesh_place(count)
    greet(count)
    chunks = rows // chunk
    summed = RowSum(count, rows, chunk, left, weight, True, scratch[:10])
    main = Gather(count, rows_ref, chunk, *scratch[10:])
    sums_ref[...] = jnp.zeros_like(sums_ref)
    summed.send()

    def close(index):
        at = rows_at(index, chunk)
        total = summed.total(index)
        dy = dy_ref[at, :].astype(F32)
        back, per_gain = norm_backward(residual_ref[at, :], total, gain_ref[...])
        grad = dy + back
        grad_ref[at, :] = grad
        rows_ref[place, at, :] = grad.astype(BF16)
        main.send(index)
        sums_ref[0:1, :] += column_sum(per_gain)
        sums_ref[1:2, :] += column_sum(total)
        sums_ref[2:3, :] += column_sum(grad)
        sums_ref[3:4, :] += column_sum(dy)

    each(chunks, close)
    weight_sum[...] = jnp.zeros_like(weight_sum)

    def use(owner, index):
        got = rows_ref[owner, rows_at(index, chunk), :]
        at = pl.ds(pl.multiple_of(owner * rows + index * chunk, chunk), chunk)
        mixed_grad_ref[at, :] = back_product(got, out_weight_ref[...]).astype(BF16)
        weight_sum[...] += rows_product(mixed_ref[at, :], got)

    main.consume(chunks, use)
    weight_grad_ref[...] = weight_sum[...].astype(BF16)
    each(chunks, main.sent)
    each(chunks, summed.finish)


def input_back_kernel(
    count, copies, chunk, shared, pairs, owner, left, weight, x_ref, grad_ref, gain_ref, small_ref, skip_ref,
    qkv_ref, outw_ref, out_ref, small_out, first_ref, qkv_all, outw_all, *scratch
):
    copy, place = lax.axis_index("dp"), lax.axis_index("mp")
    barrier = pltpu.get_barrier_semaphore()
    for step in range(1, copies):
        pl.semaphore_signal(
            barrier, inc=1, device_id={"dp": lax.rem(copy + step, copies)}, device_id_type=pl.DeviceIdType.MESH
        )
    for step in range(1, count):
        pl.semaphore_signal(
            barrier, inc=1, device_id={"mp": lax.rem(place + step, count)}, device_id_type=pl.DeviceIdType.MESH
        )
    pl.semaphore_wait(barrier, copies + count - 2)
    rows = x_ref.shape[0]
    chunks = rows // chunk
    summed = RowSum(count, rows, chunk, left, weight, False, scratch[:10])
    outw = DpReduce(copies, outw_ref, *scratch[10:15])
    qkv = DpReduce(copies, qkv_ref, *scratch[15:20])
    all_ref, qkv_slab, outw_slab, own_small = scratch[20:24]
    side_chunk = skip_ref.shape[0] // 2
    side = Gather(count, all_ref, side_chunk, *scratch[24:27])
    qkv_back = DpGather(copies, qkv_slab, qkv_all, *scratch[27:29])
    outw_back = DpGather(copies, outw_slab, outw_all, *scratch[29:31])
    copy_in, part_in, part_out, copy_sems, part_sems = scratch[31:]

    def small_copy(axis, own, size, source, slots, sems, step, slot):
        return pltpu.make_async_remote_copy(
            src_ref=source, dst_ref=slots.at[slot], send_sem=sems.at[0, step], recv_sem=sems.at[1, slot],
            device_id={axis: lax.rem(own + step, size)}, device_id_type=pl.DeviceIdType.MESH,
        )

    def small_start(axis, own, size, source, slots, sems):
        slots[own] = source[...]
        for step in range(1, size):
            small_copy(axis, own, size, source, slots, sems, step, own).start()

    def small_total(axis, own, size, source, slots, sems):
        for step in range(1, size):
            slot = lax.rem(own + size - step, size)
            small_copy(axis, own, size, source, slots, sems, step, slot).wait_recv()
            small_copy(axis, own, size, source, slots, sems, step, own).wait_send()
        total = slots[0]
        for slot in range(1, size):
            total = total + slots[slot]
        return total

    over_copies = ("dp", copy, copies, own_small, copy_in, copy_sems)
    over_parts = ("mp", place, count, part_out, part_in, part_sems)
    qkv.send()
    outw.send()
    own_small[...] = small_ref[...]
    summed.send()

    def side_start(index):
        all_ref[place, rows_at(index, side_chunk), :] = skip_ref[rows_at(index, side_chunk), :]
        side.send(index)

    each(2, side_start)

    def close(index):
        at = rows_at(index, chunk)
        total = summed.total(index)
        back, per_gain = norm_backward(x_ref[at, :].astype(F32), total, gain_ref[...])
        out_ref[at, :] = (grad_ref[at, :] + back).astype(BF16)
        own_small[4:5, :] += column_sum(per_gain)
        own_small[5:6, :] += column_sum(total)
        spread(index, chunks, copies, [qkv.pass_on, outw.pass_on])

    each(chunks, close)
    small_start(*over_copies)
    qkv_slab[...] = qkv.total().astype(BF16)
    qkv_back.send()
    outw_slab[...] = outw.total().astype(BF16)
    outw_back.send()
    each(2, side.hand_on)
    part_out[...] = small_total(*over_copies)
    small_start(*over_parts)

    def pass_on(index):
        qkv_back.pass_on(index)
        outw_back.pass_on(index)

    each(qkv.at.outer, pass_on)
    each(2, side.finish)
    width = skip_ref.shape[1] // pairs
    for slot in range(pairs):
        user = user_of(owner, place * pairs + slot)
        held = all_ref[lax.div(user, pairs)]
        value = held[:, 0:width]
        for part in range(1, pairs):
            value = jnp.where(lax.rem(user, pairs) == part, held[:, part * width : (part + 1) * width], value)
        first_ref[:, slot * width : (slot + 1) * width] = value
    every = small_total(*over_parts)
    row = lax.broadcasted_iota(jnp.int32, every.shape, 0)
    small_out[...] = jnp.where(row < shared, every, part_out[...])
    each(chunks, summed.finish)
    outw_back.finish()
    qkv_back.finish()


def user_of(owner, head):
    user = jnp.int32(0)
    for pair in range(owner.shape[0]):
        user = jnp.maximum(user, jnp.where(owner[pair] == head, pair, 0))
    return user


def call(kernel, number, inputs, outputs, scratch, flops, scalars=0):
    moved = sum(a.size * a.dtype.itemsize for a in (*inputs, *outputs))
    return pl.pallas_call(
        kernel,
        out_shape=outputs,
        in_specs=[pl.BlockSpec(memory_space=pltpu.SMEM)] * scalars
        + [pl.BlockSpec(memory_space=pltpu.VMEM)] * (len(inputs) - scalars),
        out_specs=[pl.BlockSpec(memory_space=pltpu.VMEM)] * len(outputs),
        scratch_shapes=scratch,
        compiler_params=pltpu.CompilerParams(collective_id=number, has_side_effects=True),
        cost_estimate=pl.CostEstimate(flops=flops, bytes_accessed=moved, transcendentals=0),
    )(*inputs)


def like(shape, kind):
    return jax.ShapeDtypeStruct(shape, kind)


def body(
    inputs,
    first_values,
    cotangent,
    seq_lengths,
    value_owner,
    attn_norm_gain,
    attn_norm_bias,
    qkv_weight,
    qv_bias,
    out_weight,
    out_bias,
    mlp_norm_gain,
    mlp_norm_bias,
    up_weight,
    up_bias,
    down_weight,
    down_bias,
):
    local_rows, model_width = inputs.shape
    group_rows = local_rows * lax.axis_size("mp")
    pairs_dev, head_size = qkv_weight.shape[1], qkv_weight.shape[3]
    seats = (seq_lengths, value_owner, lax.axis_index("mp").reshape(1).astype(jnp.int32))
    copies = lax.axis_size("dp")

    qkv_rows = jnp.transpose(qkv_weight, (1, 2, 3, 0)).reshape(pairs_dev, 5 * head_size, model_width)
    bias_pack = jnp.concatenate(
        [qv_bias[:, 0:2], jnp.zeros_like(qv_bias[:, 0:2]), qv_bias[:, 2:3], jnp.zeros_like(qv_bias[:, 2:3])],
        axis=1,
    ).reshape(1, pairs_dev * PACK * head_size)
    out_flat = out_weight.reshape(pairs_dev * 2 * head_size, model_width)

    count = lax.axis_size("mp")
    chunk = min(128, local_rows)
    chunks = local_rows // chunk
    row = (1, model_width)
    whole = (count, local_rows, model_width)
    slim = pairs_dev * head_size
    sum_scratch = row_sum_scratch(count, local_rows, chunk, model_width)
    main_sems, side_sems = gather_sems(count, chunks), gather_sems(count, 2)
    dense = 2 * group_rows * model_width

    packs = pairs_dev * PACK * head_size
    rows_one, all_first, packed, qkv_pack = call(
        functools.partial(open_kernel, count, chunk), 0,
        (inputs, attn_norm_gain.reshape(row), attn_norm_bias.reshape(row), first_values.reshape(group_rows, slim),
         qkv_rows, bias_pack),
        [like(whole, BF16), like((count, group_rows, slim), BF16), like((group_rows, packs), BF16),
         like((packs, model_width), BF16)],
        main_sems + side_sems, dense * packs,
    )
    rows_one = rows_one.reshape(group_rows, model_width)
    cotangent_late = lax.optimization_barrier((cotangent, rows_one))[0]
    grad_rows = lax.all_gather(cotangent_late, "mp", axis=0, tiled=True)
    mixed, totals = attend_forward(*seats, packed, all_first)
    units = up_bias.shape[0]
    rows_two, residual, hidden_pre, hidden = call(
        functools.partial(attend_out_kernel, count, chunk), 1,
        (mixed, out_flat, inputs, out_bias.reshape(row), mlp_norm_gain.reshape(row), mlp_norm_bias.reshape(row),
         up_weight, up_bias.reshape(1, units)),
        [like(whole, BF16), like(inputs.shape, F32), like((group_rows, units), F32), like((group_rows, units), BF16)],
        sum_scratch + main_sems, dense * (256 + units),
    )
    rows_two = rows_two.reshape(group_rows, model_width)
    grad_hidden = back_product(grad_rows, down_weight)
    grad_pre = jax.vjp(gelu_tanh, hidden_pre)[1](grad_hidden)[0].astype(BF16)
    grad_down_weight = rows_product(hidden, grad_rows).astype(BF16)
    grad_up_weight = rows_product(rows_two, grad_pre).astype(BF16)
    grad_up_bias = jnp.sum(grad_pre.astype(F32), axis=0)
    outer, inner = split_copies(copies)

    def sliced(values):
        return values.reshape(outer, inner, values.shape[0] // copies, values.shape[1])

    late = (grad_up_weight, grad_down_weight)
    grad_pre, late = lax.optimization_barrier((grad_pre, late))
    late_sums = lax.psum(late, "dp")
    grad_residual, sums_two, grad_mixed, grad_out_weight = call(
        functools.partial(mlp_back_kernel, count, chunk), 2,
        (grad_pre, up_weight, residual, cotangent, mlp_norm_gain.reshape(row), out_flat, mixed),
        [like(inputs.shape, F32), like((8, model_width), F32), like(mixed.shape, BF16), like(out_flat.shape, BF16)],
        [pltpu.VMEM(whole, BF16), pltpu.VMEM(out_flat.shape, F32)] + sum_scratch + main_sems,
        dense * up_bias.shape[0],
    )
    grad_flat, grad_skip, pack_sums, output = call(
        functools.partial(attend_backward_kernel, count, chunk, pairs_dev), 5,
        (seq_lengths, value_owner, packed, all_first, grad_mixed, totals, hidden, down_weight, residual,
         down_bias.reshape(row)),
        [like((group_rows, packs), BF16), like((group_rows, slim), BF16), like((8, packs), F32),
         like(inputs.shape, BF16)],
        [pltpu.VMEM((group_rows, LANES), F32), pltpu.VMEM((group_rows, LANES), F32),
         pltpu.VMEM((group_rows, LANES), BF16)] + sum_scratch,
        group_rows * 1024 * 256 * 10 * pairs_dev, scalars=2,
    )
    pack_sums = pack_sums[0].reshape(pairs_dev, PACK, head_size)
    grad_qv_bias = jnp.concatenate([pack_sums[:, 0:2], pack_sums[:, 4:5]], axis=1)
    grad_qkv_weight = rows_product(grad_flat, rows_one).astype(BF16)
    grad_qkv_weight = grad_qkv_weight.reshape(pairs_dev, PACK, head_size, model_width)[:, 0:5]
    grad_qkv_weight = sliced(grad_qkv_weight.reshape(pairs_dev * 5 * head_size, model_width))
    grad_out_weight = sliced(grad_out_weight)
    wide_bias = jnp.pad(grad_up_bias, (0, model_width - grad_up_bias.shape[0])).reshape(row)
    slim_bias = jnp.pad(grad_qv_bias.reshape(-1), (0, model_width - grad_qv_bias.size)).reshape(row)
    own_sums = jnp.concatenate([sums_two[0:4], jnp.zeros((2, model_width), F32), wide_bias, slim_bias], axis=0)
    block = pltpu.VMEM(own_sums.shape, F32)
    grad_inputs, small, grad_first, qkv_sum, out_sum = call(
        functools.partial(input_back_kernel, count, copies, chunk, 6, pairs_dev), 3,
        (value_owner, grad_flat, qkv_pack, inputs, grad_residual, attn_norm_gain.reshape(row), own_sums, grad_skip,
         grad_qkv_weight, grad_out_weight),
        [like(inputs.shape, BF16), like(own_sums.shape, F32), like((group_rows, slim), BF16),
         like(grad_qkv_weight.shape, BF16), like(grad_out_weight.shape, BF16)],
        sum_scratch + reduce_scratch(copies, grad_out_weight) + reduce_scratch(copies, grad_qkv_weight)
        + [pltpu.VMEM((count, group_rows, slim), BF16), pltpu.VMEM(grad_qkv_weight.shape[2:], BF16),
           pltpu.VMEM(grad_out_weight.shape[2:], BF16), block]
        + side_sems + gather_scratch(copies) + gather_scratch(copies)
        + [pltpu.VMEM((copies, *own_sums.shape), F32), pltpu.VMEM((count, *own_sums.shape), F32), block,
           pltpu.SemaphoreType.DMA((2, copies)), pltpu.SemaphoreType.DMA((2, count))],
        dense * packs, scalars=1,
    )
    qkv_sum = qkv_sum.reshape(pairs_dev, 5, head_size, model_width).astype(F32)
    qkv_sum = jnp.transpose(qkv_sum, (3, 0, 1, 2))
    late_sums = (*(part.astype(F32) for part in late_sums), out_sum.reshape(out_weight.shape).astype(F32))
    grad_first = grad_first.reshape(group_rows, pairs_dev, head_size)
    norm_sums = (small[4], small[5], small[2], small[0], small[1], small[3])
    bias_sums = (small[7, : grad_qv_bias.size].reshape(qv_bias.shape), small[6, : grad_up_bias.shape[0]])

    return (
        output,
        grad_inputs,
        grad_first,
        norm_sums[0],
        norm_sums[1],
        qkv_sum,
        bias_sums[0],
        late_sums[2],
        norm_sums[2],
        norm_sums[3],
        norm_sums[4],
        late_sums[0],
        bias_sums[1],
        late_sums[1],
        norm_sums[5],
    )


def solution(mesh):
    return jax.shard_map(
        body,
        mesh=mesh,
        in_specs=(
            P(("dp", "mp"), None),
            P("dp", "mp", None),
            P(("dp", "mp"), None),
            P("dp"),
            P(),
            P(),
            P(),
            P(None, "mp", None, None),
            P("mp", None, None),
            P("mp", None, None, None),
            P(),
            P(),
            P(),
            P(None, "mp"),
            P("mp"),
            P("mp", None),
            P(),
        ),
        out_specs=(
            P(("dp", "mp"), None),
            P(("dp", "mp"), None),
            P("dp", "mp", None),
            P(),
            P(),
            P(None, "mp", None, None),
            P("mp", None, None),
            P("mp", None, None, None),
            P(),
            P(),
            P(),
            P(None, "mp"),
            P("mp"),
            P("mp", None),
            P(),
        ),
        check_vma=False,
    )
```

```python
import functools

import jax
import jax.numpy as jnp
from jax import lax
from jax.experimental import pallas as pl
from jax.experimental.pallas import tpu as pltpu
from jax.sharding import PartitionSpec as P


SHORT = 512
QROWS = 256
LANES = 128
PACK = 6

EPSILON = 1e-05
MASKED = -1e30
GELU_C = 0.7978845608028654
BF16 = jnp.bfloat16
F32 = jnp.float32


def gelu_tanh(values):
    return 0.5 * values * (1.0 + jnp.tanh(GELU_C * (values + 0.044715 * values * values * values)))


def rows_product(left, right):
    return lax.dot_general(left, right, (((0,), (0,)), ((), ())), preferred_element_type=F32)


def back_product(left, weight):
    return lax.dot_general(left, weight, (((1,), (1,)), ((), ())), preferred_element_type=F32)


def product(left, right):
    return jnp.dot(left, right, preferred_element_type=F32)


def opens_at(lengths, row):
    begin, opens = jnp.int32(0), jnp.int32(0)
    for slot in range(lengths.shape[0]):
        opens = jnp.maximum(opens, jnp.where(begin == row, 1, 0))
        begin = begin + lengths[slot]
    return opens


def head_lanes(head):
    lane = lax.broadcasted_iota(jnp.int32, (1, LANES), 1)
    return (lane < LANES // 2) if head == 0 else (lane >= LANES // 2)


def causal_tile():
    row = lax.broadcasted_iota(jnp.int32, (QROWS, QROWS), 0)
    column = lax.broadcasted_iota(jnp.int32, (QROWS, QROWS), 1)
    return column <= row


def pick_values(half, fresh, held, value_ref):
    if held.shape[1] < LANES:
        turned = jnp.concatenate([held, held], axis=1)
    else:
        turned = jnp.concatenate([held[:, LANES // 2 :], held[:, : LANES // 2]], axis=1)
        turned = jnp.where(half == 1, held, turned)
    value_ref[...] = jnp.where(head_lanes(0), fresh, turned)


def attend_forward_kernel(pairs, lengths, owner, place, qkv_ref, first_ref, mixed_ref, totals_ref, value_ref):
    half = lax.rem(owner[place[0] * pairs + pl.program_id(0)], pairs)
    pick_values(half, qkv_ref[:, 2 * LANES : 3 * LANES], first_ref[0], value_ref)
    blocks = qkv_ref.shape[0] // SHORT
    scale = (LANES // 2) ** (-0.5)

    def block(index, carried):
        base = pl.multiple_of(index * SHORT, SHORT)
        for half in range(SHORT // QROWS):
            first = base + half * QROWS

            def attend(with_previous):
                query = qkv_ref[pl.ds(first, QROWS), 0:LANES] * jnp.asarray(scale, BF16)
                spans = []
                if with_previous:
                    spans.append((base - SHORT, SHORT))
                if half:
                    spans.append((base, half * QROWS))
                spans.append((first, QROWS))
                mixed = jnp.zeros((QROWS, LANES), F32)
                totals = []
                for head in range(2):
                    chosen = head_lanes(head)
                    query_head = jnp.where(chosen, query, jnp.zeros_like(query))
                    scores = [
                        back_product(query_head, qkv_ref[pl.ds(at, size), LANES : 2 * LANES])
                        for at, size in spans
                    ]
                    scores[-1] = jnp.where(causal_tile(), scores[-1], MASKED)
                    top = scores[0].max(axis=1, keepdims=True)
                    for part in scores[1:]:
                        top = jnp.maximum(top, part.max(axis=1, keepdims=True))
                    total = jnp.zeros((QROWS, 1), F32)
                    gathered = jnp.zeros((QROWS, LANES), F32)
                    for (at, size), part in zip(spans, scores):
                        weights = jnp.exp(part - top)
                        total = total + weights.sum(axis=1, keepdims=True)
                        values = value_ref[pl.ds(at, size), :]
                        values = jnp.where(chosen, values, jnp.zeros_like(values))
                        gathered = gathered + product(weights.astype(BF16), values)
                    mixed = mixed + gathered / total
                    totals.append(top + jnp.log(total))
                mixed_ref[pl.ds(first, QROWS), :] = mixed.astype(BF16)
                totals_ref[pl.ds(first, QROWS), :] = jnp.where(
                    head_lanes(0), totals[0], totals[1]
                )

            @pl.when(opens_at(lengths, base) == 0)
            def _():
                attend(True)

            @pl.when(opens_at(lengths, base) == 1)
            def _():
                attend(False)

        return carried

    lax.fori_loop(0, blocks, block, 0)


def attend_backward_kernel(
    count, copies, chunk, pairs, lengths, owner, qkv_ref, first_ref, grad_ref, totals_ref, left, weight, residual_ref, shift_ref,
    outw_ref, out_ref, skip_ref, sums_ref, layer_ref, outw_all,
    key_sum, value_sum, value_ref, *scratch
):
    blocks = qkv_ref.shape[0] // SHORT
    scale = (LANES // 2) ** (-0.5)
    place, _, _ = mesh_place(count)
    greet(count, copies)
    rows = residual_ref.shape[0]
    chunks = rows // chunk
    summed = RowSum(count, rows, chunk, left, weight, False, scratch[:10])
    outw = DpReduce(copies, outw_ref, *scratch[10:15])
    outw_slab = scratch[15]
    outw_back = DpGather(copies, outw_slab, outw_all, *scratch[16:18])
    outw.send()
    turns = pairs * blocks
    sums_ref[...] = jnp.zeros_like(sums_ref)
    summed.send()

    def between(number):
        @pl.when(number == turns // 8)
        def _():
            each(outw.at.outer, outw.pass_on)

        @pl.when(number == turns // 2)
        def _():
            outw_slab[...] = outw.total().astype(BF16)
            outw_back.send()

        @pl.when(number == 7 * turns // 8)
        def _():
            each(outw.at.outer, outw_back.pass_on)

    def one_pair(pair):
        column = pl.multiple_of(pair * 3 * LANES, LANES)
        side = pl.multiple_of(pair * LANES, LANES)
        query_at, key_at, fresh_at = (pl.ds(column + part * LANES, LANES) for part in range(3))
        used = owner[place * pairs + pair]
        held = first_ref[lax.div(used, pairs)]
        pick_values(lax.rem(used, pairs), qkv_ref[:, fresh_at], held, value_ref)
        key_sum[...] = jnp.zeros_like(key_sum)
        value_sum[...] = jnp.zeros_like(value_sum)

        def block(index):
            base = pl.multiple_of(index * SHORT, SHORT)
            joined = opens_at(lengths, base) == 0

            def attend(half, with_previous):
                first = base + half * QROWS
                query = qkv_ref[pl.ds(first, QROWS), query_at] * jnp.asarray(scale, BF16)
                grad = grad_ref[pl.ds(first, QROWS), pl.ds(side, LANES)]
                spans = []
                if with_previous:
                    spans.append((base - SHORT, SHORT))
                if half:
                    spans.append((base, half * QROWS))
                spans.append((first, QROWS))
                grad_query = jnp.zeros((QROWS, LANES), F32)
                both = totals_ref[pl.ds(first, QROWS), pl.ds(side, LANES)]
                for head in range(2):
                    chosen = head_lanes(head)
                    query_head = jnp.where(chosen, query, jnp.zeros_like(query))
                    grad_head = jnp.where(chosen, grad, jnp.zeros_like(grad))
                    at_lane = head * (LANES // 2)
                    totals = both[:, at_lane : at_lane + 1]
                    probs, grads = [], []
                    inner = jnp.zeros((QROWS, 1), F32)
                    for number, (at, size) in enumerate(spans):
                        keys = qkv_ref[pl.ds(at, size), key_at]
                        part = jnp.exp(back_product(query_head, keys) - totals)
                        if number == len(spans) - 1:
                            part = jnp.where(causal_tile(), part, 0.0)
                        elif with_previous and number == 0:
                            part = jnp.where(joined, part, 0.0)
                        values = value_ref[pl.ds(at, size), :]
                        weighted = part * back_product(grad_head, values)
                        inner = inner + weighted.sum(axis=1, keepdims=True)
                        probs.append(part)
                        grads.append(weighted)
                    for (at, size), part, weighted in zip(spans, probs, grads):
                        keys = qkv_ref[pl.ds(at, size), key_at]
                        keys = jnp.where(chosen, keys, jnp.zeros_like(keys))
                        grad_scores = (weighted - part * inner).astype(BF16)
                        grad_query = grad_query + product(grad_scores, keys)
                        key_sum[pl.ds(at, size), :] += rows_product(grad_scores, query_head)
                        value_sum[pl.ds(at, size), :] += rows_product(part.astype(BF16), grad_head)
                out_ref[pl.ds(first, QROWS), query_at] = (grad_query * scale).astype(BF16)

            for half in range(SHORT // QROWS):

                @pl.when(index > 0)
                def _():
                    attend(half, True)

                @pl.when(index == 0)
                def _():
                    attend(half, False)

        each(blocks, lambda index: (block(index), between(pair * blocks + index)))
        out_ref[:, key_at] = key_sum[...].astype(BF16)
        out_ref[:, fresh_at] = value_sum[...].astype(BF16)
        for slot in range(pairs):

            @pl.when(pair == slot)
            def _():
                width = LANES // 2
                skip_ref[:, slot * width : (slot + 1) * width] = value_sum[:, width:].astype(BF16)

        for at in (query_at, fresh_at):
            sums_ref[0:1, at] = column_sum(out_ref[:, at].astype(F32))

    each(pairs, one_pair)

    def close(index):
        at = rows_at(index, chunk)
        layer_ref[at, :] = (residual_ref[at, :] + summed.total(index) + shift_ref[...]).astype(BF16)

    each(chunks, close)
    each(chunks, summed.finish)
    outw_back.finish()


def attend_forward(lengths, owner, place, packed, firsts):
    rows, pairs = packed.shape[0], packed.shape[1] // (3 * LANES)
    return pl.pallas_call(
        functools.partial(attend_forward_kernel, pairs),
        grid_spec=pltpu.PrefetchScalarGridSpec(
            num_scalar_prefetch=3,
            grid=(pairs,),
            in_specs=[
                pl.BlockSpec((rows, 3 * LANES), lambda p, c, o, m: (0, p)),
                pl.BlockSpec((1, rows, firsts.shape[2]), lambda p, c, o, m: (lax.div(o[m[0] * pairs + p], pairs), 0, 0)),
            ],
            out_specs=[
                pl.BlockSpec((rows, LANES), lambda p, c, o, m: (0, p)),
                pl.BlockSpec((rows, LANES), lambda p, c, o, m: (0, p)),
            ],
            scratch_shapes=[pltpu.VMEM((rows, LANES), BF16)],
        ),
        out_shape=[
            jax.ShapeDtypeStruct((rows, pairs * LANES), BF16),
            jax.ShapeDtypeStruct((rows, pairs * LANES), F32),
        ],
        cost_estimate=pl.CostEstimate(
            flops=rows * 1024 * 256 * 4 * pairs, bytes_accessed=8 << 20, transcendentals=rows * 2048
        ),
        name="attend_forward",
    )(lengths, owner, place, packed, firsts)


def mesh_place(count):
    place = lax.axis_index("mp")
    core = lax.rem(place, 2)
    chip = lax.div(place, 2)
    chips = count // 2

    def across(step, other):
        return lax.rem(chip + step + chips, chips) * 2 + (1 - core if other else core)

    return place, place + 1 - 2 * core, across


def remote(source, target, sems, index, device):
    return pltpu.make_async_remote_copy(
        src_ref=source,
        dst_ref=target,
        send_sem=sems.at[(0, *index)],
        recv_sem=sems.at[(1, *index)],
        device_id={"mp": device},
        device_id_type=pl.DeviceIdType.MESH,
    )


def greet(count, copies=0):
    _, partner, across = mesh_place(count)
    barrier = pltpu.get_barrier_semaphore()
    for device in [partner] + [across(step, False) for step in range(1, count // 2)]:
        pl.semaphore_signal(
            barrier, inc=1, device_id={"mp": device}, device_id_type=pl.DeviceIdType.MESH
        )
    others = DpPlace(copies).greet(barrier) if copies else 0
    pl.semaphore_wait(barrier, count // 2 + others)


def each(count, step):
    def run(index, carried):
        step(index)
        return carried

    lax.fori_loop(0, count, run, 0)


class Gather:
    def __init__(self, count, out_ref, chunk, near, far, passed):
        self.count, self.out, self.chunk = count, out_ref, chunk
        self.near, self.far, self.passed = near, far, passed
        self.place, self.partner, self.across = mesh_place(count)

    def part(self, owner, index):
        return self.out.at[owner, pl.ds(pl.multiple_of(index * self.chunk, self.chunk), self.chunk), :]

    def send(self, index):
        own = self.part(self.place, index)
        for step in range(1, self.count // 2):
            remote(own, own, self.far, (step - 1, index), self.across(step, False)).start()
        remote(own, own, self.near, (index,), self.partner).start()

    def hand_on(self, index):
        for step in range(1, self.count // 2):
            got = self.part(self.across(-step, False), index)
            remote(got, got, self.far, (step - 1, index), self.across(step, False)).wait_recv()
            remote(got, got, self.passed, (step - 1, index), self.partner).start()

    def consume(self, chunks, use):
        far = self.count // 2 - 1
        chip, core = lax.div(self.place, 2), lax.rem(self.place, 2)

        def turn(number):
            kind, index = lax.div(number, chunks), lax.rem(number, chunks)
            step = lax.rem(kind + 2 * far - 2, max(far, 1)) + 1
            owner = lax.rem(chip - step + self.count // 2, self.count // 2) * 2
            owner = owner + jnp.where(kind < far + 2, core, 1 - core)
            owner = jnp.where(kind == 0, self.place, jnp.where(kind == 1, self.partner, owner))
            got = self.part(owner, index)

            @pl.when(kind == 1)
            def _():
                remote(got, got, self.near, (index,), self.partner).wait_recv()

            @pl.when((kind >= 2) & (kind < far + 2))
            def _():
                remote(got, got, self.far, (step - 1, index), self.across(step, False)).wait_recv()
                remote(got, got, self.passed, (step - 1, index), self.partner).start()

            @pl.when(kind >= far + 2)
            def _():
                remote(got, got, self.passed, (step - 1, index), self.partner).wait_recv()

            use(owner, index)

        each((2 * far + 2) * chunks, turn)

    def sent(self, index):
        own = self.part(self.place, index)
        remote(own, own, self.near, (index,), self.partner).wait_send()
        for step in range(1, self.count // 2):
            remote(own, own, self.far, (step - 1, index), self.across(step, False)).wait_send()
            got = self.part(self.across(-step, False), index)
            remote(got, got, self.passed, (step - 1, index), self.partner).wait_send()

    def finish(self, index):
        own = self.part(self.place, index)
        near = self.part(self.partner, index)
        remote(own, near, self.near, (index,), self.partner).wait()
        for step in range(1, self.count // 2):
            remote(own, own, self.far, (step - 1, index), self.across(step, False)).wait_send()
            got = self.part(self.across(-step, True), index)
            remote(got, got, self.passed, (step - 1, index), self.partner).wait()


def gather_sems(count, chunks):
    far = max(count // 2 - 1, 1)
    return [
        pltpu.SemaphoreType.DMA((2, chunks)),
        pltpu.SemaphoreType.DMA((2, far, chunks)),
        pltpu.SemaphoreType.DMA((2, far, chunks)),
    ]


class RowSum:
    def __init__(self, count, rows, chunk, left, weight, flipped, buffers):
        self.count, self.rows, self.chunk = count, rows, chunk
        self.left, self.weight, self.flipped = left, weight, flipped
        (self.pair_out, self.pair_in, self.far_out, self.far_in, self.near_out, self.near_in, self.own) = buffers[:7]
        self.pair, self.far, self.near = buffers[7:]
        self.place, self.partner, self.across = mesh_place(count)

    def product(self, owner, index):
        at = pl.multiple_of(owner * self.rows + index * self.chunk, self.chunk)
        rows = self.left[pl.ds(at, self.chunk), :]
        return (back_product if self.flipped else product)(rows, self.weight[...])

    def pair_copy(self, step, index):
        return remote(
            self.pair_out.at[step - 1, index], self.pair_in.at[step - 1, index],
            self.pair, (step - 1, index), self.partner,
        )

    def far_copy(self, step, index):
        return remote(
            self.far_out.at[step - 1, index], self.far_in.at[step - 1, index],
            self.far, (step - 1, index), self.across(step, False),
        )

    def near_copy(self, index):
        return remote(self.near_out.at[index], self.near_in.at[index], self.near, (index,), self.partner)

    def send(self):
        chunks, far = self.rows // self.chunk, self.count // 2 - 1
        core = lax.rem(self.place, 2)

        def turn(number):
            kind, index = lax.div(number, chunks), lax.rem(number, chunks)
            step = lax.rem(kind, max(far, 1)) + 1
            owner = lax.rem(lax.div(self.place, 2) + step, self.count // 2) * 2
            owner = owner + jnp.where(kind < far, 1 - core, core)
            owner = jnp.where(kind == 2 * far, self.partner, owner)
            owner = jnp.where(kind > 2 * far, self.place, owner)
            rows = self.product(owner, index)

            @pl.when(kind < far)
            def _():
                self.pair_out[step - 1, index] = rows.astype(BF16)
                self.pair_copy(step, index).start()

            @pl.when((kind >= far) & (kind < 2 * far))
            def _():
                self.pair_copy(step, index).wait_recv()
                self.far_out[step - 1, index] = (rows + self.pair_in[step - 1, index].astype(F32)).astype(BF16)
                self.far_copy(step, index).start()

            @pl.when(kind == 2 * far)
            def _():
                self.near_out[index] = rows.astype(BF16)
                self.near_copy(index).start()

            @pl.when(kind > 2 * far)
            def _():
                self.own[index] = rows

        each((2 * far + 2) * chunks, turn)

    def total(self, index):
        self.near_copy(index).wait_recv()
        rows = self.own[index] + self.near_in[index].astype(F32)
        for step in range(1, self.count // 2):
            self.far_copy(step, index).wait_recv()
            rows = rows + self.far_in[step - 1, index].astype(F32)
        return rows

    def finish(self, index):
        self.near_copy(index).wait_send()
        for step in range(1, self.count // 2):
            self.pair_copy(step, index).wait_send()
            self.far_copy(step, index).wait_send()


def split_copies(copies):
    inner = 1
    while (2 * inner) ** 2 <= copies:
        inner *= 2
    return copies // inner, inner


def dp_copy(source, target, send_sem, recv_sem, device):
    return pltpu.make_async_remote_copy(
        src_ref=source, dst_ref=target, send_sem=send_sem, recv_sem=recv_sem,
        device_id={"dp": device}, device_id_type=pl.DeviceIdType.MESH,
    )


class DpPlace:
    def __init__(self, copies):
        self.outer, self.inner = split_copies(copies)
        here = lax.axis_index("dp")
        self.z, self.y = lax.div(here, self.inner), lax.rem(here, self.inner)

    def along_y(self, step):
        return lax.rem(self.y + step + self.inner, self.inner)

    def along_z(self, step):
        return lax.rem(self.z + step + self.outer, self.outer)

    def device(self, z, y):
        return z * self.inner + y

    def greet(self, barrier):
        for step in range(1, self.inner):
            pl.semaphore_signal(
                barrier, inc=1, device_id={"dp": self.device(self.z, self.along_y(step))},
                device_id_type=pl.DeviceIdType.MESH,
            )
        for step in range(1, self.outer):
            pl.semaphore_signal(
                barrier, inc=1, device_id={"dp": self.device(self.along_z(step), self.y)},
                device_id_type=pl.DeviceIdType.MESH,
            )
        return self.inner + self.outer - 2


class DpReduce:
    def __init__(self, copies, source, y_in, z_out, z_in, y_sems, z_sems):
        self.at = DpPlace(copies)
        self.source, self.y_in, self.z_out, self.z_in = source, y_in, z_out, z_in
        self.y_sems, self.z_sems = y_sems, z_sems

    def y_copy(self, step, z):
        peer = self.at.along_y(step)
        return dp_copy(
            self.source.at[z, peer], self.y_in.at[step - 1, z],
            self.y_sems.at[0, step - 1, z], self.y_sems.at[1, step - 1, z], self.at.device(self.at.z, peer),
        )

    def z_copy(self, step):
        peer = self.at.along_z(step + 1)
        return dp_copy(
            self.z_out.at[step], self.z_in.at[step],
            self.z_sems.at[0, step], self.z_sems.at[1, step], self.at.device(peer, self.at.y),
        )

    def send(self):
        def start(step):
            for y_step in range(1, self.at.inner):
                self.y_copy(y_step, self.at.along_z(step + 1)).start()

        each(self.at.outer, start)

    def y_total(self, z):
        total = self.source[z, self.at.y].astype(F32)
        for y_step in range(1, self.at.inner):
            self.y_copy(y_step, z).wait_recv()
            total = total + self.y_in[y_step - 1, z].astype(F32)
        return total

    def pass_on(self, step):
        @pl.when(step < self.at.outer - 1)
        def _():
            self.z_out[step] = self.y_total(self.at.along_z(step + 1)).astype(BF16)
            self.z_copy(step).start()

    def total(self):
        total = self.y_total(self.at.z)
        for step in range(self.at.outer - 1):
            self.z_copy(step).wait_recv()
            total = total + self.z_in[step].astype(F32)
        for step in range(self.at.outer - 1):
            self.z_copy(step).wait_send()
        for y_step in range(1, self.at.inner):
            for z in range(self.at.outer):
                self.y_copy(y_step, z).wait_send()
        return total


def reduce_scratch(copies, array):
    outer, inner = split_copies(copies)
    slab = array.shape[2:]
    return [
        pltpu.VMEM((inner - 1, outer, *slab), BF16),
        pltpu.VMEM((outer - 1, *slab), BF16),
        pltpu.VMEM((outer - 1, *slab), BF16),
        pltpu.SemaphoreType.DMA((2, inner - 1, outer)),
        pltpu.SemaphoreType.DMA((2, outer - 1)),
    ]


class DpGather:
    def __init__(self, copies, slab, held, z_sems, y_sems):
        self.at = DpPlace(copies)
        self.slab, self.held, self.z_sems, self.y_sems = slab, held, z_sems, y_sems

    def z_copy(self, step, z):
        here = self.held.at[z, self.at.y]
        peer = self.at.device(self.at.along_z(step + 1), self.at.y)
        return dp_copy(here, here, self.z_sems.at[0, step], self.z_sems.at[1, step], peer)

    def y_copy(self, y_step, slot, z, y):
        here = self.held.at[z, y]
        peer = self.at.device(self.at.z, self.at.along_y(y_step))
        return dp_copy(
            here, here, self.y_sems.at[0, y_step - 1, slot], self.y_sems.at[1, y_step - 1, slot], peer
        )

    def send(self):
        self.held[self.at.z, self.at.y] = self.slab[...]
        for step in range(self.at.outer - 1):
            self.z_copy(step, self.at.z).start()
        for y_step in range(1, self.at.inner):
            self.y_copy(y_step, self.at.outer - 1, self.at.z, self.at.y).start()

    def pass_on(self, step):
        @pl.when(step < self.at.outer - 1)
        def _():
            source = self.at.along_z(-step - 1)
            self.z_copy(step, source).wait_recv()
            for y_step in range(1, self.at.inner):
                self.y_copy(y_step, step, source, self.at.y).start()

    def finish(self):
        for step in range(self.at.outer - 1):
            self.z_copy(step, self.at.z).wait_send()
        for y_step in range(1, self.at.inner):
            sender = self.at.along_y(-y_step)
            for slot in range(self.at.outer):
                source = self.at.along_z(-slot - 1)
                self.y_copy(y_step, slot, source, sender).wait_recv()
                self.y_copy(y_step, slot, source, self.at.y).wait_send()


def gather_scratch(copies):
    outer, inner = split_copies(copies)
    return [pltpu.SemaphoreType.DMA((2, outer - 1)), pltpu.SemaphoreType.DMA((2, inner - 1, outer))]


def spread(index, chunks, copies, steps):
    outer = split_copies(copies)[0]
    turns = -(-outer // chunks)

    def turn(sub):
        for step in steps:
            step(index * turns + sub)

    each(turns, turn)


def row_sum_scratch(count, rows, chunk, width):
    far, chunks = max(count // 2 - 1, 1), rows // chunk
    wide = pltpu.VMEM((far, chunks, chunk, width), BF16)
    slim = pltpu.VMEM((chunks, chunk, width), BF16)
    return [
        wide, wide, wide, wide, slim, slim, pltpu.VMEM((chunks, chunk, width), F32),
        pltpu.SemaphoreType.DMA((2, far, chunks)),
        pltpu.SemaphoreType.DMA((2, far, chunks)),
        pltpu.SemaphoreType.DMA((2, chunks)),
    ]


def rows_at(index, chunk):
    return pl.ds(pl.multiple_of(index * chunk, chunk), chunk)


def standardize(values):
    average = jnp.mean(values, axis=-1, keepdims=True)
    centered = values - average
    spread = lax.rsqrt(jnp.mean(centered * centered, axis=-1, keepdims=True) + EPSILON)
    return centered * spread, spread


def norm_backward(values, grad, gain):
    normed, spread = standardize(values)
    scaled = grad * gain
    inner = jnp.mean(scaled * normed, axis=-1, keepdims=True)
    back = (scaled - jnp.mean(scaled, axis=-1, keepdims=True) - normed * inner) * spread
    return back, grad * normed


def column_sum(values):
    return jnp.sum(values, axis=0, keepdims=True)


def open_kernel(
    count, chunk, x_ref, gain_ref, shift_ref, first_ref, weight, bias_ref, rows_ref, all_ref, packed_ref, pack_ref, *sems
):
    rows = x_ref.shape[0]
    place, _, _ = mesh_place(count)
    greet(count)
    chunks = rows // chunk
    main = Gather(count, rows_ref, chunk, *sems[:3])
    side_chunk = first_ref.shape[0] // 2
    side = Gather(count, all_ref, side_chunk, *sems[3:])

    def start(index):
        values = x_ref[rows_at(index, chunk), :].astype(F32)
        normed = standardize(values)[0] * gain_ref[...] + shift_ref[...]
        rows_ref[place, rows_at(index, chunk), :] = normed.astype(BF16)
        main.send(index)

    each(chunks, start)

    def side_start(index):
        all_ref[place, rows_at(index, side_chunk), :] = first_ref[rows_at(index, side_chunk), :]
        side.send(index)

    each(2, side_start)

    held = weight.shape[1]
    span = pack_ref.shape[0] // weight.shape[0]
    for pair in range(weight.shape[0]):
        pack_ref[pair * span : pair * span + held, :] = weight[pair]
        pack_ref[pair * span + held : (pair + 1) * span, :] = jnp.zeros((span - held, weight.shape[2]), BF16)

    def use(owner, index):
        got = rows_ref[owner, rows_at(index, chunk), :]
        at = pl.ds(pl.multiple_of(owner * rows + index * chunk, chunk), chunk)
        packed_ref[at, :] = (back_product(got, pack_ref[...]) + bias_ref[...]).astype(BF16)

    main.consume(chunks, use)
    each(2, side.hand_on)
    each(chunks, main.sent)
    each(2, side.finish)


def attend_out_kernel(
    count, chunk, left, weight, x_ref, bias_ref, gain_ref, shift_ref, up_ref, up_bias_ref,
    rows_ref, residual_ref, pre_ref, hidden_ref, *scratch
):
    rows = x_ref.shape[0]
    place, _, _ = mesh_place(count)
    greet(count)
    chunks = rows // chunk
    summed = RowSum(count, rows, chunk, left, weight, False, scratch[:10])
    main = Gather(count, rows_ref, chunk, *scratch[10:])
    summed.send()

    def close(index):
        at = rows_at(index, chunk)
        values = x_ref[at, :].astype(F32) + summed.total(index) + bias_ref[...]
        residual_ref[at, :] = values
        normed = standardize(values)[0] * gain_ref[...] + shift_ref[...]
        rows_ref[place, at, :] = normed.astype(BF16)
        main.send(index)

    each(chunks, close)

    def use(owner, index):
        got = rows_ref[owner, rows_at(index, chunk), :]
        at = pl.ds(pl.multiple_of(owner * rows + index * chunk, chunk), chunk)
        pre = product(got, up_ref[...]) + up_bias_ref[...]
        pre_ref[at, :] = pre
        hidden_ref[at, :] = gelu_tanh(pre).astype(BF16)

    main.consume(chunks, use)
    each(chunks, main.sent)
    each(chunks, summed.finish)


def mlp_back_kernel(
    count, chunk, left, weight, residual_ref, dy_ref, gain_ref, out_weight_ref, mixed_ref,
    grad_ref, sums_ref, mixed_grad_ref, weight_grad_ref, rows_ref, weight_sum, *scratch
):
    rows = residual_ref.shape[0]
    place, _, _ = mesh_place(count)
    greet(count)
    chunks = rows // chunk
    summed = RowSum(count, rows, chunk, left, weight, True, scratch[:10])
    main = Gather(count, rows_ref, chunk, *scratch[10:])
    sums_ref[...] = jnp.zeros_like(sums_ref)
    summed.send()

    def close(index):
        at = rows_at(index, chunk)
        total = summed.total(index)
        dy = dy_ref[at, :].astype(F32)
        back, per_gain = norm_backward(residual_ref[at, :], total, gain_ref[...])
        grad = dy + back
        grad_ref[at, :] = grad
        rows_ref[place, at, :] = grad.astype(BF16)
        main.send(index)
        sums_ref[0:1, :] += column_sum(per_gain)
        sums_ref[1:2, :] += column_sum(total)
        sums_ref[2:3, :] += column_sum(grad)
        sums_ref[3:4, :] += column_sum(dy)

    each(chunks, close)
    weight_sum[...] = jnp.zeros_like(weight_sum)

    def use(owner, index):
        got = rows_ref[owner, rows_at(index, chunk), :]
        at = pl.ds(pl.multiple_of(owner * rows + index * chunk, chunk), chunk)
        mixed_grad_ref[at, :] = back_product(got, out_weight_ref[...]).astype(BF16)
        weight_sum[...] += rows_product(mixed_ref[at, :], got)

    main.consume(chunks, use)
    weight_grad_ref[...] = weight_sum[...].astype(BF16)
    each(chunks, main.sent)
    each(chunks, summed.finish)


def input_back_kernel(
    count, copies, chunk, shared, pairs, owner, left, weight, x_ref, grad_ref, gain_ref, small_ref, skip_ref,
    qkv_ref, out_ref, small_out, first_ref, qkv_all, *scratch
):
    copy, place = lax.axis_index("dp"), lax.axis_index("mp")
    barrier = pltpu.get_barrier_semaphore()
    for step in range(1, copies):
        pl.semaphore_signal(
            barrier, inc=1, device_id={"dp": lax.rem(copy + step, copies)}, device_id_type=pl.DeviceIdType.MESH
        )
    for step in range(1, count):
        pl.semaphore_signal(
            barrier, inc=1, device_id={"mp": lax.rem(place + step, count)}, device_id_type=pl.DeviceIdType.MESH
        )
    pl.semaphore_wait(barrier, copies + count - 2)
    rows = x_ref.shape[0]
    chunks = rows // chunk
    summed = RowSum(count, rows, chunk, left, weight, False, scratch[:10])
    qkv = DpReduce(copies, qkv_ref, *scratch[10:15])
    all_ref, qkv_slab, own_small = scratch[15:18]
    side_chunk = skip_ref.shape[0] // 2
    side = Gather(count, all_ref, side_chunk, *scratch[18:21])
    qkv_back = DpGather(copies, qkv_slab, qkv_all, *scratch[21:23])
    copy_in, part_in, part_out, copy_sems, part_sems = scratch[23:]

    def small_copy(axis, own, size, source, slots, sems, step, slot):
        return pltpu.make_async_remote_copy(
            src_ref=source, dst_ref=slots.at[slot], send_sem=sems.at[0, step], recv_sem=sems.at[1, slot],
            device_id={axis: lax.rem(own + step, size)}, device_id_type=pl.DeviceIdType.MESH,
        )

    def small_start(axis, own, size, source, slots, sems):
        slots[own] = source[...]
        for step in range(1, size):
            small_copy(axis, own, size, source, slots, sems, step, own).start()

    def small_total(axis, own, size, source, slots, sems):
        for step in range(1, size):
            slot = lax.rem(own + size - step, size)
            small_copy(axis, own, size, source, slots, sems, step, slot).wait_recv()
            small_copy(axis, own, size, source, slots, sems, step, own).wait_send()
        total = slots[0]
        for slot in range(1, size):
            total = total + slots[slot]
        return total

    over_copies = ("dp", copy, copies, own_small, copy_in, copy_sems)
    over_parts = ("mp", place, count, part_out, part_in, part_sems)
    qkv.send()
    own_small[...] = small_ref[...]
    summed.send()

    def side_start(index):
        all_ref[place, rows_at(index, side_chunk), :] = skip_ref[rows_at(index, side_chunk), :]
        side.send(index)

    each(2, side_start)

    def close(index):
        at = rows_at(index, chunk)
        total = summed.total(index)
        back, per_gain = norm_backward(x_ref[at, :].astype(F32), total, gain_ref[...])
        out_ref[at, :] = (grad_ref[at, :] + back).astype(BF16)
        own_small[4:5, :] += column_sum(per_gain)
        own_small[5:6, :] += column_sum(total)
        spread(index, chunks, copies, [qkv.pass_on])

    each(chunks, close)
    small_start(*over_copies)
    qkv_slab[...] = qkv.total().astype(BF16)
    qkv_back.send()
    each(2, side.hand_on)
    part_out[...] = small_total(*over_copies)
    small_start(*over_parts)

    def pass_on(index):
        qkv_back.pass_on(index)

    each(qkv.at.outer, pass_on)
    each(2, side.finish)
    width = skip_ref.shape[1] // pairs
    for slot in range(pairs):
        user = user_of(owner, place * pairs + slot)
        held = all_ref[lax.div(user, pairs)]
        value = held[:, 0:width]
        for part in range(1, pairs):
            value = jnp.where(lax.rem(user, pairs) == part, held[:, part * width : (part + 1) * width], value)
        first_ref[:, slot * width : (slot + 1) * width] = value
    every = small_total(*over_parts)
    row = lax.broadcasted_iota(jnp.int32, every.shape, 0)
    small_out[...] = jnp.where(row < shared, every, part_out[...])
    each(chunks, summed.finish)
    qkv_back.finish()


def user_of(owner, head):
    user = jnp.int32(0)
    for pair in range(owner.shape[0]):
        user = jnp.maximum(user, jnp.where(owner[pair] == head, pair, 0))
    return user


def call(kernel, number, inputs, outputs, scratch, flops, scalars=0):
    moved = sum(a.size * a.dtype.itemsize for a in (*inputs, *outputs))
    return pl.pallas_call(
        kernel,
        out_shape=outputs,
        in_specs=[pl.BlockSpec(memory_space=pltpu.SMEM)] * scalars
        + [pl.BlockSpec(memory_space=pltpu.VMEM)] * (len(inputs) - scalars),
        out_specs=[pl.BlockSpec(memory_space=pltpu.VMEM)] * len(outputs),
        scratch_shapes=scratch,
        compiler_params=pltpu.CompilerParams(collective_id=number, has_side_effects=True),
        cost_estimate=pl.CostEstimate(flops=flops, bytes_accessed=moved, transcendentals=0),
    )(*inputs)


def like(shape, kind):
    return jax.ShapeDtypeStruct(shape, kind)


def body(
    inputs,
    first_values,
    cotangent,
    seq_lengths,
    value_owner,
    attn_norm_gain,
    attn_norm_bias,
    qkv_weight,
    qv_bias,
    out_weight,
    out_bias,
    mlp_norm_gain,
    mlp_norm_bias,
    up_weight,
    up_bias,
    down_weight,
    down_bias,
):
    local_rows, model_width = inputs.shape
    group_rows = local_rows * lax.axis_size("mp")
    pairs_dev, head_size = qkv_weight.shape[1], qkv_weight.shape[3]
    seats = (seq_lengths, value_owner, lax.axis_index("mp").reshape(1).astype(jnp.int32))
    copies = lax.axis_size("dp")

    qkv_rows = jnp.transpose(qkv_weight, (1, 2, 3, 0)).reshape(pairs_dev, 5 * head_size, model_width)
    bias_pack = jnp.concatenate(
        [qv_bias[:, 0:2], jnp.zeros_like(qv_bias[:, 0:2]), qv_bias[:, 2:3], jnp.zeros_like(qv_bias[:, 2:3])],
        axis=1,
    ).reshape(1, pairs_dev * PACK * head_size)
    out_flat = out_weight.reshape(pairs_dev * 2 * head_size, model_width)

    count = lax.axis_size("mp")
    chunk = min(128, local_rows)
    chunks = local_rows // chunk
    row = (1, model_width)
    whole = (count, local_rows, model_width)
    slim = pairs_dev * head_size
    sum_scratch = row_sum_scratch(count, local_rows, chunk, model_width)
    main_sems, side_sems = gather_sems(count, chunks), gather_sems(count, 2)
    dense = 2 * group_rows * model_width

    packs = pairs_dev * PACK * head_size
    rows_one, all_first, packed, qkv_pack = call(
        functools.partial(open_kernel, count, chunk), 0,
        (inputs, attn_norm_gain.reshape(row), attn_norm_bias.reshape(row), first_values.reshape(group_rows, slim),
         qkv_rows, bias_pack),
        [like(whole, BF16), like((count, group_rows, slim), BF16), like((group_rows, packs), BF16),
         like((packs, model_width), BF16)],
        main_sems + side_sems, dense * packs,
    )
    rows_one = rows_one.reshape(group_rows, model_width)
    cotangent_late = lax.optimization_barrier((cotangent, rows_one))[0]
    grad_rows = lax.all_gather(cotangent_late, "mp", axis=0, tiled=True)
    mixed, totals = attend_forward(*seats, packed, all_first)
    units = up_bias.shape[0]
    rows_two, residual, hidden_pre, hidden = call(
        functools.partial(attend_out_kernel, count, chunk), 1,
        (mixed, out_flat, inputs, out_bias.reshape(row), mlp_norm_gain.reshape(row), mlp_norm_bias.reshape(row),
         up_weight, up_bias.reshape(1, units)),
        [like(whole, BF16), like(inputs.shape, F32), like((group_rows, units), F32), like((group_rows, units), BF16)],
        sum_scratch + main_sems, dense * (256 + units),
    )
    rows_two = rows_two.reshape(group_rows, model_width)
    grad_hidden = back_product(grad_rows, down_weight)
    grad_pre = jax.vjp(gelu_tanh, hidden_pre)[1](grad_hidden)[0].astype(BF16)
    grad_down_weight = rows_product(hidden, grad_rows).astype(BF16)
    grad_up_weight = rows_product(rows_two, grad_pre).astype(BF16)
    grad_up_bias = jnp.sum(grad_pre.astype(F32), axis=0)
    outer, inner = split_copies(copies)

    def sliced(values):
        return values.reshape(outer, inner, values.shape[0] // copies, values.shape[1])

    late = (grad_up_weight, grad_down_weight)
    grad_pre, late = lax.optimization_barrier((grad_pre, late))
    late_sums = lax.psum(late, "dp")
    grad_residual, sums_two, grad_mixed, grad_out_weight = call(
        functools.partial(mlp_back_kernel, count, chunk), 2,
        (grad_pre, up_weight, residual, cotangent, mlp_norm_gain.reshape(row), out_flat, mixed),
        [like(inputs.shape, F32), like((8, model_width), F32), like(mixed.shape, BF16), like(out_flat.shape, BF16)],
        [pltpu.VMEM(whole, BF16), pltpu.VMEM(out_flat.shape, F32)] + sum_scratch + main_sems,
        dense * up_bias.shape[0],
    )
    grad_out_weight = sliced(grad_out_weight)
    grad_flat, grad_skip, pack_sums, output, out_sum = call(
        functools.partial(attend_backward_kernel, count, copies, chunk, pairs_dev), 5,
        (seq_lengths, value_owner, packed, all_first, grad_mixed, totals, hidden, down_weight, residual,
         down_bias.reshape(row), grad_out_weight),
        [like((group_rows, packs), BF16), like((group_rows, slim), BF16), like((8, packs), F32),
         like(inputs.shape, BF16), like(grad_out_weight.shape, BF16)],
        [pltpu.VMEM((group_rows, LANES), F32), pltpu.VMEM((group_rows, LANES), F32),
         pltpu.VMEM((group_rows, LANES), BF16)] + sum_scratch + reduce_scratch(copies, grad_out_weight)
        + [pltpu.VMEM(grad_out_weight.shape[2:], BF16)] + gather_scratch(copies),
        group_rows * 1024 * 256 * 10 * pairs_dev, scalars=2,
    )
    pack_sums = pack_sums[0].reshape(pairs_dev, PACK, head_size)
    grad_qv_bias = jnp.concatenate([pack_sums[:, 0:2], pack_sums[:, 4:5]], axis=1)
    grad_qkv_weight = rows_product(grad_flat, rows_one).astype(BF16)
    grad_qkv_weight = grad_qkv_weight.reshape(pairs_dev, PACK, head_size, model_width)[:, 0:5]
    grad_qkv_weight = sliced(grad_qkv_weight.reshape(pairs_dev * 5 * head_size, model_width))
    wide_bias = jnp.pad(grad_up_bias, (0, model_width - grad_up_bias.shape[0])).reshape(row)
    slim_bias = jnp.pad(grad_qv_bias.reshape(-1), (0, model_width - grad_qv_bias.size)).reshape(row)
    own_sums = jnp.concatenate([sums_two[0:4], jnp.zeros((2, model_width), F32), wide_bias, slim_bias], axis=0)
    block = pltpu.VMEM(own_sums.shape, F32)
    grad_inputs, small, grad_first, qkv_sum = call(
        functools.partial(input_back_kernel, count, copies, chunk, 6, pairs_dev), 3,
        (value_owner, grad_flat, qkv_pack, inputs, grad_residual, attn_norm_gain.reshape(row), own_sums, grad_skip,
         grad_qkv_weight),
        [like(inputs.shape, BF16), like(own_sums.shape, F32), like((group_rows, slim), BF16),
         like(grad_qkv_weight.shape, BF16)],
        sum_scratch + reduce_scratch(copies, grad_qkv_weight)
        + [pltpu.VMEM((count, group_rows, slim), BF16), pltpu.VMEM(grad_qkv_weight.shape[2:], BF16), block]
        + side_sems + gather_scratch(copies)
        + [pltpu.VMEM((copies, *own_sums.shape), F32), pltpu.VMEM((count, *own_sums.shape), F32), block,
           pltpu.SemaphoreType.DMA((2, copies)), pltpu.SemaphoreType.DMA((2, count))],
        dense * packs, scalars=1,
    )
    qkv_sum = qkv_sum.reshape(pairs_dev, 5, head_size, model_width).astype(F32)
    qkv_sum = jnp.transpose(qkv_sum, (3, 0, 1, 2))
    late_sums = (*(part.astype(F32) for part in late_sums), out_sum.reshape(out_weight.shape).astype(F32))
    grad_first = grad_first.reshape(group_rows, pairs_dev, head_size)
    norm_sums = (small[4], small[5], small[2], small[0], small[1], small[3])
    bias_sums = (small[7, : grad_qv_bias.size].reshape(qv_bias.shape), small[6, : grad_up_bias.shape[0]])

    return (
        output,
        grad_inputs,
        grad_first,
        norm_sums[0],
        norm_sums[1],
        qkv_sum,
        bias_sums[0],
        late_sums[2],
        norm_sums[2],
        norm_sums[3],
        norm_sums[4],
        late_sums[0],
        bias_sums[1],
        late_sums[1],
        norm_sums[5],
    )


def solution(mesh):
    return jax.shard_map(
        body,
        mesh=mesh,
        in_specs=(
            P(("dp", "mp"), None),
            P("dp", "mp", None),
            P(("dp", "mp"), None),
            P("dp"),
            P(),
            P(),
            P(),
            P(None, "mp", None, None),
            P("mp", None, None),
            P("mp", None, None, None),
            P(),
            P(),
            P(),
            P(None, "mp"),
            P("mp"),
            P("mp", None),
            P(),
        ),
        out_specs=(
            P(("dp", "mp"), None),
            P(("dp", "mp"), None),
            P("dp", "mp", None),
            P(),
            P(),
            P(None, "mp", None, None),
            P("mp", None, None),
            P("mp", None, None, None),
            P(),
            P(),
            P(),
            P(None, "mp"),
            P("mp"),
            P("mp", None),
            P(),
        ),
        check_vma=False,
    )
```
